32 devices in a mesh: dp: 1 (over z), fsdp: 32 (over y, x, core).
Axes of the slice: x: 4, y: 4, z: 1, core: 2. Of those that a mesh axis runs over, the one named last changes fastest.
The devices are a block of a 4x4x8 slice.
Arguments:
- tokens: int32 [32, 64], P(('dp', 'fsdp'))
- embed_table: bfloat16 [32064, 3072], P('fsdp')
- norm_attn: bfloat16 [3072], P('fsdp')
- w_qkv: bfloat16 [3072, 9216], P('fsdp')
- w_out: bfloat16 [3072, 3072], P('fsdp')
- norm_mlp: bfloat16 [3072], P('fsdp')
- w_gate_up: bfloat16 [3072, 16384], P('fsdp')
- w_down: bfloat16 [8192, 3072], P('fsdp')
- rope_scale: float32 [48], replicated
Outputs:
- output 1: bfloat16 [32, 64, 3072], P(('dp', 'fsdp'))
- output 2: bfloat16 [32, 64, 32, 96], P(('dp', 'fsdp'))
- output 3: bfloat16 [32, 64, 32, 96], P(('dp', 'fsdp'))
All inputs are finite; a program needn't handle non-finite values.
Results may differ from the reference program's by a relative error of at most 0.0101458.
Values are sent between devices in bfloat16 or wider.
A program may use at most 768 MiB of HBM per device.

```python
import jax
import jax.numpy as jnp
from jax import lax

BATCH = 32
SEQ = 64
D = 3072
HEADS = 32
KV_HEADS = 32
HEAD = 96
FF = 8192
VOCAB = 32064

Q_WIDTH = HEADS * HEAD
KV_WIDTH = KV_HEADS * HEAD
HEAD_GROUP = HEADS // KV_HEADS
HALF_DIM = HEAD // 2
NORM_EPS = 1e-5
ROPE_THETA = 10000.0


def draw_tokens(tok_key):
    level_key, id_key = jax.random.split(tok_key)
    tok_level = jax.random.randint(level_key, (BATCH, SEQ), 0, 4)
    id_limit = VOCAB // jnp.power(8, tok_level)
    tokens = jax.random.randint(id_key, (BATCH, SEQ), 0, id_limit)
    return tokens.at[0, 0].set(VOCAB - 1).astype(jnp.int32)


def setup_inputs(seed: int = 0, part: int = 0) -> dict:
    base_key = jax.random.key(seed)
    sub_keys = jax.random.split(base_key, 9)
    tokens = draw_tokens(jax.random.fold_in(sub_keys[0], part))
    embed_table = jax.random.normal(sub_keys[1], (VOCAB, D), jnp.float32)
    norm_attn = 1.0 + 0.3 * jax.random.normal(sub_keys[2], (D,), jnp.float32)
    w_qkv = 1.5 * D ** -0.5 * jax.random.normal(sub_keys[3], (D, Q_WIDTH + 2 * KV_WIDTH), jnp.float32)
    w_out = Q_WIDTH ** -0.5 * jax.random.normal(sub_keys[4], (Q_WIDTH, D), jnp.float32)
    norm_mlp = 1.0 + 0.3 * jax.random.normal(sub_keys[5], (D,), jnp.float32)
    w_gate_up = D ** -0.5 * jax.random.normal(sub_keys[6], (D, 2 * FF), jnp.float32)
    w_down = FF ** -0.5 * jax.random.normal(sub_keys[7], (FF, D), jnp.float32)
    rope_scale = jax.random.uniform(sub_keys[8], (HALF_DIM,), jnp.float32, 1.0, 4.0)
    return {
        'tokens': tokens,
        'embed_table': embed_table.astype(jnp.bfloat16),
        'norm_attn': norm_attn.astype(jnp.bfloat16),
        'w_qkv': w_qkv.astype(jnp.bfloat16),
        'w_out': w_out.astype(jnp.bfloat16),
        'norm_mlp': norm_mlp.astype(jnp.bfloat16),
        'w_gate_up': w_gate_up.astype(jnp.bfloat16),
        'w_down': w_down.astype(jnp.bfloat16),
        'rope_scale': rope_scale,
    }


def rms_norm(hidden, gain):
    h_f32 = hidden.astype(jnp.float32)
    inv_rms = lax.rsqrt(jnp.mean(h_f32 * h_f32, axis=-1, keepdims=True) + NORM_EPS)
    return (h_f32 * inv_rms * gain.astype(jnp.float32)).astype(jnp.bfloat16)


def reference(tokens, embed_table, norm_attn, w_qkv, w_out, norm_mlp, w_gate_up, w_down, rope_scale):
    freq_expo = jnp.arange(HALF_DIM, dtype=jnp.float32) * (2.0 / HEAD)
    inv_freq = 1.0 / (rope_scale * jnp.power(ROPE_THETA, freq_expo))
    angles = jnp.arange(SEQ, dtype=jnp.float32)[:, None] * inv_freq[None, :]
    cos_tab = jnp.cos(angles)[:, None, :]
    sin_tab = jnp.sin(angles)[:, None, :]
    causal = jnp.arange(SEQ)[:, None] >= jnp.arange(SEQ)[None, :]

    def rotate(proj):
        low_half = proj[..., :HALF_DIM]
        high_half = proj[..., HALF_DIM:]
        return jnp.concatenate([low_half * cos_tab - high_half * sin_tab, high_half * cos_tab + low_half * sin_tab], axis=-1)

    def one_sequence(seq_tokens):
        hidden = jnp.take(embed_table, seq_tokens, axis=0)
        normed = rms_norm(hidden, norm_attn)
        qkv_proj = jnp.dot(normed, w_qkv, preferred_element_type=jnp.float32)
        query_rot = rotate(qkv_proj[:, :Q_WIDTH].reshape(SEQ, HEADS, HEAD)).astype(jnp.bfloat16)
        key_rot = rotate(qkv_proj[:, Q_WIDTH:Q_WIDTH + KV_WIDTH].reshape(SEQ, KV_HEADS, HEAD)).astype(jnp.bfloat16)
        values = qkv_proj[:, Q_WIDTH + KV_WIDTH:].reshape(SEQ, KV_HEADS, HEAD).astype(jnp.bfloat16)
        q_grouped = query_rot.reshape(SEQ, KV_HEADS, HEAD_GROUP, HEAD)
        scores = jnp.einsum('qkgd,skd->kgqs', q_grouped.astype(jnp.float32), key_rot.astype(jnp.float32)) * (HEAD ** -0.5)
        scores = jnp.where(causal, scores, -jnp.inf)
        scores = scores - jnp.max(scores, axis=-1, keepdims=True)
        weights = jnp.exp(scores)
        attn_probs = (weights / jnp.sum(weights, axis=-1, keepdims=True)).astype(jnp.bfloat16)
        context = jnp.einsum('kgqs,skd->qkgd', attn_probs.astype(jnp.float32), values.astype(jnp.float32))
        context = context.astype(jnp.bfloat16).reshape(SEQ, Q_WIDTH)
        attn_proj = jnp.dot(context, w_out, preferred_element_type=jnp.float32)
        resid_mid = (hidden.astype(jnp.float32) + attn_proj).astype(jnp.bfloat16)
        normed_mlp = rms_norm(resid_mid, norm_mlp)
        gate_up = jnp.dot(normed_mlp, w_gate_up, preferred_element_type=jnp.float32)
        mlp_act = (jax.nn.silu(gate_up[:, :FF]) * gate_up[:, FF:]).astype(jnp.bfloat16)
        down_proj = jnp.dot(mlp_act, w_down, preferred_element_type=jnp.float32)
        layer_out = (resid_mid.astype(jnp.float32) + down_proj).astype(jnp.bfloat16)
        return layer_out, key_rot, values

    hidden_out, key_cache, value_cache = lax.map(one_sequence, tokens)
    return hidden_out, key_cache, value_cache
```

```python
import functools
import math

import jax
import jax.numpy as jnp
from jax import lax
from jax.experimental import pallas as pl
from jax.experimental.pallas import tpu as pltpu
from jax.sharding import PartitionSpec as P

NORM_EPS = 1e-5
ROPE_THETA = 10000.0
AXIS = 'fsdp'
MESH = pl.DeviceIdType.MESH
ANY = pl.BlockSpec(memory_space=pl.ANY)
VMEM_LIMIT = 60 * 1024 * 1024


class Place:
    def __init__(self, side):
        me = lax.axis_index(AXIS)
        self.side = side
        self.c = lax.rem(me, 2)
        chip = lax.div(me, 2)
        self.y = lax.div(chip, side)
        self.x = lax.rem(chip, side)
        self.me = me
        self.partner = me + 1 - 2 * self.c

    def chip(self, dy, dx):
        s = self.side
        return lax.rem(self.y + dy + s, s) * s + lax.rem(self.x + dx + s, s)

    def dev(self, dy, dx):
        return self.chip(dy, dx) * 2 + self.c


def barrier(devices):
    sem = pltpu.get_barrier_semaphore()
    for d in devices:
        pl.semaphore_signal(sem, inc=1, device_id={AXIS: d}, device_id_type=MESH)
    pl.semaphore_wait(sem, len(devices))


class Msgs:
    def __init__(self, send_sem, recv_sem):
        self.send_sem, self.recv_sem = send_sem, recv_sem
        self.index, self.copies = {}, []

    def start(self, name, src, dst, dev):
        i = len(self.copies)
        self.index[name] = i
        copy = pltpu.make_async_remote_copy(
            src_ref=src, dst_ref=dst, send_sem=self.send_sem.at[i], recv_sem=self.recv_sem.at[i],
            device_id={AXIS: dev}, device_id_type=MESH)
        copy.start()
        self.copies.append(copy)

    def recv(self, name):
        self.copies[self.index[name]].wait_recv()

    def drain(self):
        for copy in self.copies:
            copy.wait_send()


AG_MSGS = 40
RS_MSGS = 40


def torus_all_gather(pos, m, blk, width):
    q = width // 4
    halves = (0, 1)
    order = (0, -1, 1, 2)

    def at(h, a, b):
        return (b, a) if h == 0 else (a, b)

    def chip(h, a, b):
        return pos.chip(*at(h, a, b))

    def dev(h, a, b):
        return pos.dev(*at(h, a, b))

    def send(h, name, a, b, lo, n, ta, tb):
        ref = blk(chip(h, a, b), 2 * q * h + lo, n)
        m.start(('ag', h) + name, ref, ref, dev(h, ta, tb))

    def recv(h, *name):
        m.recv(('ag', h) + name)

    def second(h, a):
        send(h, ('2p', a), a, 0, 0, 2 * q, 0, 1)
        send(h, ('2m', a), a, 0, 0, 2 * q, 0, -1)

    def second_forward(h, a):
        recv(h, '2p', a)
        send(h, ('2pf', a), a, -1, 0, q, 0, 1)
        recv(h, '2m', a)
        send(h, ('2mf', a), a, 1, q, q, 0, -1)

    for h in halves:
        send(h, ('1p',), 0, 0, 0, 2 * q, 1, 0)
        send(h, ('1m',), 0, 0, 0, 2 * q, -1, 0)
    for h in halves:
        second(h, 0)
    for h in halves:
        recv(h, '1p')
        send(h, ('1pf',), -1, 0, 0, q, 1, 0)
        second(h, -1)
    for h in halves:
        recv(h, '1m')
        send(h, ('1mf',), 1, 0, q, q, -1, 0)
        second(h, 1)
    for h in halves:
        second_forward(h, 0)
    for h in halves:
        recv(h, '1pf')
        recv(h, '1mf')
        second(h, 2)
    for a in (-1, 1, 2):
        for h in halves:
            second_forward(h, a)
    for a in order:
        for h in halves:
            recv(h, '2pf', a)
            recv(h, '2mf', a)


def torus_reduce_scatter(pos, m, part, recv_buf, width):
    q = width // 4
    halves = (0, 1)
    slots = {}

    def at(h, a, b):
        return (a, b) if h == 0 else (b, a)

    def chip(h, a, b):
        return pos.chip(*at(h, a, b))

    def dev(h, a, b):
        return pos.dev(*at(h, a, b))

    def slot(key, n):
        if key not in slots:
            slots[key] = sum(k for _, k in slots.values()), n
        return slots[key][0]

    def send(h, name, a, b, lo, n, ta, tb):
        key = ('rs', h) + name
        first = slot(key, n // q)
        src = part.at[chip(h, a, b), :, pl.ds(2 * q * h + lo, n)]
        m.start(key, src, recv_buf.at[:, pl.ds(first * q, n)], dev(h, ta, tb))

    def recv_add(h, name, a, b, lo, n):
        key = ('rs', h) + name
        m.recv(key)
        first = slots[key][0]
        sl = pl.ds(2 * q * h + lo, n)
        p = chip(h, a, b)
        part[p, :, sl] = part[p, :, sl] + recv_buf[:, pl.ds(first * q, n)]

    order = (2, 1, -1, 0)
    for b in order:
        for h in halves:
            send(h, ('1pf', b), 2, b, 0, q, 1, 0)
            send(h, ('1mf', b), 2, b, q, q, -1, 0)
    for b in order:
        for h in halves:
            recv_add(h, ('1pf', b), 1, b, 0, q)
            send(h, ('1p', b), 1, b, 0, 2 * q, 1, 0)
            recv_add(h, ('1mf', b), -1, b, q, q)
            send(h, ('1m', b), -1, b, 0, 2 * q, -1, 0)
    for b in order:
        for h in halves:
            recv_add(h, ('1p', b), 0, b, 0, 2 * q)
            recv_add(h, ('1m', b), 0, b, 0, 2 * q)
            if b == 2:
                send(h, ('2pf',), 0, 2, 0, q, 0, 1)
                send(h, ('2mf',), 0, 2, q, q, 0, -1)
            if b == 1:
                recv_add(h, ('2pf',), 0, 1, 0, q)
                send(h, ('2p',), 0, 1, 0, 2 * q, 0, 1)
            if b == -1:
                recv_add(h, ('2mf',), 0, -1, q, q)
                send(h, ('2m',), 0, -1, 0, 2 * q, 0, -1)
            if b == 0:
                recv_add(h, ('2p',), 0, 0, 0, 2 * q)
                recv_add(h, ('2m',), 0, 0, 0, 2 * q)


def torus_neighbours(pos):
    return [pos.dev(0, 1), pos.dev(0, -1), pos.dev(1, 0), pos.dev(-1, 0)]


def offsets(side):
    every = [(dy, dx) for dy in range(side) for dx in range(side) if (dy, dx) != (0, 0)]
    return sorted(every, key=lambda o: min(o[0], side - o[0]) + min(o[1], side - o[1]))


def start_kernel(side, tok, wq, wgu, wo, table, tok_all, wq_all, wgu_all, wo_all, table_other,
                 t_send, t_recv, q_send, q_recv, g_send, g_recv, o_send, o_recv, f_send, f_recv, l_sem):
    pos = Place(side)
    offs = offsets(side)
    me_chip = pos.chip(0, 0)
    ff = wgu.shape[1] // 2
    ffb = ff // (side * side)
    barrier([pos.dev(dy, dx) for dy, dx in offs] + [pos.partner])

    def remote(src, dst, s, r, dev):
        return pltpu.make_async_remote_copy(src_ref=src, dst_ref=dst, send_sem=s, recv_sem=r,
                                            device_id={AXIS: dev}, device_id_type=MESH)

    toks, qs, gs, fs = [], [], [], []
    for i, (dy, dx) in enumerate(offs):
        cp = remote(tok, tok_all.at[me_chip], t_send.at[i], t_recv.at[i], pos.dev(dy, dx))
        cp.start()
        toks.append(cp)
    tcp = remote(table, table_other, f_send.at[0], f_recv.at[0], pos.partner)
    tcp.start()
    for i, (dy, dx) in enumerate(offs):
        cp = remote(wq.at[pos.chip(dy, dx)], wq_all.at[me_chip, pos.c], q_send.at[i], q_recv.at[i], pos.dev(dy, dx))
        cp.start()
        qs.append(cp)
    own = [pltpu.make_async_copy(tok, tok_all.at[me_chip], l_sem.at[0]),
           pltpu.make_async_copy(wq.at[me_chip], wq_all.at[me_chip, pos.c], l_sem.at[1]),
           pltpu.make_async_copy(wo, wo_all.at[me_chip, pos.c], l_sem.at[2])]
    for j in (0, 1):
        src = wgu.at[:, pl.ds(pl.multiple_of(j * ff + me_chip * ffb, 128), ffb)]
        own.append(pltpu.make_async_copy(src, wgu_all.at[me_chip, pos.c, :, pl.ds(j * ffb, ffb)], l_sem.at[3 + j]))
    for cp in own:
        cp.start()
    for i, (dy, dx) in enumerate(offs):
        for j in (0, 1):
            src = wgu.at[:, pl.ds(pl.multiple_of(j * ff + pos.chip(dy, dx) * ffb, 128), ffb)]
            cp = remote(src, wgu_all.at[me_chip, pos.c, :, pl.ds(j * ffb, ffb)],
                        g_send.at[2 * i + j], g_recv.at[2 * i + j], pos.dev(dy, dx))
            cp.start()
            gs.append(cp)
    for cp in own:
        cp.wait()

    def forward(k, ref):
        cp = remote(ref, ref, f_send.at[k], f_recv.at[k], pos.partner)
        cp.start()
        fs.append(cp)

    forward(1, wq_all.at[me_chip, pos.c])
    forward(2, wgu_all.at[me_chip, pos.c])
    forward(3, wo_all.at[me_chip, pos.c])
    for i, (dy, dx) in enumerate(offs):
        qs[i].wait_recv()
        forward(4 + i, wq_all.at[pos.chip(-dy, -dx), pos.c])
    m = Msgs(o_send, o_recv)
    torus_all_gather(pos, m, lambda p, lo, n: wo_all.at[p, pos.c, :, pl.ds(lo, n)], wo.shape[1])
    n = len(offs)
    for i, (dy, dx) in enumerate(offs):
        forward(4 + n + i, wo_all.at[pos.chip(-dy, -dx), pos.c])
    for i, (dy, dx) in enumerate(offs):
        gs[2 * i].wait_recv()
        gs[2 * i + 1].wait_recv()
        forward(4 + 2 * n + i, wgu_all.at[pos.chip(-dy, -dx), pos.c])
    for cp in toks:
        cp.wait()
    tcp.wait()
    for cp in qs + gs:
        cp.wait_send()
    m.drain()
    for cp in fs:
        cp.wait()


def embed_kernel(side, part_hbm, x_all, part, recv_buf, s1, r1, s2, r2, l_sem):
    pos = Place(side)
    barrier(torus_neighbours(pos))
    width = x_all.shape[2]
    loads = [pltpu.make_async_copy(part_hbm.at[i], part.at[i], l_sem.at[i]) for i in range(side * side)]
    for cp in loads:
        cp.start()
    for cp in loads:
        cp.wait()
    m = Msgs(s1, r1)
    torus_reduce_scatter(pos, m, part, recv_buf, width)
    me_chip = pos.chip(0, 0)
    x_all[me_chip] = part[me_chip]
    m2 = Msgs(s2, r2)
    torus_all_gather(pos, m2, lambda p, lo, n: x_all.at[p, :, pl.ds(lo, n)], width)
    m.drain()
    m2.drain()


def gather_kernel(side, x, x_all, s2, r2, l_sem):
    pos = Place(side)
    me_chip = pos.chip(0, 0)
    cp = pltpu.make_async_copy(x, x_all.at[me_chip], l_sem.at[0])
    cp.start()
    barrier(torus_neighbours(pos))
    cp.wait()
    m = Msgs(s2, r2)
    torus_all_gather(pos, m, lambda p, lo, n: x_all.at[p, :, pl.ds(lo, n)], x_all.shape[2])
    m.drain()


def scatter_kernel(side, part_hbm, out, part, recv_buf, s1, r1, l_sem):
    pos = Place(side)
    barrier(torus_neighbours(pos))
    width = out.shape[1]
    loads = [pltpu.make_async_copy(part_hbm.at[i], part.at[i], l_sem.at[i]) for i in range(side * side)]
    for cp in loads:
        cp.start()
    for cp in loads:
        cp.wait()
    m = Msgs(s1, r1)
    torus_reduce_scatter(pos, m, part, recv_buf, width)
    out[...] = part[pos.chip(0, 0)]
    m.drain()


def exchange_kernel(side, src, dst, sems, recvs, l_sem):
    pos = Place(side)
    offs = offsets(side)
    me_chip = pos.chip(0, 0)
    barrier([pos.dev(dy, dx) for dy, dx in offs])
    copies = []
    for i, (dy, dx) in enumerate(offs):
        cp = pltpu.make_async_remote_copy(
            src_ref=src.at[pos.chip(dy, dx)], dst_ref=dst.at[me_chip], send_sem=sems.at[i], recv_sem=recvs.at[i],
            device_id={AXIS: pos.dev(dy, dx)}, device_id_type=MESH)
        cp.start()
        copies.append(cp)
    own = pltpu.make_async_copy(src.at[me_chip], dst.at[me_chip], l_sem.at[0])
    own.start()
    own.wait()
    for cp in copies:
        cp.wait()


def dma(n):
    return pltpu.SemaphoreType.DMA((n,))


def params(cid):
    return pltpu.CompilerParams(collective_id=cid, has_side_effects=True, vmem_limit_bytes=VMEM_LIMIT)


def rms_norm(hidden, gain):
    h_f32 = hidden.astype(jnp.float32)
    inv_rms = lax.rsqrt(jnp.mean(h_f32 * h_f32, axis=-1, keepdims=True) + NORM_EPS)
    return (h_f32 * inv_rms * gain.astype(jnp.float32)).astype(jnp.bfloat16)


def apply_rope(proj, rope_scale):
    seq_len = proj.shape[1]
    head_dim = proj.shape[-1]
    half_dim = head_dim // 2
    freq_expo = jnp.arange(half_dim, dtype=jnp.float32) * (2.0 / head_dim)
    inv_freq = 1.0 / (rope_scale * jnp.power(ROPE_THETA, freq_expo))
    angles = jnp.arange(seq_len, dtype=jnp.float32)[:, None] * inv_freq[None, :]
    cos_tab = jnp.cos(angles)[:, None, :]
    sin_tab = jnp.sin(angles)[:, None, :]
    low_half = proj[..., :half_dim]
    high_half = proj[..., half_dim:]
    return jnp.concatenate([low_half * cos_tab - high_half * sin_tab, high_half * cos_tab + low_half * sin_tab], axis=-1)


def solution(mesh):
    batch_axes = ('dp', AXIS)
    row_spec = P(AXIS, None)
    n_dev = mesh.shape[AXIS]
    chips = n_dev // 2
    side = math.isqrt(chips)
    n_off = chips - 1

    def device_step(tokens, embed_table, norm_attn, w_qkv, w_out, norm_mlp, w_gate_up, w_down, rope_scale):
        f32, bf16 = jnp.float32, jnp.bfloat16
        seq = tokens.shape[1]
        rows, d_model = w_out.shape
        rows_table = embed_table.shape[0]
        head_dim = 2 * rope_scale.shape[0]
        q_width = rows * n_dev
        kv_width = (w_qkv.shape[1] - q_width) // 2
        heads = q_width // head_dim // chips
        kv_heads = kv_width // head_dim // chips
        qb, kb = heads * head_dim, kv_heads * head_dim
        width = qb + 2 * kb
        pad_width = -(-(width + 2) // 128) * 128
        ff = w_gate_up.shape[1] // 2
        ffb = ff // chips
        me = lax.axis_index(AXIS)
        rest = jnp.zeros((chips, rows, pad_width - width - 2), bf16)
        wq_blocks = jnp.concatenate([
            w_qkv[:, :q_width].reshape(rows, chips, qb).transpose(1, 0, 2),
            w_qkv[:, q_width:q_width + kv_width].reshape(rows, chips, kb).transpose(1, 0, 2),
            w_qkv[:, q_width + kv_width:].reshape(rows, chips, kb).transpose(1, 0, 2),
            jnp.broadcast_to(norm_attn[None, :, None], (chips, rows, 1)),
            jnp.broadcast_to(norm_mlp[None, :, None], (chips, rows, 1)), rest], axis=-1)

        tok_all, wq_all, wgu_all, wo_all, table_other = pl.pallas_call(
            functools.partial(start_kernel, side), name='start',
            out_shape=(jax.ShapeDtypeStruct((chips, 1, seq), jnp.int32),
                       jax.ShapeDtypeStruct((chips, 2, rows, pad_width), bf16),
                       jax.ShapeDtypeStruct((chips, 2, rows, 2 * ffb), bf16),
                       jax.ShapeDtypeStruct((chips, 2, rows, d_model), bf16),
                       jax.ShapeDtypeStruct((rows_table, d_model), bf16)),
            in_specs=[ANY] * 5, out_specs=(ANY,) * 5,
            scratch_shapes=[dma(n_off), dma(n_off), dma(n_off), dma(n_off), dma(2 * n_off), dma(2 * n_off),
                            dma(AG_MSGS), dma(AG_MSGS), dma(4 + 3 * n_off), dma(4 + 3 * n_off), dma(5)],
            compiler_params=params(1),
        )(tokens, wq_blocks, w_gate_up, w_out, embed_table)

        gains = wq_all[..., width:width + 2].reshape(d_model, 2)
        gain_attn, gain_mlp = gains[:, 0], gains[:, 1]
        wq_own = wq_all.reshape(d_model, pad_width)
        wgu_own = wgu_all.reshape(d_model, 2 * ffb)
        wo_full = wo_all.reshape(q_width, d_model)

        ids = tok_all.reshape(chips * seq)
        row_ids = jnp.arange(rows_table, dtype=jnp.int32)

        def pick(device, table):
            hot = ((ids - device * rows_table)[:, None] == row_ids[None, :]).astype(bf16)
            return jnp.dot(hot, table, preferred_element_type=f32)

        part = (pick(me, embed_table) + pick(me + 1 - 2 * lax.rem(me, 2), table_other)).astype(bf16)
        part = part.reshape(chips, seq, d_model)

        x_all = pl.pallas_call(
            functools.partial(embed_kernel, side), name='embed',
            out_shape=jax.ShapeDtypeStruct((chips, seq, d_model), bf16),
            in_specs=[ANY], out_specs=pl.BlockSpec(memory_space=pltpu.VMEM),
            scratch_shapes=[pltpu.VMEM((chips, seq, d_model), bf16),
                            pltpu.VMEM((seq, d_model * n_off), bf16),
                            dma(RS_MSGS), dma(RS_MSGS), dma(AG_MSGS), dma(AG_MSGS), dma(chips)],
            compiler_params=params(2),
        )(part)
        chip = lax.div(me, 2)
        x_own = lax.dynamic_index_in_dim(x_all, chip, 0, keepdims=False)

        normed = rms_norm(x_all.reshape(chips * seq, d_model), gain_attn)
        proj = jnp.dot(normed, wq_own, preferred_element_type=f32)[:, :width].reshape(chips, seq, width)
        query = apply_rope(proj[..., :qb].reshape(chips, seq, heads, head_dim), rope_scale).astype(bf16)
        key = apply_rope(proj[..., qb:qb + kb].reshape(chips, seq, kv_heads, head_dim), rope_scale).astype(bf16)
        value = proj[..., qb + kb:].astype(bf16).reshape(chips, seq, kv_heads, head_dim)
        q_grouped = query.reshape(chips, seq, kv_heads, heads // kv_heads, head_dim)
        scores = jnp.einsum('bqkgd,bskd->bkgqs', q_grouped, key, preferred_element_type=f32) * (head_dim ** -0.5)
        causal = jnp.arange(seq)[:, None] >= jnp.arange(seq)[None, :]
        scores = jnp.where(causal, scores, -jnp.inf)
        scores = scores - jnp.max(scores, axis=-1, keepdims=True)
        weights = jnp.exp(scores)
        probs = (weights / jnp.sum(weights, axis=-1, keepdims=True)).astype(bf16)
        context = jnp.einsum('bkgqs,bskd->bqkgd', probs, value, preferred_element_type=f32).astype(bf16)
        context = context.reshape(chips, seq, qb)
        packed = jnp.concatenate([context, key.reshape(chips, seq, kb), value.reshape(chips, seq, kb)], axis=-1)

        mine = pl.pallas_call(
            functools.partial(exchange_kernel, side), name='to_sequences',
            out_shape=jax.ShapeDtypeStruct((chips, seq, width), bf16),
            in_specs=[ANY], out_specs=ANY,
            scratch_shapes=[dma(n_off), dma(n_off), dma(1)],
            compiler_params=params(3),
        )(packed)
        ctx_own = mine[..., :qb].transpose(1, 0, 2).reshape(seq, q_width)
        key_own = mine[..., qb:qb + kb].reshape(chips, seq, kv_heads, head_dim).transpose(1, 0, 2, 3)
        val_own = mine[..., qb + kb:].reshape(chips, seq, kv_heads, head_dim).transpose(1, 0, 2, 3)
        key_own = key_own.reshape(1, seq, chips * kv_heads, head_dim)
        val_own = val_own.reshape(1, seq, chips * kv_heads, head_dim)

        attn_proj = jnp.dot(ctx_own, wo_full, preferred_element_type=f32)
        x_mid = (x_own.astype(f32) + attn_proj).astype(bf16)
        normed_mlp = rms_norm(x_mid, gain_mlp)

        h_all = pl.pallas_call(
            functools.partial(gather_kernel, side), name='gather_hidden',
            out_shape=jax.ShapeDtypeStruct((chips, seq, d_model), bf16),
            in_specs=[pl.BlockSpec(memory_space=pltpu.VMEM)], out_specs=pl.BlockSpec(memory_space=pl.ANY),
            scratch_shapes=[dma(AG_MSGS), dma(AG_MSGS), dma(1)],
            compiler_params=params(4),
        )(normed_mlp)

        wd_other = pl.pallas_call(
            swap_kernel, name='swap_down',
            out_shape=jax.ShapeDtypeStruct(w_down.shape, bf16),
            in_specs=[ANY], out_specs=ANY, scratch_shapes=[dma(1), dma(1)],
            compiler_params=params(6),
        )(w_down)
        first = lax.rem(me, 2) == 0

        gate_up = jnp.dot(h_all.reshape(chips * seq, d_model), wgu_own, preferred_element_type=f32)
        act = (jax.nn.silu(gate_up[:, :ffb]) * gate_up[:, ffb:]).astype(bf16)
        half = ffb // 2
        act_own = lax.dynamic_slice_in_dim(act, lax.rem(me, 2) * half, half, axis=1)
        act_other = lax.dynamic_slice_in_dim(act, (1 - lax.rem(me, 2)) * half, half, axis=1)
        down = (jnp.dot(act_own, w_down, preferred_element_type=f32)
                + jnp.dot(act_other, wd_other, preferred_element_type=f32))

        total = pl.pallas_call(
            functools.partial(scatter_kernel, side), name='scatter_down',
            out_shape=jax.ShapeDtypeStruct((seq, d_model), f32),
            in_specs=[ANY], out_specs=pl.BlockSpec(memory_space=pltpu.VMEM),
            scratch_shapes=[pltpu.VMEM((chips, seq, d_model), f32),
                            pltpu.VMEM((seq, d_model * n_off), f32),
                            dma(RS_MSGS), dma(RS_MSGS), dma(chips)],
            compiler_params=params(5),
        )(down.reshape(chips, seq, d_model))
        layer_out = (x_mid.astype(f32) + total).astype(bf16)
        return layer_out[None], key_own, val_own

    return jax.shard_map(
        device_step,
        mesh=mesh,
        in_specs=(P(batch_axes, None), row_spec, P(AXIS), row_spec, row_spec, P(AXIS), row_spec, row_spec, P(None)),
        out_specs=(P(batch_axes, None, None), P(batch_axes, None, None, None), P(batch_axes, None, None, None)),
        check_vma=False,
    )


def swap_kernel(src, dst, send_sem, recv_sem):
    me = lax.axis_index(AXIS)
    partner = me + 1 - 2 * lax.rem(me, 2)
    barrier([partner])
    cp = pltpu.make_async_remote_copy(src_ref=src, dst_ref=dst, send_sem=send_sem.at[0], recv_sem=recv_sem.at[0],
                                      device_id={AXIS: partner}, device_id_type=MESH)
    cp.start()
    cp.wait()
```

```python
import functools
import math

import jax
import jax.numpy as jnp
from jax import lax
from jax.experimental import pallas as pl
from jax.experimental.pallas import tpu as pltpu
from jax.sharding import PartitionSpec as P

NORM_EPS = 1e-5
ROPE_THETA = 10000.0
AXIS = 'fsdp'
MESH = pl.DeviceIdType.MESH
ANY = pl.BlockSpec(memory_space=pl.ANY)
VMEM_LIMIT = 60 * 1024 * 1024


class Place:
    def __init__(self, side):
        me = lax.axis_index(AXIS)
        self.side = side
        self.c = lax.rem(me, 2)
        chip = lax.div(me, 2)
        self.y = lax.div(chip, side)
        self.x = lax.rem(chip, side)
        self.me = me
        self.partner = me + 1 - 2 * self.c

    def chip(self, dy, dx):
        s = self.side
        return lax.rem(self.y + dy + s, s) * s + lax.rem(self.x + dx + s, s)

    def dev(self, dy, dx):
        return self.chip(dy, dx) * 2 + self.c


def barrier(devices):
    sem = pltpu.get_barrier_semaphore()
    for d in devices:
        pl.semaphore_signal(sem, inc=1, device_id={AXIS: d}, device_id_type=MESH)
    pl.semaphore_wait(sem, len(devices))


class Msgs:
    def __init__(self, send_sem, recv_sem):
        self.send_sem, self.recv_sem = send_sem, recv_sem
        self.index, self.copies = {}, []

    def start(self, name, src, dst, dev):
        i = len(self.copies)
        self.index[name] = i
        copy = pltpu.make_async_remote_copy(
            src_ref=src, dst_ref=dst, send_sem=self.send_sem.at[i], recv_sem=self.recv_sem.at[i],
            device_id={AXIS: dev}, device_id_type=MESH)
        copy.start()
        self.copies.append(copy)

    def recv(self, name):
        self.copies[self.index[name]].wait_recv()

    def drain(self):
        for copy in self.copies:
            copy.wait_send()


AG_MSGS = 40
RS_MSGS = 40


def torus_all_gather(pos, m, blk, width):
    q = width // 4
    halves = (0, 1)
    order = (0, -1, 1, 2)

    def at(h, a, b):
        return (b, a) if h == 0 else (a, b)

    def chip(h, a, b):
        return pos.chip(*at(h, a, b))

    def dev(h, a, b):
        return pos.dev(*at(h, a, b))

    def send(h, name, a, b, lo, n, ta, tb):
        ref = blk(chip(h, a, b), 2 * q * h + lo, n)
        m.start(('ag', h) + name, ref, ref, dev(h, ta, tb))

    def recv(h, *name):
        m.recv(('ag', h) + name)

    def second(h, a):
        send(h, ('2p', a), a, 0, 0, 2 * q, 0, 1)
        send(h, ('2m', a), a, 0, 0, 2 * q, 0, -1)

    def second_forward(h, a):
        recv(h, '2p', a)
        send(h, ('2pf', a), a, -1, 0, q, 0, 1)
        recv(h, '2m', a)
        send(h, ('2mf', a), a, 1, q, q, 0, -1)

    for h in halves:
        send(h, ('1p',), 0, 0, 0, 2 * q, 1, 0)
        send(h, ('1m',), 0, 0, 0, 2 * q, -1, 0)
    for h in halves:
        second(h, 0)
    for h in halves:
        recv(h, '1p')
        send(h, ('1pf',), -1, 0, 0, q, 1, 0)
        second(h, -1)
    for h in halves:
        recv(h, '1m')
        send(h, ('1mf',), 1, 0, q, q, -1, 0)
        second(h, 1)
    for h in halves:
        second_forward(h, 0)
    for h in halves:
        recv(h, '1pf')
        recv(h, '1mf')
        second(h, 2)
    for a in (-1, 1, 2):
        for h in halves:
            second_forward(h, a)
    for a in order:
        for h in halves:
            recv(h, '2pf', a)
            recv(h, '2mf', a)


def torus_reduce_scatter(pos, m, part, recv_buf, width):
    q = width // 4
    halves = (0, 1)
    slots = {}

    def at(h, a, b):
        return (a, b) if h == 0 else (b, a)

    def chip(h, a, b):
        return pos.chip(*at(h, a, b))

    def dev(h, a, b):
        return pos.dev(*at(h, a, b))

    def slot(key, n):
        if key not in slots:
            slots[key] = sum(k for _, k in slots.values()), n
        return slots[key][0]

    def send(h, name, a, b, lo, n, ta, tb):
        key = ('rs', h) + name
        first = slot(key, n // q)
        src = part.at[chip(h, a, b), :, pl.ds(2 * q * h + lo, n)]
        m.start(key, src, recv_buf.at[:, pl.ds(first * q, n)], dev(h, ta, tb))

    def recv_add(h, name, a, b, lo, n):
        key = ('rs', h) + name
        m.recv(key)
        first = slots[key][0]
        sl = pl.ds(2 * q * h + lo, n)
        p = chip(h, a, b)
        part[p, :, sl] = part[p, :, sl] + recv_buf[:, pl.ds(first * q, n)]

    order = (2, 1, -1, 0)
    for b in order:
        for h in halves:
            send(h, ('1pf', b), 2, b, 0, q, 1, 0)
            send(h, ('1mf', b), 2, b, q, q, -1, 0)
    for b in order:
        for h in halves:
            recv_add(h, ('1pf', b), 1, b, 0, q)
            send(h, ('1p', b), 1, b, 0, 2 * q, 1, 0)
            recv_add(h, ('1mf', b), -1, b, q, q)
            send(h, ('1m', b), -1, b, 0, 2 * q, -1, 0)
    for b in order:
        for h in halves:
            recv_add(h, ('1p', b), 0, b, 0, 2 * q)
            recv_add(h, ('1m', b), 0, b, 0, 2 * q)
            if b == 2:
                send(h, ('2pf',), 0, 2, 0, q, 0, 1)
                send(h, ('2mf',), 0, 2, q, q, 0, -1)
            if b == 1:
                recv_add(h, ('2pf',), 0, 1, 0, q)
                send(h, ('2p',), 0, 1, 0, 2 * q, 0, 1)
            if b == -1:
                recv_add(h, ('2mf',), 0, -1, q, q)
                send(h, ('2m',), 0, -1, 0, 2 * q, 0, -1)
            if b == 0:
                recv_add(h, ('2p',), 0, 0, 0, 2 * q)
                recv_add(h, ('2m',), 0, 0, 0, 2 * q)


SLOTS = ((0, 0), (0, 1), (0, -1), (1, 0), (-1, 0), (1, 1), (1, -1), (-1, 1), (-1, -1),
         (2, 0), (0, 2), (2, 1), (2, -1), (1, 2), (-1, 2), (2, 2))


def slot_of(a, b):
    return SLOTS.index(((a + 1) % 4 - 1, (b + 1) % 4 - 1))


def swap_if(h, a, b):
    return (b, a) if h == 0 else (a, b)


HALVES = (0, 1)


class Gather:
    def __init__(self, pos, m, blk, width):
        self.pos, self.m, self.blk, self.q = pos, m, blk, width // 4

    def send(self, h, name, a, b, lo, n, ta, tb):
        lo = 2 * self.q * h + lo
        src = self.blk(slot_of(*swap_if(h, a, b)), lo, n)
        dst = self.blk(slot_of(*swap_if(h, a - ta, b - tb)), lo, n)
        self.m.start(('ag', h) + name, src, dst, self.pos.dev(*swap_if(h, ta, tb)))

    def recv(self, h, *name):
        self.m.recv(('ag', h) + name)

    def second(self, h, a):
        self.send(h, ('2p', a), a, 0, 0, 2 * self.q, 0, 1)
        self.send(h, ('2m', a), a, 0, 0, 2 * self.q, 0, -1)

    def second_forward(self, a):
        for h in HALVES:
            self.recv(h, '2p', a)
            self.send(h, ('2pf', a), a, -1, 0, self.q, 0, 1)
            self.recv(h, '2m', a)
            self.send(h, ('2mf', a), a, 1, self.q, self.q, 0, -1)

    def last(self, a):
        for h in HALVES:
            self.recv(h, '2pf', a)
            self.recv(h, '2mf', a)

    def begin(self):
        q = self.q
        for h in HALVES:
            self.send(h, ('1p',), 0, 0, 0, 2 * q, 1, 0)
            self.send(h, ('1m',), 0, 0, 0, 2 * q, -1, 0)
        for h in HALVES:
            self.second(h, 0)
        for h in HALVES:
            self.recv(h, '1p')
            self.send(h, ('1pf',), -1, 0, 0, q, 1, 0)
            self.second(h, -1)
        for h in HALVES:
            self.recv(h, '1m')
            self.send(h, ('1mf',), 1, 0, q, q, -1, 0)
            self.second(h, 1)
        self.second_forward(0)

    def middle(self):
        for h in HALVES:
            self.recv(h, '1pf')
            self.recv(h, '1mf')
            self.second(h, 2)

    def run(self, hook=lambda first, n: None):
        self.begin()
        self.middle()
        hook(0, 5)
        self.second_forward(-1)
        self.second_forward(1)
        hook(5, 4)
        self.second_forward(2)
        self.last(0)
        hook(9, 2)
        self.last(-1)
        self.last(1)
        hook(11, 4)
        self.last(2)
        hook(15, 1)


class Scatter:
    def __init__(self, pos, m, part, recv_buf, rows, width):
        self.pos, self.m, self.part, self.recv_buf = pos, m, part, recv_buf
        self.rows, self.q = rows, width // 4
        self.places = {}

    def send(self, h, name, a, b, lo, n, ta, tb):
        key = ('rs', h) + name
        self.places[key] = sum(k for _, k in self.places.values()), n // self.q
        first = self.places[key][0]
        src = self.part.at[pl.ds(slot_of(*swap_if(1 - h, a, b)) * self.rows, self.rows), pl.ds(2 * self.q * h + lo, n)]
        dst = self.recv_buf.at[:, pl.ds(first * self.q, n)]
        self.m.start(key, src, dst, self.pos.dev(*swap_if(1 - h, ta, tb)))

    def recv_add(self, h, name, a, b, lo, n):
        key = ('rs', h) + name
        self.m.recv(key)
        there = pl.ds(self.places[key][0] * self.q, n)
        here = pl.ds(2 * self.q * h + lo, n)
        base = slot_of(*swap_if(1 - h, a, b)) * self.rows

        @pl.loop(0, self.rows // 16)
        def _(i):
            mine = pl.ds(pl.multiple_of(base + i * 16, 16), 16)
            theirs = pl.ds(pl.multiple_of(i * 16, 16), 16)
            self.part[mine, here] = self.part[mine, here] + self.recv_buf[theirs, there]

    def begin(self):
        q = self.q
        for b in (2, 1, -1, 0):
            for h in HALVES:
                self.send(h, ('1pf', b), 2, b, 0, q, 1, 0)
                self.send(h, ('1mf', b), 2, b, q, q, -1, 0)

    def finish(self):
        q = self.q
        order = (2, 1, -1, 0)
        for b in order:
            for h in HALVES:
                self.recv_add(h, ('1pf', b), 1, b, 0, q)
                self.send(h, ('1p', b), 1, b, 0, 2 * q, 1, 0)
                self.recv_add(h, ('1mf', b), -1, b, q, q)
                self.send(h, ('1m', b), -1, b, 0, 2 * q, -1, 0)
        for b in order:
            for h in HALVES:
                self.recv_add(h, ('1p', b), 0, b, 0, 2 * q)
                self.recv_add(h, ('1m', b), 0, b, 0, 2 * q)
                if b == 2:
                    self.send(h, ('2pf',), 0, 2, 0, q, 0, 1)
                    self.send(h, ('2mf',), 0, 2, q, q, 0, -1)
                if b == 1:
                    self.recv_add(h, ('2pf',), 0, 1, 0, q)
                    self.send(h, ('2p',), 0, 1, 0, 2 * q, 0, 1)
                if b == -1:
                    self.recv_add(h, ('2mf',), 0, -1, q, q)
                    self.send(h, ('2m',), 0, -1, 0, 2 * q, 0, -1)
                if b == 0:
                    self.recv_add(h, ('2p',), 0, 0, 0, 2 * q)
                    self.recv_add(h, ('2m',), 0, 0, 0, 2 * q)


def torus_neighbours(pos):
    return [pos.dev(0, 1), pos.dev(0, -1), pos.dev(1, 0), pos.dev(-1, 0)]


def offsets(side):
    return [(1, 1), (-1, -1), (1, -1), (-1, 1), (0, 1), (1, 0), (0, -1), (-1, 0),
            (2, 2), (0, 2), (2, 0), (1, 2), (-1, 2), (2, 1), (2, -1)]


def start_kernel(side, tok, wq, wgu, wo, table, tok_all, wq_all, wgu_all, wo_all, table_other,
                 t_send, t_recv, q_send, q_recv, g_send, g_recv, o_send, o_recv, f_send, f_recv, l_sem):
    pos = Place(side)
    offs = offsets(side)
    me_chip = pos.chip(0, 0)
    ff = wgu.shape[1] // 2
    ffb = ff // (side * side)
    barrier([pos.dev(dy, dx) for dy, dx in offs] + [pos.partner])

    def remote(src, dst, s, r, dev):
        return pltpu.make_async_remote_copy(src_ref=src, dst_ref=dst, send_sem=s, recv_sem=r,
                                            device_id={AXIS: dev}, device_id_type=MESH)

    toks, qs, gs, fs = [], [], [], []
    for i, (dy, dx) in enumerate(offs):
        cp = remote(tok, tok_all.at[me_chip], t_send.at[i], t_recv.at[i], pos.dev(dy, dx))
        cp.start()
        toks.append(cp)
    tcp = remote(table, table_other, f_send.at[0], f_recv.at[0], pos.partner)
    tcp.start()
    for i, (dy, dx) in enumerate(offs):
        cp = remote(wq.at[pos.chip(dy, dx)], wq_all.at[me_chip, pos.c], q_send.at[i], q_recv.at[i], pos.dev(dy, dx))
        cp.start()
        qs.append(cp)
    own = [pltpu.make_async_copy(tok, tok_all.at[me_chip], l_sem.at[0]),
           pltpu.make_async_copy(wq.at[me_chip], wq_all.at[me_chip, pos.c], l_sem.at[1]),
           pltpu.make_async_copy(wo, wo_all.at[me_chip, pos.c], l_sem.at[2])]
    for j in (0, 1):
        src = wgu.at[:, pl.ds(pl.multiple_of(j * ff + me_chip * ffb, 128), ffb)]
        own.append(pltpu.make_async_copy(src, wgu_all.at[me_chip, pos.c, :, pl.ds(j * ffb, ffb)], l_sem.at[3 + j]))
    for cp in own:
        cp.start()
    for i, (dy, dx) in enumerate(offs):
        for j in (0, 1):
            src = wgu.at[:, pl.ds(pl.multiple_of(j * ff + pos.chip(dy, dx) * ffb, 128), ffb)]
            cp = remote(src, wgu_all.at[me_chip, pos.c, :, pl.ds(j * ffb, ffb)],
                        g_send.at[2 * i + j], g_recv.at[2 * i + j], pos.dev(dy, dx))
            cp.start()
            gs.append(cp)
    for cp in own:
        cp.wait()

    def forward(k, ref):
        cp = remote(ref, ref, f_send.at[k], f_recv.at[k], pos.partner)
        cp.start()
        fs.append(cp)

    forward(1, wq_all.at[me_chip, pos.c])
    forward(2, wgu_all.at[me_chip, pos.c])
    forward(3, wo_all.at[me_chip, pos.c])
    for i, (dy, dx) in enumerate(offs):
        qs[i].wait_recv()
        forward(4 + i, wq_all.at[pos.chip(-dy, -dx), pos.c])
    m = Msgs(o_send, o_recv)
    torus_all_gather(pos, m, lambda p, lo, n: wo_all.at[p, pos.c, :, pl.ds(lo, n)], wo.shape[1])
    n = len(offs)
    for i, (dy, dx) in enumerate(offs):
        forward(4 + n + i, wo_all.at[pos.chip(-dy, -dx), pos.c])
    for i, (dy, dx) in enumerate(offs):
        gs[2 * i].wait_recv()
        gs[2 * i + 1].wait_recv()
        forward(4 + 2 * n + i, wgu_all.at[pos.chip(-dy, -dx), pos.c])
    for cp in toks:
        cp.wait()
    tcp.wait()
    for cp in qs + gs:
        cp.wait_send()
    m.drain()
    for cp in fs:
        cp.wait()


def embed_kernel(side, part_hbm, x_all, part, recv_buf, s1, r1, s2, r2, l_sem):
    pos = Place(side)
    barrier(torus_neighbours(pos))
    width = x_all.shape[2]
    loads = [pltpu.make_async_copy(part_hbm.at[i], part.at[i], l_sem.at[i]) for i in range(side * side)]
    for cp in loads:
        cp.start()
    for cp in loads:
        cp.wait()
    m = Msgs(s1, r1)
    torus_reduce_scatter(pos, m, part, recv_buf, width)
    me_chip = pos.chip(0, 0)
    x_all[me_chip] = part[me_chip]
    m2 = Msgs(s2, r2)
    torus_all_gather(pos, m2, lambda p, lo, n: x_all.at[p, :, pl.ds(lo, n)], width)
    m.drain()
    m2.drain()


def mlp_kernel(h_own, x_mid, wgu_hbm, wd_hbm, out, h_all, wgu, wd, act, part, recv_buf,
               s1, r1, s2, r2, w_send, w_recv, l_sem):
    pos = Place(4)
    f32, bf16 = jnp.float32, jnp.bfloat16
    rows, width = out.shape
    ffb = act.shape[1]
    half = ffb // 2
    tile = 256
    loads = [pltpu.make_async_copy(h_own, h_all.at[pl.ds(0, rows)], l_sem.at[0]),
             pltpu.make_async_copy(wgu_hbm, wgu, l_sem.at[1]),
             pltpu.make_async_copy(wd_hbm, wd.at[pos.c], l_sem.at[2])]
    for cp in loads:
        cp.start()
    barrier(torus_neighbours(pos) + [pos.partner])
    push = pltpu.make_async_remote_copy(src_ref=wd_hbm, dst_ref=wd.at[pos.c], send_sem=w_send.at[0], recv_sem=w_recv.at[0],
                                        device_id={AXIS: pos.partner}, device_id_type=MESH)
    push.start()
    loads[0].wait()
    waited = []

    def gate_up(first, n):
        if not waited:
            loads[1].wait()
            waited.append(True)
        mine = pl.ds(first * rows, n * rows)

        @pl.loop(0, ffb // tile)
        def _(i):
            lo = pl.multiple_of(i * tile, tile)
            h = h_all[mine, :]
            g = jnp.dot(h, wgu[:, :, :, pl.ds(lo, tile)].reshape(width, tile), preferred_element_type=f32)
            u = jnp.dot(h, wgu[:, :, :, pl.ds(pl.multiple_of(ffb + lo, tile), tile)].reshape(width, tile),
                        preferred_element_type=f32)
            act[mine, pl.ds(lo, tile)] = (jax.nn.silu(g) * u).astype(bf16)

    def down(first, n):
        mine = pl.ds(first * rows, n * rows)

        @pl.loop(0, width // tile)
        def _(i):
            cols = pl.ds(pl.multiple_of(i * tile, tile), tile)
            part[mine, cols] = jnp.dot(act[mine, :], wd[:, :, cols].reshape(2 * half, tile), preferred_element_type=f32)

    m = Msgs(s1, r1)
    Gather(pos, m, lambda s, lo, n: h_all.at[pl.ds(s * rows, rows), pl.ds(lo, n)], width).run(gate_up)
    loads[2].wait()
    push.wait()
    m2 = Msgs(s2, r2)
    scatter = Scatter(pos, m2, part, recv_buf, rows, width)
    down(9, 7)
    scatter.begin()
    down(0, 9)
    scatter.finish()
    out[...] = (x_mid[...].astype(f32) + part[pl.ds(0, rows), :]).astype(bf16)
    m.drain()
    m2.drain()


def exchange_kernel(side, src, dst, sems, recvs, l_sem):
    pos = Place(side)
    offs = offsets(side)
    me_chip = pos.chip(0, 0)
    barrier([pos.dev(dy, dx) for dy, dx in offs])
    copies = []
    for i, (dy, dx) in enumerate(offs):
        cp = pltpu.make_async_remote_copy(
            src_ref=src.at[pos.chip(dy, dx)], dst_ref=dst.at[me_chip], send_sem=sems.at[i], recv_sem=recvs.at[i],
            device_id={AXIS: pos.dev(dy, dx)}, device_id_type=MESH)
        cp.start()
        copies.append(cp)
    own = pltpu.make_async_copy(src.at[me_chip], dst.at[me_chip], l_sem.at[0])
    own.start()
    own.wait()
    for cp in copies:
        cp.wait()


def dma(n):
    return pltpu.SemaphoreType.DMA((n,))


def params(cid):
    return pltpu.CompilerParams(collective_id=cid, has_side_effects=True, vmem_limit_bytes=VMEM_LIMIT)


def rms_norm(hidden, gain):
    h_f32 = hidden.astype(jnp.float32)
    inv_rms = lax.rsqrt(jnp.mean(h_f32 * h_f32, axis=-1, keepdims=True) + NORM_EPS)
    return (h_f32 * inv_rms * gain.astype(jnp.float32)).astype(jnp.bfloat16)


def apply_rope(proj, rope_scale):
    seq_len = proj.shape[1]
    head_dim = proj.shape[-1]
    half_dim = head_dim // 2
    freq_expo = jnp.arange(half_dim, dtype=jnp.float32) * (2.0 / head_dim)
    inv_freq = 1.0 / (rope_scale * jnp.power(ROPE_THETA, freq_expo))
    angles = jnp.arange(seq_len, dtype=jnp.float32)[:, None] * inv_freq[None, :]
    cos_tab = jnp.cos(angles)[:, None, :]
    sin_tab = jnp.sin(angles)[:, None, :]
    low_half = proj[..., :half_dim]
    high_half = proj[..., half_dim:]
    return jnp.concatenate([low_half * cos_tab - high_half * sin_tab, high_half * cos_tab + low_half * sin_tab], axis=-1)


def solution(mesh):
    batch_axes = ('dp', AXIS)
    row_spec = P(AXIS, None)
    n_dev = mesh.shape[AXIS]
    chips = n_dev // 2
    side = math.isqrt(chips)
    n_off = chips - 1

    def device_step(tokens, embed_table, norm_attn, w_qkv, w_out, norm_mlp, w_gate_up, w_down, rope_scale):
        f32, bf16 = jnp.float32, jnp.bfloat16
        seq = tokens.shape[1]
        rows, d_model = w_out.shape
        rows_table = embed_table.shape[0]
        head_dim = 2 * rope_scale.shape[0]
        q_width = rows * n_dev
        kv_width = (w_qkv.shape[1] - q_width) // 2
        heads = q_width // head_dim // chips
        kv_heads = kv_width // head_dim // chips
        qb, kb = heads * head_dim, kv_heads * head_dim
        width = qb + 2 * kb
        pad_width = -(-(width + 2) // 128) * 128
        ff = w_gate_up.shape[1] // 2
        ffb = ff // chips
        me = lax.axis_index(AXIS)
        rest = jnp.zeros((chips, rows, pad_width - width - 2), bf16)
        wq_blocks = jnp.concatenate([
            w_qkv[:, :q_width].reshape(rows, chips, qb).transpose(1, 0, 2),
            w_qkv[:, q_width:q_width + kv_width].reshape(rows, chips, kb).transpose(1, 0, 2),
            w_qkv[:, q_width + kv_width:].reshape(rows, chips, kb).transpose(1, 0, 2),
            jnp.broadcast_to(norm_attn[None, :, None], (chips, rows, 1)),
            jnp.broadcast_to(norm_mlp[None, :, None], (chips, rows, 1)), rest], axis=-1)

        tok_all, wq_all, wgu_all, wo_all, table_other = pl.pallas_call(
            functools.partial(start_kernel, side), name='start',
            out_shape=(jax.ShapeDtypeStruct((chips, 1, seq), jnp.int32),
                       jax.ShapeDtypeStruct((chips, 2, rows, pad_width), bf16),
                       jax.ShapeDtypeStruct((chips, 2, rows, 2 * ffb), bf16),
                       jax.ShapeDtypeStruct((chips, 2, rows, d_model), bf16),
                       jax.ShapeDtypeStruct((rows_table, d_model), bf16)),
            in_specs=[ANY] * 5, out_specs=(ANY,) * 5,
            scratch_shapes=[dma(n_off), dma(n_off), dma(n_off), dma(n_off), dma(2 * n_off), dma(2 * n_off),
                            dma(AG_MSGS), dma(AG_MSGS), dma(4 + 3 * n_off), dma(4 + 3 * n_off), dma(5)],
            compiler_params=params(1),
        )(tokens, wq_blocks, w_gate_up, w_out, embed_table)

        gains = wq_all[..., width:width + 2].reshape(d_model, 2)
        gain_attn, gain_mlp = gains[:, 0], gains[:, 1]
        wq_own = wq_all.reshape(d_model, pad_width)
        wo_full = wo_all.reshape(q_width, d_model)

        ids = tok_all.reshape(chips * seq)
        row_ids = jnp.arange(rows_table, dtype=jnp.int32)

        def pick(device, table):
            hot = ((ids - device * rows_table)[:, None] == row_ids[None, :]).astype(bf16)
            return jnp.dot(hot, table, preferred_element_type=f32)

        part = (pick(me, embed_table) + pick(me + 1 - 2 * lax.rem(me, 2), table_other)).astype(bf16)
        part = part.reshape(chips, seq, d_model)

        x_all = pl.pallas_call(
            functools.partial(embed_kernel, side), name='embed',
            out_shape=jax.ShapeDtypeStruct((chips, seq, d_model), bf16),
            in_specs=[ANY], out_specs=pl.BlockSpec(memory_space=pltpu.VMEM),
            scratch_shapes=[pltpu.VMEM((chips, seq, d_model), bf16),
                            pltpu.VMEM((seq, d_model * n_off), bf16),
                            dma(RS_MSGS), dma(RS_MSGS), dma(AG_MSGS), dma(AG_MSGS), dma(chips)],
            compiler_params=params(2),
        )(part)
        chip = lax.div(me, 2)
        x_own = lax.dynamic_index_in_dim(x_all, chip, 0, keepdims=False)

        normed = rms_norm(x_all.reshape(chips * seq, d_model), gain_attn)
        proj = jnp.dot(normed, wq_own, preferred_element_type=f32)[:, :width].reshape(chips, seq, width)
        query = apply_rope(proj[..., :qb].reshape(chips, seq, heads, head_dim), rope_scale).astype(bf16)
        key = apply_rope(proj[..., qb:qb + kb].reshape(chips, seq, kv_heads, head_dim), rope_scale).astype(bf16)
        value = proj[..., qb + kb:].astype(bf16).reshape(chips, seq, kv_heads, head_dim)
        q_grouped = query.reshape(chips, seq, kv_heads, heads // kv_heads, head_dim)
        scores = jnp.einsum('bqkgd,bskd->bkgqs', q_grouped, key, preferred_element_type=f32) * (head_dim ** -0.5)
        causal = jnp.arange(seq)[:, None] >= jnp.arange(seq)[None, :]
        scores = jnp.where(causal, scores, -jnp.inf)
        scores = scores - jnp.max(scores, axis=-1, keepdims=True)
        weights = jnp.exp(scores)
        probs = (weights / jnp.sum(weights, axis=-1, keepdims=True)).astype(bf16)
        context = jnp.einsum('bkgqs,bskd->bqkgd', probs, value, preferred_element_type=f32).astype(bf16)
        context = context.reshape(chips, seq, qb)
        packed = jnp.concatenate([context, key.reshape(chips, seq, kb), value.reshape(chips, seq, kb)], axis=-1)

        mine = pl.pallas_call(
            functools.partial(exchange_kernel, side), name='to_sequences',
            out_shape=jax.ShapeDtypeStruct((chips, seq, width), bf16),
            in_specs=[ANY], out_specs=ANY,
            scratch_shapes=[dma(n_off), dma(n_off), dma(1)],
            compiler_params=params(3),
        )(packed)
        ctx_own = mine[..., :qb].transpose(1, 0, 2).reshape(seq, q_width)
        key_own = mine[..., qb:qb + kb].reshape(chips, seq, kv_heads, head_dim).transpose(1, 0, 2, 3)
        val_own = mine[..., qb + kb:].reshape(chips, seq, kv_heads, head_dim).transpose(1, 0, 2, 3)
        key_own = key_own.reshape(1, seq, chips * kv_heads, head_dim)
        val_own = val_own.reshape(1, seq, chips * kv_heads, head_dim)

        attn_proj = jnp.dot(ctx_own, wo_full, preferred_element_type=f32)
        x_mid = (x_own.astype(f32) + attn_proj).astype(bf16)
        normed_mlp = rms_norm(x_mid, gain_mlp)

        vmem = pl.BlockSpec(memory_space=pltpu.VMEM)
        layer_out = pl.pallas_call(
            mlp_kernel, name='mlp',
            out_shape=jax.ShapeDtypeStruct((seq, d_model), bf16),
            in_specs=[ANY, vmem, ANY, ANY], out_specs=vmem,
            scratch_shapes=[pltpu.VMEM((chips * seq, d_model), bf16),
                            pltpu.VMEM((chips, 2, rows, 2 * ffb), bf16),
                            pltpu.VMEM((2, ffb // 2, d_model), bf16),
                            pltpu.VMEM((chips * seq, ffb), bf16),
                            pltpu.VMEM((chips * seq, d_model), f32),
                            pltpu.VMEM((seq, d_model * n_off), f32),
                            dma(AG_MSGS), dma(AG_MSGS), dma(RS_MSGS), dma(RS_MSGS), dma(1), dma(1), dma(3)],
            compiler_params=params(4),
        )(normed_mlp, x_mid, wgu_all, w_down)
        return layer_out[None], key_own, val_own

    return jax.shard_map(
        device_step,
        mesh=mesh,
        in_specs=(P(batch_axes, None), row_spec, P(AXIS), row_spec, row_spec, P(AXIS), row_spec, row_spec, P(None)),
        out_specs=(P(batch_axes, None, None), P(batch_axes, None, None, None), P(batch_axes, None, None, None)),
        check_vma=False,
    )
```

```python
import jax
import jax.numpy as jnp
from jax import lax
from jax.experimental import pallas as pl
from jax.experimental.pallas import tpu as pltpu
from jax.sharding import PartitionSpec as P

NORM_EPS = 1e-5
ROPE_THETA = 10000.0
AXIS = 'fsdp'
MESH = pl.DeviceIdType.MESH
ANY = pl.BlockSpec(memory_space=pl.ANY)
VMEM_LIMIT = 60 * 1024 * 1024


class Place:
    def __init__(self, side):
        me = lax.axis_index(AXIS)
        self.side = side
        self.c = lax.rem(me, 2)
        chip = lax.div(me, 2)
        self.y = lax.div(chip, side)
        self.x = lax.rem(chip, side)
        self.me = me
        self.partner = me + 1 - 2 * self.c

    def chip(self, dy, dx):
        s = self.side
        return lax.rem(self.y + dy + s, s) * s + lax.rem(self.x + dx + s, s)

    def dev(self, dy, dx):
        return self.chip(dy, dx) * 2 + self.c


def barrier(devices):
    sem = pltpu.get_barrier_semaphore()
    for d in devices:
        pl.semaphore_signal(sem, inc=1, device_id={AXIS: d}, device_id_type=MESH)
    pl.semaphore_wait(sem, len(devices))


class Msgs:
    def __init__(self, send_sem, recv_sem):
        self.send_sem, self.recv_sem = send_sem, recv_sem
        self.index, self.copies = {}, []

    def start(self, name, src, dst, dev):
        i = len(self.copies)
        self.index[name] = i
        copy = pltpu.make_async_remote_copy(
            src_ref=src, dst_ref=dst, send_sem=self.send_sem.at[i], recv_sem=self.recv_sem.at[i],
            device_id={AXIS: dev}, device_id_type=MESH)
        copy.start()
        self.copies.append(copy)

    def recv(self, name):
        self.copies[self.index[name]].wait_recv()

    def drain(self):
        for copy in self.copies:
            copy.wait_send()


AG_MSGS = 40
RS_MSGS = 40


SLOTS = ((0, 0), (0, 1), (0, -1), (1, 0), (-1, 0), (1, 1), (1, -1), (-1, 1), (-1, -1),
         (2, 0), (0, 2), (2, 1), (2, -1), (1, 2), (-1, 2), (2, 2))


def slot_of(a, b):
    return SLOTS.index(((a + 1) % 4 - 1, (b + 1) % 4 - 1))


def swap_if(h, a, b):
    return (b, a) if h == 0 else (a, b)


HALVES = (0, 1)


class Gather:
    def __init__(self, pos, m, blk, width, by_chip=False):
        self.pos, self.m, self.blk, self.q, self.by_chip = pos, m, blk, width // 4, by_chip

    def send(self, h, name, a, b, lo, n, ta, tb):
        lo = 2 * self.q * h + lo
        if self.by_chip:
            src = dst = self.blk(self.pos.chip(*swap_if(h, a, b)), lo, n)
        else:
            src = self.blk(slot_of(*swap_if(h, a, b)), lo, n)
            dst = self.blk(slot_of(*swap_if(h, a - ta, b - tb)), lo, n)
        self.m.start(('ag', h) + name, src, dst, self.pos.dev(*swap_if(h, ta, tb)))

    def recv(self, h, *name):
        self.m.recv(('ag', h) + name)

    def second(self, h, a):
        self.send(h, ('2p', a), a, 0, 0, 2 * self.q, 0, 1)
        self.send(h, ('2m', a), a, 0, 0, 2 * self.q, 0, -1)

    def second_forward(self, a):
        for h in HALVES:
            self.recv(h, '2p', a)
            self.send(h, ('2pf', a), a, -1, 0, self.q, 0, 1)
            self.recv(h, '2m', a)
            self.send(h, ('2mf', a), a, 1, self.q, self.q, 0, -1)

    def last(self, a):
        for h in HALVES:
            self.recv(h, '2pf', a)
            self.recv(h, '2mf', a)

    def begin(self):
        q = self.q
        for h in HALVES:
            self.send(h, ('1p',), 0, 0, 0, 2 * q, 1, 0)
            self.send(h, ('1m',), 0, 0, 0, 2 * q, -1, 0)
        for h in HALVES:
            self.second(h, 0)
        for h in HALVES:
            self.recv(h, '1p')
            self.send(h, ('1pf',), -1, 0, 0, q, 1, 0)
            self.second(h, -1)
        for h in HALVES:
            self.recv(h, '1m')
            self.send(h, ('1mf',), 1, 0, q, q, -1, 0)
            self.second(h, 1)
        self.second_forward(0)

    def middle(self):
        for h in HALVES:
            self.recv(h, '1pf')
            self.recv(h, '1mf')
            self.second(h, 2)

    def run(self, hook=lambda first, n: None):
        self.begin()
        self.rest(hook)

    def rest(self, hook, before_last=lambda: None):
        self.middle()
        hook(0, 5)
        self.second_forward(-1)
        self.second_forward(1)
        hook(5, 4)
        self.second_forward(2)
        before_last()
        self.last(0)
        hook(9, 2)
        self.last(-1)
        self.last(1)
        hook(11, 4)
        self.last(2)
        hook(15, 1)


class Scatter:
    def __init__(self, pos, m, part, recv_buf, rows, width):
        self.pos, self.m, self.part, self.recv_buf = pos, m, part, recv_buf
        self.rows, self.q = rows, width // 4
        self.places = {}

    def send(self, h, name, a, b, lo, n, ta, tb):
        key = ('rs', h) + name
        self.places[key] = sum(k for _, k in self.places.values()), n // self.q
        first = self.places[key][0]
        src = self.part.at[pl.ds(slot_of(*swap_if(1 - h, a, b)) * self.rows, self.rows), pl.ds(2 * self.q * h + lo, n)]
        dst = self.recv_buf.at[:, pl.ds(first * self.q, n)]
        self.m.start(key, src, dst, self.pos.dev(*swap_if(1 - h, ta, tb)))

    def recv_add(self, h, name, a, b, lo, n):
        key = ('rs', h) + name
        self.m.recv(key)
        there = pl.ds(self.places[key][0] * self.q, n)
        here = pl.ds(2 * self.q * h + lo, n)
        base = slot_of(*swap_if(1 - h, a, b)) * self.rows

        @pl.loop(0, self.rows // 16)
        def _(i):
            mine = pl.ds(pl.multiple_of(base + i * 16, 16), 16)
            theirs = pl.ds(pl.multiple_of(i * 16, 16), 16)
            self.part[mine, here] = self.part[mine, here] + self.recv_buf[theirs, there]

    def begin(self):
        q = self.q
        for b in (2, 1, -1, 0):
            for h in HALVES:
                self.send(h, ('1pf', b), 2, b, 0, q, 1, 0)
                self.send(h, ('1mf', b), 2, b, q, q, -1, 0)

    def finish(self, hook=lambda i: None):
        q = self.q
        order = (2, 1, -1, 0)
        calls = iter(range(16))
        for b in order:
            for h in HALVES:
                self.recv_add(h, ('1pf', b), 1, b, 0, q)
                self.send(h, ('1p', b), 1, b, 0, 2 * q, 1, 0)
                self.recv_add(h, ('1mf', b), -1, b, q, q)
                self.send(h, ('1m', b), -1, b, 0, 2 * q, -1, 0)
                hook(next(calls))
        for b in order:
            for h in HALVES:
                self.recv_add(h, ('1p', b), 0, b, 0, 2 * q)
                self.recv_add(h, ('1m', b), 0, b, 0, 2 * q)
                if b == 2:
                    self.send(h, ('2pf',), 0, 2, 0, q, 0, 1)
                    self.send(h, ('2mf',), 0, 2, q, q, 0, -1)
                if b == 1:
                    self.recv_add(h, ('2pf',), 0, 1, 0, q)
                    self.send(h, ('2p',), 0, 1, 0, 2 * q, 0, 1)
                if b == -1:
                    self.recv_add(h, ('2mf',), 0, -1, q, q)
                    self.send(h, ('2m',), 0, -1, 0, 2 * q, 0, -1)
                if b == 0:
                    self.recv_add(h, ('2p',), 0, 0, 0, 2 * q)
                    self.recv_add(h, ('2m',), 0, 0, 0, 2 * q)
                hook(next(calls))


def torus_neighbours(pos):
    return [pos.dev(0, 1), pos.dev(0, -1), pos.dev(1, 0), pos.dev(-1, 0)]


def offsets(side):
    return [(1, 1), (-1, -1), (1, -1), (-1, 1), (0, 1), (1, 0), (0, -1), (-1, 0),
            (2, 2), (0, 2), (2, 0), (1, 2), (-1, 2), (2, 1), (2, -1)]


def remote(src, dst, sems, i, dev):
    return pltpu.make_async_remote_copy(src_ref=src, dst_ref=dst, send_sem=sems.at[0, i], recv_sem=sems.at[1, i],
                                        device_id={AXIS: dev}, device_id_type=MESH)


def front_kernel(tok, gains, wqkv, cos2, sin2, wgu, wo, table,
                 x_own, mine, wgu_all, wo_all, gain_rows,
                 tok_all, tok_col, tbl, hot, part, recv_buf, x_all, wq_out, wq, normed, proj, packed,
                 t_sem, q_sem, qf_sem, g_sem, gf_sem, o_sem, of_sem, r_sem, a_sem, e_sem, l_sem):
    f32, bf16 = jnp.float32, jnp.bfloat16
    pos = Place(4)
    offs = offsets(4)
    here = pos.chip(0, 0)
    rows, lanes = wq_out.shape[1], 128
    seq, width = x_own.shape
    n_slots = len(SLOTS)
    n_off = len(offs)
    ff = wgu.shape[1] // 2
    ffb = ff // n_slots
    head_dim = wqkv.shape[1] // (6 * n_slots)
    table_rows = table.shape[0]
    tile = 256
    loads = [pltpu.make_async_copy(table, tbl.at[pos.c], l_sem.at[0]),
             pltpu.make_async_copy(tok, tok_all.at[0], l_sem.at[1]),
             pltpu.make_async_copy(wo, wo_all.at[here, pos.c], l_sem.at[2])]
    for j in (0, 1):
        src = wgu.at[:, pl.ds(pl.multiple_of(j * ff + here * ffb, 128), ffb)]
        loads.append(pltpu.make_async_copy(src, wgu_all.at[here, pos.c, :, pl.ds(j * ffb, ffb)], l_sem.at[3 + j]))
    for cp in loads:
        cp.start()
    barrier([pos.dev(dy, dx) for dy, dx in offs] + [pos.partner])

    toks = [remote(tok, tok_all.at[slot_of(-dy, -dx)], t_sem, i, pos.dev(dy, dx)) for i, (dy, dx) in enumerate(offs)]
    for cp in toks:
        cp.start()
    swap = remote(table, tbl.at[pos.c], t_sem, n_off, pos.partner)
    swap.start()

    for p in range(n_slots):
        for k in range(6):
            j, hd = k // 2, k % 2
            lo = (j * 2 * n_slots + p * 2 + hd) * head_dim
            block = jnp.concatenate([wqkv[:, lo:lo + head_dim], jnp.zeros((rows, lanes - head_dim), bf16)], axis=1)
            if k == 4:
                block = block + gains[...]
            wq_out[p, :, k * lanes:(k + 1) * lanes] = block
    my_rows = pl.ds(pl.multiple_of(pos.me * rows, 32), rows)
    qs = [remote(wq_out.at[pos.chip(dy, dx)], wq.at[my_rows], q_sem, i, pos.dev(dy, dx)) for i, (dy, dx) in enumerate(offs)]
    for cp in qs:
        cp.start()
    wq[my_rows, :] = wq_out[here]

    loads[1].wait()
    for i, (dy, dx) in enumerate(offs):
        toks[i].wait_recv()
    for s in range(n_slots):
        column = jnp.transpose(tok_all[s].astype(f32))
        tok_col[pl.ds(s * seq, seq), :] = column[:seq, 0:1]
    loads[0].wait()
    swap.wait_recv()
    group = hot.shape[1]
    for g in range(n_slots * seq // group):
        mine_rows = pl.ds(g * group, group)
        for cc in (0, 1):
            ids = lax.broadcasted_iota(jnp.int32, (group, table_rows), 1) + (here * 2 + cc) * table_rows
            hot[cc] = jnp.where(tok_col[mine_rows, :] == ids.astype(f32), 1.0, 0.0).astype(bf16)

        @pl.loop(0, width // tile)
        def _(i):
            cols = pl.ds(pl.multiple_of(i * tile, tile), tile)
            total = (jnp.dot(hot[0], tbl[0, :, cols], preferred_element_type=f32)
                     + jnp.dot(hot[1], tbl[1, :, cols], preferred_element_type=f32))
            part[mine_rows, cols] = total.astype(bf16)

    m = Msgs(r_sem.at[0], r_sem.at[1])
    scatter = Scatter(pos, m, part, recv_buf, seq, width)
    scatter.begin()

    fwd = []

    def forward(sems, i, ref):
        cp = remote(ref, ref, sems, i, pos.partner)
        cp.start()
        fwd.append(cp)
        return cp

    q_fwd = [forward(qf_sem, n_off, wq.at[my_rows])]
    for i, (dy, dx) in enumerate(offs):
        qs[i].wait_recv()
        q_fwd.append(forward(qf_sem, i, wq.at[pl.ds(pl.multiple_of(pos.dev(-dy, -dx) * rows, 32), rows)]))
    for cp in q_fwd:
        cp.wait_recv()
    for k in range(width // lanes):
        square = jnp.transpose(wq[pl.ds(k * lanes, lanes), 4 * lanes:5 * lanes].astype(f32))
        gain_rows[:, k * lanes:(k + 1) * lanes] = square[head_dim:head_dim + 8, :]

    gs = []
    for i, (dy, dx) in enumerate(offs):
        for j in (0, 1):
            src = wgu.at[:, pl.ds(pl.multiple_of(j * ff + pos.chip(dy, dx) * ffb, 128), ffb)]
            gs.append(remote(src, wgu_all.at[here, pos.c, :, pl.ds(j * ffb, ffb)], g_sem, 2 * i + j, pos.dev(dy, dx)))

    def send_gate_up(i):
        for cp in gs[2 * i:2 * i + 2]:
            cp.start()

    scatter.finish(send_gate_up)
    x_all[pl.ds(0, seq), :] = part[pl.ds(0, seq), :]
    x_own[...] = part[pl.ds(0, seq), :]

    sends = []

    def attend(first, n):
        base = first * seq

        @pl.loop(0, n * seq // 16)
        def _(i):
            x = x_all[pl.ds(pl.multiple_of(base + i * 16, 16), 16), :].astype(f32)
            inv = lax.rsqrt(jnp.mean(x * x, axis=-1, keepdims=True) + NORM_EPS)
            normed[pl.ds(pl.multiple_of(i * 16, 16), 16), :] = (x * inv * gain_rows[0:1, :]).astype(bf16)

        @pl.loop(0, 3)
        def _(i):
            cols = pl.ds(pl.multiple_of(i * tile, tile), tile)
            proj[pl.ds(0, n * seq), cols] = jnp.dot(normed[pl.ds(0, n * seq), :], wq[:, cols], preferred_element_type=f32)

        lane = lax.broadcasted_iota(jnp.int32, (seq, lanes), 1)
        causal = lax.broadcasted_iota(jnp.int32, (seq, seq), 0) >= lax.broadcasted_iota(jnp.int32, (seq, seq), 1)

        def rope(u):
            other = jnp.where(lane < head_dim // 2, pltpu.roll(u, lanes - head_dim // 2, 1), pltpu.roll(u, head_dim // 2, 1))
            return (u * cos2[...] + other * sin2[...]).astype(bf16)

        @pl.loop(0, n)
        def _(s):
            mine_rows = pl.ds(pl.multiple_of(s * seq, seq), seq)
            for hd in (0, 1):
                q = rope(proj[mine_rows, hd * lanes:(hd + 1) * lanes])
                k = rope(proj[mine_rows, (2 + hd) * lanes:(3 + hd) * lanes])
                v = proj[mine_rows, (4 + hd) * lanes:(5 + hd) * lanes].astype(bf16)
                scores = lax.dot_general(q, k, (((1,), (1,)), ((), ())), preferred_element_type=f32) * (head_dim ** -0.5)
                scores = jnp.where(causal, scores, -jnp.inf)
                e = jnp.exp(scores - jnp.max(scores, axis=-1, keepdims=True))
                probs = (e / jnp.sum(e, axis=-1, keepdims=True)).astype(bf16)
                context = jnp.dot(probs, v, preferred_element_type=f32).astype(bf16)
                packed[first + s, :, hd * lanes:(hd + 1) * lanes] = context
                packed[first + s, :, (2 + hd) * lanes:(3 + hd) * lanes] = k
                packed[first + s, :, (4 + hd) * lanes:(5 + hd) * lanes] = v

        for s in range(first, first + n):
            if s == 0:
                cp = pltpu.make_async_copy(packed.at[0], mine.at[here], l_sem.at[5])
            else:
                cp = remote(packed.at[s], mine.at[here], e_sem, s - 1, pos.dev(*SLOTS[s]))
            cp.start()
            sends.append(cp)

    m2 = Msgs(a_sem.at[0], a_sem.at[1])
    gather = Gather(pos, m2, lambda s, lo, n: x_all.at[pl.ds(s * seq, seq), pl.ds(lo, n)], width)
    m3 = Msgs(o_sem.at[0], o_sem.at[1])
    out_gather = Gather(pos, m3, lambda p, lo, n: wo_all.at[p, pos.c, :, pl.ds(lo, n)], width, by_chip=True)
    for cp in loads[2:]:
        cp.wait()
    forward(gf_sem, n_off, wgu_all.at[here, pos.c])
    gather.begin()
    gather.rest(attend, out_gather.begin)

    def forward_out(first, n):
        for s in range(first, first + n):
            forward(of_sem, s, wo_all.at[pos.chip(*SLOTS[s]), pos.c])

    for i, (dy, dx) in enumerate(offs):
        gs[2 * i].wait_recv()
        gs[2 * i + 1].wait_recv()
        forward(gf_sem, i, wgu_all.at[pos.chip(-dy, -dx), pos.c])
    out_gather.rest(forward_out)
    for cp in sends:
        cp.wait()
    for cp in toks + qs + gs + [swap]:
        cp.wait_send()
    for cp in fwd[:1 + n_off]:
        cp.wait_send()
    for cp in fwd[1 + n_off:]:
        cp.wait()
    for msgs in (m, m2, m3):
        msgs.drain()


def mlp_kernel(h_own, x_mid, wgu_hbm, wd_hbm, out, h_all, wgu, wd, act, part, recv_buf,
               s1, r1, s2, r2, w_send, w_recv, l_sem):
    pos = Place(4)
    f32, bf16 = jnp.float32, jnp.bfloat16
    rows, width = out.shape
    ffb = act.shape[1]
    half = ffb // 2
    tile = 256
    loads = [pltpu.make_async_copy(h_own, h_all.at[pl.ds(0, rows)], l_sem.at[0]),
             pltpu.make_async_copy(wgu_hbm, wgu, l_sem.at[1]),
             pltpu.make_async_copy(wd_hbm, wd.at[pos.c], l_sem.at[2])]
    for cp in loads:
        cp.start()
    barrier(torus_neighbours(pos) + [pos.partner])
    push = pltpu.make_async_remote_copy(src_ref=wd_hbm, dst_ref=wd.at[pos.c], send_sem=w_send.at[0], recv_sem=w_recv.at[0],
                                        device_id={AXIS: pos.partner}, device_id_type=MESH)
    push.start()
    loads[0].wait()
    waited = []

    def gate_up(first, n):
        if not waited:
            loads[1].wait()
            waited.append(True)
        mine = pl.ds(first * rows, n * rows)

        @pl.loop(0, ffb // tile)
        def _(i):
            lo = pl.multiple_of(i * tile, tile)
            h = h_all[mine, :]
            g = jnp.dot(h, wgu[:, :, :, pl.ds(lo, tile)].reshape(width, tile), preferred_element_type=f32)
            u = jnp.dot(h, wgu[:, :, :, pl.ds(pl.multiple_of(ffb + lo, tile), tile)].reshape(width, tile),
                        preferred_element_type=f32)
            act[mine, pl.ds(lo, tile)] = (jax.nn.silu(g) * u).astype(bf16)

    def down(first, n):
        mine = pl.ds(first * rows, n * rows)

        @pl.loop(0, width // tile)
        def _(i):
            cols = pl.ds(pl.multiple_of(i * tile, tile), tile)
            part[mine, cols] = jnp.dot(act[mine, :], wd[:, :, cols].reshape(2 * half, tile), preferred_element_type=f32)

    m = Msgs(s1, r1)
    Gather(pos, m, lambda s, lo, n: h_all.at[pl.ds(s * rows, rows), pl.ds(lo, n)], width).run(gate_up)
    loads[2].wait()
    push.wait()
    m2 = Msgs(s2, r2)
    scatter = Scatter(pos, m2, part, recv_buf, rows, width)
    down(9, 7)
    scatter.begin()
    down(0, 9)
    scatter.finish()
    out[...] = (x_mid[...].astype(f32) + part[pl.ds(0, rows), :]).astype(bf16)
    m.drain()
    m2.drain()


def exchange_kernel(side, src, dst, sems, recvs, l_sem):
    pos = Place(side)
    offs = offsets(side)
    me_chip = pos.chip(0, 0)
    barrier([pos.dev(dy, dx) for dy, dx in offs])
    copies = []
    for i, (dy, dx) in enumerate(offs):
        cp = pltpu.make_async_remote_copy(
            src_ref=src.at[pos.chip(dy, dx)], dst_ref=dst.at[me_chip], send_sem=sems.at[i], recv_sem=recvs.at[i],
            device_id={AXIS: pos.dev(dy, dx)}, device_id_type=MESH)
        cp.start()
        copies.append(cp)
    own = pltpu.make_async_copy(src.at[me_chip], dst.at[me_chip], l_sem.at[0])
    own.start()
    own.wait()
    for cp in copies:
        cp.wait()


def dma(n):
    return pltpu.SemaphoreType.DMA((n,))


def dma2(n):
    return pltpu.SemaphoreType.DMA((2, n))


def params(cid):
    return pltpu.CompilerParams(collective_id=cid, has_side_effects=True, vmem_limit_bytes=VMEM_LIMIT)


def rms_norm(hidden, gain):
    h_f32 = hidden.astype(jnp.float32)
    inv_rms = lax.rsqrt(jnp.mean(h_f32 * h_f32, axis=-1, keepdims=True) + NORM_EPS)
    return (h_f32 * inv_rms * gain.astype(jnp.float32)).astype(jnp.bfloat16)


def rope_tables(rope_scale, seq_len, lanes):
    half_dim = rope_scale.shape[0]
    freq_expo = jnp.arange(half_dim, dtype=jnp.float32) * (2.0 / (2 * half_dim))
    inv_freq = 1.0 / (rope_scale * jnp.power(ROPE_THETA, freq_expo))
    angles = jnp.arange(seq_len, dtype=jnp.float32)[:, None] * inv_freq[None, :]
    cos, sin = jnp.cos(angles), jnp.sin(angles)
    rest = jnp.zeros((seq_len, lanes - 2 * half_dim), jnp.float32)
    return jnp.concatenate([cos, cos, rest], axis=1), jnp.concatenate([-sin, sin, rest], axis=1)


def solution(mesh):
    batch_axes = ('dp', AXIS)
    row_spec = P(AXIS, None)
    n_dev = mesh.shape[AXIS]
    chips = n_dev // 2
    n_off = chips - 1

    def device_step(tokens, embed_table, norm_attn, w_qkv, w_out, norm_mlp, w_gate_up, w_down, rope_scale):
        f32, bf16 = jnp.float32, jnp.bfloat16
        seq = tokens.shape[1]
        rows, d_model = w_out.shape
        head_dim = 2 * rope_scale.shape[0]
        q_width = rows * n_dev
        ff = w_gate_up.shape[1] // 2
        ffb = ff // chips
        lanes = 128
        tok = jnp.zeros((8, lanes), jnp.int32) + jnp.pad(tokens, ((0, 0), (0, lanes - seq)))
        column = lax.broadcasted_iota(jnp.int32, (rows, lanes), 1)
        gains = (jnp.where(column == head_dim, norm_attn[:, None], 0)
                 + jnp.where(column == head_dim + 1, norm_mlp[:, None], 0)).astype(bf16)
        cos2, sin2 = rope_tables(rope_scale, seq, lanes)
        vmem = pl.BlockSpec(memory_space=pltpu.VMEM)

        x_own, mine, wgu_all, wo_all, gain_rows = pl.pallas_call(
            front_kernel, name='front',
            out_shape=(jax.ShapeDtypeStruct((seq, d_model), bf16),
                       jax.ShapeDtypeStruct((chips, seq, 6 * lanes), bf16),
                       jax.ShapeDtypeStruct((chips, 2, rows, 2 * ffb), bf16),
                       jax.ShapeDtypeStruct((chips, 2, rows, d_model), bf16),
                       jax.ShapeDtypeStruct((8, d_model), f32)),
            in_specs=[ANY, vmem, vmem, vmem, vmem, ANY, ANY, ANY], out_specs=(vmem, ANY, ANY, ANY, vmem),
            scratch_shapes=[pltpu.VMEM((chips, 8, lanes), jnp.int32),
                            pltpu.VMEM((chips * seq, 1), f32),
                            pltpu.VMEM((2,) + embed_table.shape, bf16),
                            pltpu.VMEM((2, 4 * seq, embed_table.shape[0]), bf16),
                            pltpu.VMEM((chips * seq, d_model), bf16),
                            pltpu.VMEM((seq, d_model * n_off), bf16),
                            pltpu.VMEM((chips * seq, d_model), bf16),
                            pltpu.VMEM((chips, rows, 6 * lanes), bf16),
                            pltpu.VMEM((d_model, 6 * lanes), bf16),
                            pltpu.VMEM((5 * seq, d_model), bf16),
                            pltpu.VMEM((5 * seq, 6 * lanes), f32),
                            pltpu.VMEM((chips, seq, 6 * lanes), bf16),
                            dma2(n_off + 1), dma2(n_off), dma2(n_off + 1), dma2(2 * n_off), dma2(n_off + 1),
                            dma2(AG_MSGS), dma2(chips), dma2(RS_MSGS), dma2(AG_MSGS), dma2(n_off), dma(6)],
            compiler_params=params(1),
        )(tok, gains, w_qkv, cos2, sin2, w_gate_up, w_out, embed_table)

        wo_full = wo_all.reshape(q_width, d_model)
        gain_mlp = gain_rows[1]
        heads = mine.reshape(chips, seq, 6, lanes)[..., :head_dim].transpose(2, 1, 0, 3)

        def by_head(i):
            return jnp.stack([heads[2 * i], heads[2 * i + 1]], axis=2).reshape(seq, 2 * chips, head_dim)

        ctx_own = by_head(0).reshape(seq, q_width)
        key_own = by_head(1)[None]
        val_own = by_head(2)[None]

        attn_proj = jnp.dot(ctx_own, wo_full, preferred_element_type=f32)
        x_mid = (x_own.astype(f32) + attn_proj).astype(bf16)
        normed_mlp = rms_norm(x_mid, gain_mlp)

        layer_out = pl.pallas_call(
            mlp_kernel, name='mlp',
            out_shape=jax.ShapeDtypeStruct((seq, d_model), bf16),
            in_specs=[ANY, vmem, ANY, ANY], out_specs=vmem,
            scratch_shapes=[pltpu.VMEM((chips * seq, d_model), bf16),
                            pltpu.VMEM((chips, 2, rows, 2 * ffb), bf16),
                            pltpu.VMEM((2, ffb // 2, d_model), bf16),
                            pltpu.VMEM((chips * seq, ffb), bf16),
                            pltpu.VMEM((chips * seq, d_model), f32),
                            pltpu.VMEM((seq, d_model * n_off), f32),
                            dma(AG_MSGS), dma(AG_MSGS), dma(RS_MSGS), dma(RS_MSGS), dma(1), dma(1), dma(3)],
            compiler_params=params(4),
        )(normed_mlp, x_mid, wgu_all, w_down)
        return layer_out[None], key_own, val_own

    return jax.shard_map(
        device_step,
        mesh=mesh,
        in_specs=(P(batch_axes, None), row_spec, P(AXIS), row_spec, row_spec, P(AXIS), row_spec, row_spec, P(None)),
        out_specs=(P(batch_axes, None, None), P(batch_axes, None, None, None), P(batch_axes, None, None, None)),
        check_vma=False,
    )
```

```python
import jax
import jax.numpy as jnp
from jax import lax
from jax.experimental import pallas as pl
from jax.experimental.pallas import tpu as pltpu
from jax.sharding import PartitionSpec as P

NORM_EPS = 1e-5
ROPE_THETA = 10000.0
AXIS = 'fsdp'
MESH = pl.DeviceIdType.MESH
ANY = pl.BlockSpec(memory_space=pl.ANY)
VMEM_LIMIT = 60 * 1024 * 1024


class Place:
    def __init__(self, side):
        me = lax.axis_index(AXIS)
        self.side = side
        self.c = lax.rem(me, 2)
        chip = lax.div(me, 2)
        self.y = lax.div(chip, side)
        self.x = lax.rem(chip, side)
        self.me = me
        self.partner = me + 1 - 2 * self.c

    def chip(self, dy, dx):
        s = self.side
        return lax.rem(self.y + dy + s, s) * s + lax.rem(self.x + dx + s, s)

    def dev(self, dy, dx):
        return self.chip(dy, dx) * 2 + self.c


def barrier(devices):
    sem = pltpu.get_barrier_semaphore()
    for d in devices:
        pl.semaphore_signal(sem, inc=1, device_id={AXIS: d}, device_id_type=MESH)
    pl.semaphore_wait(sem, len(devices))


class Msgs:
    def __init__(self, send_sem, recv_sem):
        self.send_sem, self.recv_sem = send_sem, recv_sem
        self.index, self.copies = {}, []

    def start(self, name, src, dst, dev):
        i = len(self.copies)
        self.index[name] = i
        copy = pltpu.make_async_remote_copy(
            src_ref=src, dst_ref=dst, send_sem=self.send_sem.at[i], recv_sem=self.recv_sem.at[i],
            device_id={AXIS: dev}, device_id_type=MESH)
        copy.start()
        self.copies.append(copy)

    def recv(self, name):
        self.copies[self.index[name]].wait_recv()

    def drain(self):
        for copy in self.copies:
            copy.wait_send()


AG_MSGS = 40
RS_MSGS = 40


SLOTS = ((0, 0), (0, 1), (0, -1), (1, 0), (-1, 0), (1, 1), (1, -1), (-1, 1), (-1, -1),
         (2, 0), (0, 2), (2, 1), (2, -1), (1, 2), (-1, 2), (2, 2))


def slot_of(a, b):
    return SLOTS.index(((a + 1) % 4 - 1, (b + 1) % 4 - 1))


def swap_if(h, a, b):
    return (b, a) if h == 0 else (a, b)


HALVES = (0, 1)


class Gather:
    def __init__(self, pos, m, blk, width, by_chip=False):
        self.pos, self.m, self.blk, self.q, self.by_chip = pos, m, blk, width // 4, by_chip

    def send(self, h, name, a, b, lo, n, ta, tb):
        lo = 2 * self.q * h + lo
        if self.by_chip:
            src = dst = self.blk(self.pos.chip(*swap_if(h, a, b)), lo, n)
        else:
            src = self.blk(slot_of(*swap_if(h, a, b)), lo, n)
            dst = self.blk(slot_of(*swap_if(h, a - ta, b - tb)), lo, n)
        self.m.start(('ag', h) + name, src, dst, self.pos.dev(*swap_if(h, ta, tb)))

    def recv(self, h, *name):
        self.m.recv(('ag', h) + name)

    def second(self, h, a):
        self.send(h, ('2p', a), a, 0, 0, 2 * self.q, 0, 1)
        self.send(h, ('2m', a), a, 0, 0, 2 * self.q, 0, -1)

    def second_forward(self, a):
        for h in HALVES:
            self.recv(h, '2p', a)
            self.send(h, ('2pf', a), a, -1, 0, self.q, 0, 1)
            self.recv(h, '2m', a)
            self.send(h, ('2mf', a), a, 1, self.q, self.q, 0, -1)

    def last(self, a):
        for h in HALVES:
            self.recv(h, '2pf', a)
            self.recv(h, '2mf', a)

    def begin(self):
        q = self.q
        for h in HALVES:
            self.send(h, ('1p',), 0, 0, 0, 2 * q, 1, 0)
            self.send(h, ('1m',), 0, 0, 0, 2 * q, -1, 0)
        for h in HALVES:
            self.second(h, 0)
        for h in HALVES:
            self.recv(h, '1p')
            self.send(h, ('1pf',), -1, 0, 0, q, 1, 0)
            self.second(h, -1)
        for h in HALVES:
            self.recv(h, '1m')
            self.send(h, ('1mf',), 1, 0, q, q, -1, 0)
            self.second(h, 1)
        self.second_forward(0)

    def middle(self):
        for h in HALVES:
            self.recv(h, '1pf')
            self.recv(h, '1mf')
            self.second(h, 2)

    def rest(self, near=lambda: None, middle=lambda: None, before_last=lambda: None):
        self.middle()
        near()
        self.second_forward(-1)
        self.second_forward(1)
        self.second_forward(2)
        before_last()
        middle()
        for a in (0, -1, 1, 2):
            self.last(a)

    def run_slots(self, hook, before_last=lambda: None):
        self.begin()
        self.middle()
        hook(0, 5)
        self.second_forward(-1)
        self.second_forward(1)
        hook(5, 4)
        self.second_forward(2)
        before_last()
        self.last(0)
        hook(9, 2)
        self.last(-1)
        self.last(1)
        hook(11, 4)
        self.last(2)
        hook(15, 1)


class Line:
    STEPS = (0, 1, -1, 2)

    def __init__(self, pos, m, name, axis):
        self.pos, self.m, self.name, self.axis = pos, m, name, axis

    def dev(self, t):
        return self.pos.dev(0, t) if self.axis == 'x' else self.pos.dev(t, 0)

    def index(self, t):
        return lax.rem((self.pos.x if self.axis == 'x' else self.pos.y) + t + 4, 4)

    def start(self, key, src, dst, t):
        self.m.start((self.name, key), src, dst, self.dev(t))

    def recv(self, key):
        self.m.recv((self.name, key))

    def gather_begin(self, buf):
        self.start('gp', buf.at[0], buf.at[2], 1)
        self.start('gm', buf.at[0], buf.at[1], -1)

    def gather_forward(self, buf):
        half = buf.shape[1] // 2
        self.recv('gp')
        self.start('gpf', buf.at[2, pl.ds(0, half)], buf.at[3, pl.ds(0, half)], 1)
        self.recv('gm')
        self.start('gmf', buf.at[1, pl.ds(half, half)], buf.at[3, pl.ds(half, half)], -1)

    def gather_last(self):
        self.recv('gpf')
        self.recv('gmf')

    def scatter_begin(self, part, recv_buf, rows):
        half = part.shape[1] // 2
        self.rows, self.half = rows, half
        self.start('spf', part.at[self.block(2), pl.ds(0, half)], recv_buf.at[pl.ds(0, rows), pl.ds(0, half)], 1)
        self.start('smf', part.at[self.block(2), pl.ds(half, half)], recv_buf.at[pl.ds(0, rows), pl.ds(half, half)], -1)

    def block(self, t, lo=0, n=None):
        return pl.ds(pl.multiple_of(self.index(t) * self.rows + lo, 16), self.rows if n is None else n)

    def add(self, part, recv_buf, t, first, cols):
        @pl.loop(0, self.rows // 16)
        def _(i):
            lo = pl.multiple_of(i * 16, 16)
            mine = self.block(t, lo, 16)
            part[mine, cols] = part[mine, cols] + recv_buf[pl.ds(pl.multiple_of(first + lo, 16), 16), cols]

    def scatter_middle(self, part, recv_buf):
        rows, half = self.rows, self.half
        self.recv('spf')
        self.add(part, recv_buf, 1, 0, pl.ds(0, half))
        self.start('sp', part.at[self.block(1)], recv_buf.at[pl.ds(rows, rows)], 1)
        self.recv('smf')
        self.add(part, recv_buf, -1, 0, pl.ds(half, half))
        self.start('sm', part.at[self.block(-1)], recv_buf.at[pl.ds(2 * rows, rows)], -1)

    def scatter_last(self, part, recv_buf):
        every = pl.ds(0, 2 * self.half)
        self.recv('sp')
        self.add(part, recv_buf, 0, self.rows, every)
        self.recv('sm')
        self.add(part, recv_buf, 0, 2 * self.rows, every)


class Scatter:
    def __init__(self, pos, m, part, recv_buf, rows, width):
        self.pos, self.m, self.part, self.recv_buf = pos, m, part, recv_buf
        self.rows, self.q = rows, width // 4
        self.places = {}

    def send(self, h, name, a, b, lo, n, ta, tb):
        key = ('rs', h) + name
        self.places[key] = sum(k for _, k in self.places.values()), n // self.q
        first = self.places[key][0]
        src = self.part.at[pl.ds(slot_of(*swap_if(1 - h, a, b)) * self.rows, self.rows), pl.ds(2 * self.q * h + lo, n)]
        dst = self.recv_buf.at[:, pl.ds(first * self.q, n)]
        self.m.start(key, src, dst, self.pos.dev(*swap_if(1 - h, ta, tb)))

    def recv_add(self, h, name, a, b, lo, n):
        key = ('rs', h) + name
        self.m.recv(key)
        there = pl.ds(self.places[key][0] * self.q, n)
        here = pl.ds(2 * self.q * h + lo, n)
        base = slot_of(*swap_if(1 - h, a, b)) * self.rows

        @pl.loop(0, self.rows // 16)
        def _(i):
            mine = pl.ds(pl.multiple_of(base + i * 16, 16), 16)
            theirs = pl.ds(pl.multiple_of(i * 16, 16), 16)
            self.part[mine, here] = self.part[mine, here] + self.recv_buf[theirs, there]

    def begin(self):
        q = self.q
        for b in (2, 1, -1, 0):
            for h in HALVES:
                self.send(h, ('1pf', b), 2, b, 0, q, 1, 0)
                self.send(h, ('1mf', b), 2, b, q, q, -1, 0)

    def finish(self, hook=lambda i: None):
        q = self.q
        order = (2, 1, -1, 0)
        calls = iter(range(16))
        for b in order:
            for h in HALVES:
                self.recv_add(h, ('1pf', b), 1, b, 0, q)
                self.send(h, ('1p', b), 1, b, 0, 2 * q, 1, 0)
                self.recv_add(h, ('1mf', b), -1, b, q, q)
                self.send(h, ('1m', b), -1, b, 0, 2 * q, -1, 0)
                hook(next(calls))
        for b in order:
            for h in HALVES:
                self.recv_add(h, ('1p', b), 0, b, 0, 2 * q)
                self.recv_add(h, ('1m', b), 0, b, 0, 2 * q)
                if b == 2:
                    self.send(h, ('2pf',), 0, 2, 0, q, 0, 1)
                    self.send(h, ('2mf',), 0, 2, q, q, 0, -1)
                if b == 1:
                    self.recv_add(h, ('2pf',), 0, 1, 0, q)
                    self.send(h, ('2p',), 0, 1, 0, 2 * q, 0, 1)
                if b == -1:
                    self.recv_add(h, ('2mf',), 0, -1, q, q)
                    self.send(h, ('2m',), 0, -1, 0, 2 * q, 0, -1)
                if b == 0:
                    self.recv_add(h, ('2p',), 0, 0, 0, 2 * q)
                    self.recv_add(h, ('2m',), 0, 0, 0, 2 * q)
                hook(next(calls))


def torus_neighbours(pos):
    return [pos.dev(0, 1), pos.dev(0, -1), pos.dev(1, 0), pos.dev(-1, 0)]


def offsets(side):
    return [(1, 1), (-1, -1), (1, -1), (-1, 1), (0, 1), (1, 0), (0, -1), (-1, 0),
            (2, 2), (0, 2), (2, 0), (1, 2), (-1, 2), (2, 1), (2, -1)]


def remote(src, dst, sems, i, dev):
    return pltpu.make_async_remote_copy(src_ref=src, dst_ref=dst, send_sem=sems.at[0, i], recv_sem=sems.at[1, i],
                                        device_id={AXIS: dev}, device_id_type=MESH)


def front_kernel(tok, gains, wqkv, cos2, sin2, wgu, wo, table,
                 x_mid, mine, wgu_all, gain_rows,
                 tok_all, tok_col, tbl, hot, part, recv_buf, x_all, wq_out, wq, normed, proj, packed,
                 ctx_x, ctx_y, wo_x, wo_y, sum_x, sum_y, got_x, got_y,
                 t_sem, q_sem, qf_sem, g_sem, gf_sem, o_sem, of_sem, r_sem, a_sem, e_sem, c_sem, l_sem):
    f32, bf16 = jnp.float32, jnp.bfloat16
    pos = Place(4)
    offs = offsets(4)
    here = pos.chip(0, 0)
    rows, lanes = wq_out.shape[1], 128
    seq, width = packed.shape[1], x_all.shape[1]
    n_slots = len(SLOTS)
    n_off = len(offs)
    ff = wgu.shape[1] // 2
    ffb = ff // n_slots
    head_dim = wqkv.shape[1] // (6 * n_slots)
    table_rows = table.shape[0]
    tile = 256
    loads = [pltpu.make_async_copy(table, tbl.at[pos.c], l_sem.at[0]),
             pltpu.make_async_copy(tok, tok_all.at[0], l_sem.at[1])]
    colb = width // 4
    my_head = pl.ds(pl.multiple_of(pos.c * lanes, lanes), rows)
    m4 = Msgs(c_sem.at[0], c_sem.at[1])
    line_x, line_y = Line(pos, m4, 'x', 'x'), Line(pos, m4, 'y', 'y')

    def out_cols(line, t):
        return wo.at[:, pl.ds(pl.multiple_of(line.index(t) * colb, lanes), colb)]

    for k, (line, w) in enumerate(((line_x, wo_x), (line_y, wo_y))):
        loads.append(pltpu.make_async_copy(out_cols(line, 0), w.at[0, my_head], l_sem.at[6 + k]))
    for j in (0, 1):
        src = wgu.at[:, pl.ds(pl.multiple_of(j * ff + here * ffb, 128), ffb)]
        loads.append(pltpu.make_async_copy(src, wgu_all.at[here, pos.c, :, pl.ds(j * ffb, ffb)], l_sem.at[3 + j]))
    for cp in loads:
        cp.start()
    barrier([pos.dev(dy, dx) for dy, dx in offs] + [pos.partner])

    toks = [remote(tok, tok_all.at[slot_of(-dy, -dx)], t_sem, i, pos.dev(dy, dx)) for i, (dy, dx) in enumerate(offs)]
    for cp in toks:
        cp.start()
    swap = remote(table, tbl.at[pos.c], t_sem, n_off, pos.partner)
    swap.start()
    pad = jnp.zeros((4, lanes - rows, colb), bf16)
    for w in (wo_x, wo_y):
        for hd in (0, 1):
            w[:, hd * lanes + rows:(hd + 1) * lanes, :] = pad

    for p in range(n_slots):
        for k in range(6):
            j, hd = k // 2, k % 2
            lo = (j * 2 * n_slots + p * 2 + hd) * head_dim
            block = jnp.concatenate([wqkv[:, lo:lo + head_dim], jnp.zeros((rows, lanes - head_dim), bf16)], axis=1)
            if k == 4:
                block = block + gains[...]
            wq_out[p, :, k * lanes:(k + 1) * lanes] = block
    my_rows = pl.ds(pl.multiple_of(pos.me * rows, 32), rows)
    qs = [remote(wq_out.at[pos.chip(dy, dx)], wq.at[my_rows], q_sem, i, pos.dev(dy, dx)) for i, (dy, dx) in enumerate(offs)]
    for cp in qs:
        cp.start()
    os = []
    for k, (line, w) in enumerate(((line_x, wo_x), (line_y, wo_y))):
        for i, t in enumerate((1, -1, 2)):
            slot = Line.STEPS.index(2 if t == 2 else -t)
            os.append(remote(out_cols(line, t), w.at[slot, my_head], o_sem, 3 * k + i, line.dev(t)))
            os[-1].start()
    wq[my_rows, :] = wq_out[here]

    loads[1].wait()
    for i, (dy, dx) in enumerate(offs):
        toks[i].wait_recv()
    for s in range(n_slots):
        column = jnp.transpose(tok_all[s].astype(f32))
        tok_col[pl.ds(s * seq, seq), :] = column[:seq, 0:1]
    loads[0].wait()
    swap.wait_recv()
    group = hot.shape[1]
    for g in range(n_slots * seq // group):
        mine_rows = pl.ds(g * group, group)
        for cc in (0, 1):
            ids = lax.broadcasted_iota(jnp.int32, (group, table_rows), 1) + (here * 2 + cc) * table_rows
            hot[cc] = jnp.where(tok_col[mine_rows, :] == ids.astype(f32), 1.0, 0.0).astype(bf16)

        @pl.loop(0, width // tile)
        def _(i):
            cols = pl.ds(pl.multiple_of(i * tile, tile), tile)
            total = (jnp.dot(hot[0], tbl[0, :, cols], preferred_element_type=f32)
                     + jnp.dot(hot[1], tbl[1, :, cols], preferred_element_type=f32))
            part[mine_rows, cols] = total.astype(bf16)

    m = Msgs(r_sem.at[0], r_sem.at[1])
    scatter = Scatter(pos, m, part, recv_buf, seq, width)
    scatter.begin()

    fwd = []

    def forward(sems, i, ref):
        cp = remote(ref, ref, sems, i, pos.partner)
        cp.start()
        fwd.append(cp)
        return cp

    q_fwd = [forward(qf_sem, n_off, wq.at[my_rows])]
    for i, (dy, dx) in enumerate(offs):
        qs[i].wait_recv()
        q_fwd.append(forward(qf_sem, i, wq.at[pl.ds(pl.multiple_of(pos.dev(-dy, -dx) * rows, 32), rows)]))
    for cp in q_fwd:
        cp.wait_recv()
    for k in range(width // lanes):
        square = jnp.transpose(wq[pl.ds(k * lanes, lanes), 4 * lanes:5 * lanes].astype(f32))
        gain_rows[:, k * lanes:(k + 1) * lanes] = square[head_dim:head_dim + 8, :]

    gs = []
    for i, (dy, dx) in enumerate(offs):
        for j in (0, 1):
            src = wgu.at[:, pl.ds(pl.multiple_of(j * ff + pos.chip(dy, dx) * ffb, 128), ffb)]
            gs.append(remote(src, wgu_all.at[here, pos.c, :, pl.ds(j * ffb, ffb)], g_sem, 2 * i + j, pos.dev(dy, dx)))

    def send_gate_up(i):
        for cp in gs[2 * i:2 * i + 2]:
            cp.start()

    scatter.finish(send_gate_up)
    x_all[pl.ds(0, seq), :] = part[pl.ds(0, seq), :]

    sends = []

    def attend(first, n):
        base = first * seq

        @pl.loop(0, n * seq // 16)
        def _(i):
            x = x_all[pl.ds(pl.multiple_of(base + i * 16, 16), 16), :].astype(f32)
            inv = lax.rsqrt(jnp.mean(x * x, axis=-1, keepdims=True) + NORM_EPS)
            normed[pl.ds(pl.multiple_of(i * 16, 16), 16), :] = (x * inv * gain_rows[0:1, :]).astype(bf16)

        @pl.loop(0, 3)
        def _(i):
            cols = pl.ds(pl.multiple_of(i * tile, tile), tile)
            proj[pl.ds(0, n * seq), cols] = jnp.dot(normed[pl.ds(0, n * seq), :], wq[:, cols], preferred_element_type=f32)

        lane = lax.broadcasted_iota(jnp.int32, (seq, lanes), 1)
        causal = lax.broadcasted_iota(jnp.int32, (seq, seq), 0) >= lax.broadcasted_iota(jnp.int32, (seq, seq), 1)

        def rope(u):
            other = jnp.where(lane < head_dim // 2, pltpu.roll(u, lanes - head_dim // 2, 1), pltpu.roll(u, head_dim // 2, 1))
            return (u * cos2[...] + other * sin2[...]).astype(bf16)

        def one(s, seq_x, seq_y):
            mine_rows = pl.ds(s * seq, seq)
            kv = []
            for hd in (0, 1):
                q = rope(proj[mine_rows, hd * lanes:(hd + 1) * lanes])
                k = rope(proj[mine_rows, (2 + hd) * lanes:(3 + hd) * lanes])
                v = proj[mine_rows, (4 + hd) * lanes:(5 + hd) * lanes]
                v = jnp.where(lane < head_dim, v, 0.0).astype(bf16)
                scores = lax.dot_general(q, k, (((1,), (1,)), ((), ())), preferred_element_type=f32) * (head_dim ** -0.5)
                scores = jnp.where(causal, scores, -jnp.inf)
                e = jnp.exp(scores - jnp.max(scores, axis=-1, keepdims=True))
                probs = (e / jnp.sum(e, axis=-1, keepdims=True)).astype(bf16)
                context = jnp.dot(probs, v, preferred_element_type=f32).astype(bf16)
                ctx_x[0, seq_x, hd * lanes:(hd + 1) * lanes] = context[:seq // 2]
                ctx_y[0, seq_y, hd * lanes:(hd + 1) * lanes] = context[seq // 2:]
                kv.append((k[:, :head_dim], v[:, :head_dim]))
            packed[first + s] = jnp.concatenate([kv[0][0], kv[1][0], kv[0][1], kv[1][1]], axis=1)

        half = seq // 2
        for s in range(n):
            a, b = SLOTS[first + s]
            yq, xq = line_y.index(a), line_x.index(b)
            one(s, pl.ds(pl.multiple_of((yq * 4 + xq) * half, half), half), pl.ds(pl.multiple_of((xq * 4 + yq) * half, half), half))

    m2 = Msgs(a_sem.at[0], a_sem.at[1])
    gather = Gather(pos, m2, lambda s, lo, n: x_all.at[pl.ds(s * seq, seq), pl.ds(lo, n)], width)
    for cp in loads[2:]:
        cp.wait()
    forward(gf_sem, n_off, wgu_all.at[here, pos.c])
    o_fwd = [forward(of_sem, 4 * k, w.at[0, my_head]) for k, w in enumerate((wo_x, wo_y))]
    for k, w in enumerate((wo_x, wo_y)):
        for i, t in enumerate((1, -1, 2)):
            os[3 * k + i].wait_recv()
            slot = Line.STEPS.index(2 if t == 2 else -t)
            o_fwd.append(forward(of_sem, 4 * k + slot, w.at[slot, my_head]))

    gather.run_slots(attend)

    lines = ((line_x, ctx_x, wo_x, sum_x, line_y, got_x), (line_y, ctx_y, wo_y, sum_y, line_x, got_y))
    for line, ctx, *_ in lines:
        line.gather_begin(ctx)
    for s in range(n_slots):
        if s == 0:
            cp = pltpu.make_async_copy(packed.at[0], mine.at[here], l_sem.at[5])
        else:
            cp = remote(packed.at[s], mine.at[here], e_sem, s - 1, pos.dev(*SLOTS[s]))
        sends.append(cp)
    for line, ctx, *_ in lines:
        line.gather_forward(ctx)
    for cp in sends:
        cp.start()
    for cp in o_fwd:
        cp.wait_recv()

    def project(ctx, w, total, slots, add):
        @pl.loop(0, colb // tile)
        def _(i):
            cols = pl.ds(pl.multiple_of(i * tile, tile), tile)
            acc = sum(jnp.dot(ctx[j], w[j, :, cols], preferred_element_type=f32) for j in slots)
            total[:, cols] = total[:, cols] + acc if add else acc

    for line, ctx, w, total, *_ in lines:
        project(ctx, w, total, (0, 1, 2), False)
    for line, ctx, w, total, other, got in lines:
        line.gather_last()
        project(ctx, w, total, (3,), True)
        other.scatter_begin(total, got, total.shape[0] // 4)
    for line, ctx, w, total, other, got in lines:
        other.scatter_middle(total, got)
    half = seq // 2
    for k, (line, ctx, w, total, other, got) in enumerate(lines):
        other.scatter_last(total, got)
        cols = pl.ds(pl.multiple_of(line.index(0) * colb, lanes), colb)
        for t in Line.STEPS:
            a, b = (0, t) if k == 0 else (t, 0)
            x = x_all[pl.ds(slot_of(a, b) * seq + k * half, half), cols].astype(f32)
            lo = pl.multiple_of(line.index(t) * half, half)
            x_mid[k, pl.ds(lo, half), :] = (x + total[other.block(0, lo, half), :]).astype(bf16)

    for i, (dy, dx) in enumerate(offs):
        gs[2 * i].wait_recv()
        gs[2 * i + 1].wait_recv()
        forward(gf_sem, i, wgu_all.at[pos.chip(-dy, -dx), pos.c])
    for cp in sends:
        cp.wait()
    for cp in toks + qs + gs + os + [swap]:
        cp.wait_send()
    waited = q_fwd + o_fwd
    for cp in fwd:
        if any(cp is w for w in waited):
            cp.wait_send()
        else:
            cp.wait()
    for msgs in (m, m2, m4):
        msgs.drain()


def mlp_kernel(piece, gain_rows, wgu_hbm, wd_hbm, out, mid_x, mid_y, normed, wgu, wd, act, part, recv_buf,
               s1, r1, s2, r2, w_send, w_recv, l_sem):
    pos = Place(4)
    f32, bf16 = jnp.float32, jnp.bfloat16
    rows, width = out.shape
    half_rows = rows // 2
    n_rows, colb = piece.shape[1:]
    ffb = act.shape[1]
    half = ffb // 2
    tile = 256
    m = Msgs(s1, r1)
    line_x, line_y = Line(pos, m, 'x', 'x'), Line(pos, m, 'y', 'y')

    def blk(p, lo, n):
        y, x = lax.div(p, 4), lax.rem(p, 4)
        first = lo < colb
        r, c = (y, x) if first else (x, y)
        ref = mid_x if first else mid_y
        lo = lo if first else lo - colb
        return ref.at[pl.ds(pl.multiple_of(r * n_rows, n_rows), n_rows), pl.ds(pl.multiple_of(c * colb + lo, 128), n)]

    here = pos.chip(0, 0)
    loads = [pltpu.make_async_copy(piece.at[0], blk(here, 0, colb), l_sem.at[0]),
             pltpu.make_async_copy(piece.at[1], blk(here, colb, colb), l_sem.at[3]),
             pltpu.make_async_copy(wgu_hbm, wgu, l_sem.at[1]),
             pltpu.make_async_copy(wd_hbm, wd.at[pos.c], l_sem.at[2])]
    for cp in loads:
        cp.start()
    barrier(torus_neighbours(pos) + [pos.partner])
    loads[0].wait()
    loads[1].wait()
    gather = Gather(pos, m, blk, 2 * colb, by_chip=True)
    push = pltpu.make_async_remote_copy(src_ref=wd_hbm, dst_ref=wd.at[pos.c], send_sem=w_send.at[0], recv_sem=w_recv.at[0],
                                        device_id={AXIS: pos.partner}, device_id_type=MESH)
    push.start()

    def gate_up(v):
        for k, (mid, line, other) in enumerate(((mid_x, line_y, line_x), (mid_y, line_x, line_y))):
            for i, t in enumerate(Line.STEPS):
                src = pl.multiple_of(line.index(v) * n_rows + other.index(t) * half_rows, half_rows)
                dst = (k * 4 + i) * half_rows

                @pl.loop(0, half_rows // 16)
                def _(j):
                    x = mid[pl.ds(pl.multiple_of(src + j * 16, 16), 16), :].astype(f32)
                    inv = lax.rsqrt(jnp.mean(x * x, axis=-1, keepdims=True) + NORM_EPS)
                    normed[pl.ds(pl.multiple_of(dst + j * 16, 16), 16), :] = (x * inv * gain_rows[1:2, :]).astype(bf16)

        @pl.loop(0, ffb // tile)
        def _(i):
            lo = pl.multiple_of(i * tile, tile)
            h = normed[...]
            g = jnp.dot(h, wgu[:, :, :, pl.ds(lo, tile)].reshape(width, tile), preferred_element_type=f32)
            u = jnp.dot(h, wgu[:, :, :, pl.ds(pl.multiple_of(ffb + lo, tile), tile)].reshape(width, tile),
                        preferred_element_type=f32)
            a = (jax.nn.silu(g) * u).astype(bf16)
            for k in (0, 1):
                for i, t in enumerate(Line.STEPS):
                    slot = slot_of(v, t) if k == 0 else slot_of(t, v)
                    src = (k * 4 + i) * half_rows
                    act[pl.ds(slot * rows + k * half_rows, half_rows), pl.ds(lo, tile)] = a[src:src + half_rows]

    def down(first, n):
        mine = pl.ds(first * rows, n * rows)

        @pl.loop(0, width // tile)
        def _(i):
            cols = pl.ds(pl.multiple_of(i * tile, tile), tile)
            part[mine, cols] = jnp.dot(act[mine, :], wd[:, :, cols].reshape(2 * half, tile), preferred_element_type=f32)

    def near():
        loads[2].wait()
        gate_up(0)

    def middle():
        gate_up(1)
        gate_up(-1)

    gather.begin()
    gather.rest(near, middle)
    gate_up(2)
    loads[3].wait()
    push.wait()
    m2 = Msgs(s2, r2)
    scatter = Scatter(pos, m2, part, recv_buf, rows, width)
    down(9, 7)
    scatter.begin()
    down(0, 9)
    scatter.finish()
    for k, (mid, line, other) in enumerate(((mid_x, line_y, line_x), (mid_y, line_x, line_y))):
        src = pl.multiple_of(line.index(0) * n_rows + other.index(0) * half_rows, half_rows)
        mine = pl.ds(k * half_rows, half_rows)
        out[mine, :] = (mid[pl.ds(src, half_rows), :].astype(f32) + part[mine, :]).astype(bf16)
    m.drain()
    m2.drain()


def dma(n):
    return pltpu.SemaphoreType.DMA((n,))


def dma2(n):
    return pltpu.SemaphoreType.DMA((2, n))


def params(cid):
    return pltpu.CompilerParams(collective_id=cid, has_side_effects=True, vmem_limit_bytes=VMEM_LIMIT)


def rope_tables(rope_scale, seq_len, lanes):
    half_dim = rope_scale.shape[0]
    freq_expo = jnp.arange(half_dim, dtype=jnp.float32) * (2.0 / (2 * half_dim))
    inv_freq = 1.0 / (rope_scale * jnp.power(ROPE_THETA, freq_expo))
    angles = jnp.arange(seq_len, dtype=jnp.float32)[:, None] * inv_freq[None, :]
    cos, sin = jnp.cos(angles), jnp.sin(angles)
    rest = jnp.zeros((seq_len, lanes - 2 * half_dim), jnp.float32)
    return jnp.concatenate([cos, cos, rest], axis=1), jnp.concatenate([-sin, sin, rest], axis=1)


def solution(mesh):
    batch_axes = ('dp', AXIS)
    row_spec = P(AXIS, None)
    n_dev = mesh.shape[AXIS]
    chips = n_dev // 2
    n_off = chips - 1

    def device_step(tokens, embed_table, norm_attn, w_qkv, w_out, norm_mlp, w_gate_up, w_down, rope_scale):
        f32, bf16 = jnp.float32, jnp.bfloat16
        seq = tokens.shape[1]
        rows, d_model = w_out.shape
        head_dim = 2 * rope_scale.shape[0]
        q_width = rows * n_dev
        ff = w_gate_up.shape[1] // 2
        ffb = ff // chips
        lanes = 128
        tok = jnp.zeros((8, lanes), jnp.int32) + jnp.pad(tokens, ((0, 0), (0, lanes - seq)))
        column = lax.broadcasted_iota(jnp.int32, (rows, lanes), 1)
        gains = (jnp.where(column == head_dim, norm_attn[:, None], 0)
                 + jnp.where(column == head_dim + 1, norm_mlp[:, None], 0)).astype(bf16)
        cos2, sin2 = rope_tables(rope_scale, seq, lanes)
        vmem = pl.BlockSpec(memory_space=pltpu.VMEM)

        half_toks = chips * seq // 2
        colb = d_model // 4
        x_mid, mine, wgu_all, gain_rows = pl.pallas_call(
            front_kernel, name='front',
            out_shape=(jax.ShapeDtypeStruct((2, half_toks // 4, colb), bf16),
                       jax.ShapeDtypeStruct((chips, seq, 4 * head_dim), bf16),
                       jax.ShapeDtypeStruct((chips, 2, rows, 2 * ffb), bf16),
                       jax.ShapeDtypeStruct((8, d_model), f32)),
            in_specs=[ANY, vmem, vmem, vmem, vmem, ANY, ANY, ANY], out_specs=(vmem, ANY, ANY, vmem),
            scratch_shapes=[pltpu.VMEM((chips, 8, lanes), jnp.int32),
                            pltpu.VMEM((chips * seq, 1), f32),
                            pltpu.VMEM((2,) + embed_table.shape, bf16),
                            pltpu.VMEM((2, 4 * seq, embed_table.shape[0]), bf16),
                            pltpu.VMEM((chips * seq, d_model), bf16),
                            pltpu.VMEM((seq, d_model * n_off), bf16),
                            pltpu.VMEM((chips * seq, d_model), bf16),
                            pltpu.VMEM((chips, rows, 6 * lanes), bf16),
                            pltpu.VMEM((d_model, 6 * lanes), bf16),
                            pltpu.VMEM((5 * seq, d_model), bf16),
                            pltpu.VMEM((5 * seq, 6 * lanes), f32),
                            pltpu.VMEM((chips, seq, 4 * head_dim), bf16)]
                           + [pltpu.VMEM((4, half_toks, 2 * lanes), bf16)] * 2
                           + [pltpu.VMEM((4, 2 * lanes, colb), bf16)] * 2
                           + [pltpu.VMEM((half_toks, colb), f32)] * 2
                           + [pltpu.VMEM((3 * half_toks // 4, colb), f32)] * 2
                           + [dma2(n_off + 1), dma2(n_off), dma2(n_off + 1), dma2(2 * n_off), dma2(n_off + 1),
                              dma2(6), dma2(8), dma2(RS_MSGS), dma2(AG_MSGS), dma2(n_off), dma2(16), dma(8)],
            compiler_params=params(1),
        )(tok, gains, w_qkv, cos2, sin2, w_gate_up, w_out, embed_table)

        layer_out = pl.pallas_call(
            mlp_kernel, name='mlp',
            out_shape=jax.ShapeDtypeStruct((seq, d_model), bf16),
            in_specs=[ANY, vmem, ANY, ANY], out_specs=vmem,
            scratch_shapes=[pltpu.VMEM((half_toks, d_model), bf16),
                            pltpu.VMEM((half_toks, d_model), bf16),
                            pltpu.VMEM((half_toks // 2, d_model), bf16),
                            pltpu.VMEM((chips, 2, rows, 2 * ffb), bf16),
                            pltpu.VMEM((2, ffb // 2, d_model), bf16),
                            pltpu.VMEM((chips * seq, ffb), bf16),
                            pltpu.VMEM((chips * seq, d_model), f32),
                            pltpu.VMEM((seq, d_model * n_off), f32),
                            dma(AG_MSGS), dma(AG_MSGS), dma(RS_MSGS), dma(RS_MSGS), dma(1), dma(1), dma(4)],
            compiler_params=params(4),
        )(x_mid, gain_rows, wgu_all, w_down)

        heads = mine.reshape(chips, seq, 2, 2, head_dim).transpose(2, 1, 0, 3, 4).reshape(2, 1, seq, 2 * chips, head_dim)
        key_own, val_own = heads[0], heads[1]
        return layer_out[None], key_own, val_own

    return jax.shard_map(
        device_step,
        mesh=mesh,
        in_specs=(P(batch_axes, None), row_spec, P(AXIS), row_spec, row_spec, P(AXIS), row_spec, row_spec, P(None)),
        out_specs=(P(batch_axes, None, None), P(batch_axes, None, None, None), P(batch_axes, None, None, None)),
        check_vma=False,
    )
```

```python
import jax
import jax.numpy as jnp
from jax import lax
from jax.experimental import pallas as pl
from jax.experimental.pallas import tpu as pltpu
from jax.sharding import PartitionSpec as P

NORM_EPS = 1e-5
ROPE_THETA = 10000.0
AXIS = 'fsdp'
MESH = pl.DeviceIdType.MESH
ANY = pl.BlockSpec(memory_space=pl.ANY)
VMEM_LIMIT = 60 * 1024 * 1024


class Place:
    def __init__(self, side):
        me = lax.axis_index(AXIS)
        self.side = side
        self.c = lax.rem(me, 2)
        chip = lax.div(me, 2)
        self.y = lax.div(chip, side)
        self.x = lax.rem(chip, side)
        self.me = me
        self.partner = me + 1 - 2 * self.c

    def chip(self, dy, dx):
        s = self.side
        return lax.rem(self.y + dy + s, s) * s + lax.rem(self.x + dx + s, s)

    def dev(self, dy, dx):
        return self.chip(dy, dx) * 2 + self.c


def barrier(devices):
    sem = pltpu.get_barrier_semaphore()
    for d in devices:
        pl.semaphore_signal(sem, inc=1, device_id={AXIS: d}, device_id_type=MESH)
    pl.semaphore_wait(sem, len(devices))


def remote(src, dst, sems, i, dev):
    send, recv = (sems.at[k, i] for k in (0, 1))
    return pltpu.make_async_remote_copy(src_ref=src, dst_ref=dst, send_sem=send, recv_sem=recv,
                                        device_id={AXIS: dev}, device_id_type=MESH)


class Msgs:
    def __init__(self, sems):
        self.sems, self.copies, self.received = sems, {}, set()

    def start(self, name, src, dst, dev):
        assert name not in self.copies
        self.copies[name] = remote(src, dst, self.sems, len(self.copies), dev)
        self.copies[name].start()

    def recv(self, name):
        self.received.add(name)
        self.copies[name].wait_recv()

    def finish(self):
        for name in self.copies:
            if name not in self.received:
                self.recv(name)
            self.copies[name].wait_send()


class Local:
    def __init__(self, sems):
        self.sems, self.copies = sems, {}

    def start(self, name, src, dst):
        self.copies[name] = pltpu.make_async_copy(src, dst, self.sems.at[len(self.copies)])
        self.copies[name].start()

    def wait(self, *names):
        for name in names:
            self.copies[name].wait()


STEPS = (0, 1, -1, 2)
AWAY = STEPS[1:]
SLOTS = sorted(((a, b) for a in STEPS for b in STEPS), key=lambda o: (2 in o, abs(o[0]) + abs(o[1])))


def slot_of(a, b):
    return SLOTS.index(((a + 1) % 4 - 1, (b + 1) % 4 - 1))


def slot_back(t):
    return STEPS.index(2 if t == 2 else -t)


def swap_if(h, a, b):
    return (b, a) if h == 0 else (a, b)


HALVES = (0, 1)
SIGNS = (1, -1)
LANES = 128
CHUNK = 16


def whole(n):
    return 0, n


def part_for(sign):
    return lambda n: (0 if sign > 0 else n // 2, n // 2)


def chunk(i, base=0):
    return pl.ds(pl.multiple_of(base + i * CHUNK, CHUNK), CHUNK)


class Gather:
    def __init__(self, pos, m, blk, width, by_chip=False):
        self.pos, self.m, self.blk, self.half, self.by_chip = pos, m, blk, width // 2, by_chip

    def send(self, h, name, a, b, cut, ta, tb):
        lo, n = cut(self.half)
        lo += self.half * h
        if self.by_chip:
            src = dst = self.blk(self.pos.chip(*swap_if(h, a, b)), lo, n)
        else:
            src = self.blk(slot_of(*swap_if(h, a, b)), lo, n)
            dst = self.blk(slot_of(*swap_if(h, a - ta, b - tb)), lo, n)
        self.m.start((h,) + name, src, dst, self.pos.dev(*swap_if(h, ta, tb)))

    def second(self, h, a):
        for sign in SIGNS:
            self.send(h, ('second', sign, a), a, 0, whole, 0, sign)

    def second_forward(self, a):
        for h in HALVES:
            for sign in SIGNS:
                self.m.recv((h, 'second', sign, a))
                self.send(h, ('second on', sign, a), a, -sign, part_for(sign), 0, sign)

    def last(self, a):
        for h in HALVES:
            for sign in SIGNS:
                self.m.recv((h, 'second on', sign, a))

    def begin(self):
        for h in HALVES:
            for sign in SIGNS:
                self.send(h, ('first', sign), 0, 0, whole, sign, 0)
        for h in HALVES:
            self.second(h, 0)
        for sign in SIGNS:
            for h in HALVES:
                self.m.recv((h, 'first', sign))
                self.send(h, ('first on', sign), -sign, 0, part_for(sign), sign, 0)
                self.second(h, -sign)
        self.second_forward(0)
        for h in HALVES:
            for sign in SIGNS:
                self.m.recv((h, 'first on', sign))
            self.second(h, 2)

    def forward(self):
        for a in AWAY:
            self.second_forward(a)


class Scatter:
    def __init__(self, pos, m, part, recv_buf, rows, width):
        self.pos, self.m, self.part, self.recv_buf = pos, m, part, recv_buf
        self.rows, self.half, self.used, self.places = rows, width // 2, 0, {}

    def send(self, h, name, a, b, cut, ta, tb):
        lo, n = cut(self.half)
        key = (h,) + name
        there = self.places[key] = pl.ds(self.used, n)
        self.used += n
        src = self.part.at[pl.ds(slot_of(*swap_if(1 - h, a, b)) * self.rows, self.rows), pl.ds(self.half * h + lo, n)]
        self.m.start(key, src, self.recv_buf.at[:, there], self.pos.dev(*swap_if(1 - h, ta, tb)))

    def recv_add(self, h, name, a, b, cut):
        lo, n = cut(self.half)
        key = (h,) + name
        self.m.recv(key)
        there, here = self.places[key], pl.ds(self.half * h + lo, n)
        base = slot_of(*swap_if(1 - h, a, b)) * self.rows

        @pl.loop(0, self.rows // CHUNK)
        def _(i):
            mine, theirs = chunk(i, base), chunk(i)
            self.part[mine, here] = self.part[mine, here] + self.recv_buf[theirs, there]

    def begin(self):
        for b in AWAY[::-1] + (0,):
            for h in HALVES:
                for sign in SIGNS:
                    self.send(h, ('first on', sign, b), 2, b, part_for(sign), sign, 0)

    def finish(self, hook):
        calls = iter(range(len(SLOTS)))
        order = AWAY[::-1] + (0,)
        for b in order:
            for h in HALVES:
                for sign in SIGNS:
                    self.recv_add(h, ('first on', sign, b), sign, b, part_for(sign))
                    self.send(h, ('first', sign, b), sign, b, whole, sign, 0)
                hook(next(calls))
        for b in order:
            for h in HALVES:
                for sign in SIGNS:
                    self.recv_add(h, ('first', sign, b), 0, b, whole)
                if b == 2:
                    for sign in SIGNS:
                        self.send(h, ('second on', sign), 0, b, part_for(sign), 0, sign)
                elif b == 0:
                    for sign in SIGNS:
                        self.recv_add(h, ('second', sign), 0, b, whole)
                else:
                    self.recv_add(h, ('second on', b), 0, b, part_for(b))
                    self.send(h, ('second', b), 0, b, whole, 0, b)
                hook(next(calls))


class Line:
    def __init__(self, pos, m, axis):
        self.pos, self.m, self.axis = pos, m, axis

    def dev(self, t):
        return self.pos.dev(0, t) if self.axis == 'x' else self.pos.dev(t, 0)

    def index(self, t):
        side = self.pos.side
        return lax.rem((self.pos.x if self.axis == 'x' else self.pos.y) + t + side, side)

    def block(self, t, n, lo=0, size=None):
        return pl.ds(pl.multiple_of(self.index(t) * n + lo, CHUNK), n if size is None else size)

    def lanes(self, t, n):
        return pl.ds(pl.multiple_of(self.index(t) * n, LANES), n)

    def start(self, key, src, dst, t):
        self.m.start((self.axis,) + key, src, dst, self.dev(t))

    def recv(self, *key):
        self.m.recv((self.axis,) + key)

    def share(self, buf, v, rows):
        for sign in SIGNS:
            self.start(('share', sign, v), buf.at[0, rows], buf.at[slot_back(sign), rows], sign)

    def share_on(self, buf, v, rows_of):
        for sign in SIGNS:
            self.recv('share', sign, v)
            rows = rows_of(part_for(sign))
            self.start(('share on', sign, v), buf.at[slot_back(sign), rows], buf.at[slot_back(2), rows], sign)

    def share_last(self, v):
        for sign in SIGNS:
            self.recv('share on', sign, v)

    def scatter_begin(self, part, recv_buf, rows):
        for sign in SIGNS:
            cols = pl.ds(*part_for(sign)(part.shape[1]))
            self.start(('sum on', sign), part.at[self.block(2, rows), cols], recv_buf.at[pl.ds(0, rows), cols], sign)

    def add(self, part, recv_buf, t, rows, first, cols):
        @pl.loop(0, rows // CHUNK)
        def _(i):
            mine = self.block(t, rows, i * CHUNK, CHUNK)
            part[mine, cols] = part[mine, cols] + recv_buf[chunk(i, first * rows), cols]

    def scatter_middle(self, part, recv_buf, rows):
        for sign in SIGNS:
            self.recv('sum on', sign)
            self.add(part, recv_buf, sign, rows, 0, pl.ds(*part_for(sign)(part.shape[1])))
            to = recv_buf.at[pl.ds(slot_back(sign) * rows, rows)]
            self.start(('sum', sign), part.at[self.block(sign, rows)], to, sign)

    def scatter_last(self, part, recv_buf, rows):
        for sign in SIGNS:
            self.recv('sum', sign)
            self.add(part, recv_buf, 0, rows, slot_back(sign), pl.ds(*whole(part.shape[1])))


def offsets():
    return SLOTS[5:9] + SLOTS[1:5] + SLOTS[15:] + SLOTS[9:15]


def norm_rows(x, gain):
    inv = lax.rsqrt(jnp.mean(x * x, axis=-1, keepdims=True) + NORM_EPS)
    return (x * inv * gain).astype(jnp.bfloat16)


def tiles(n, tile=256):
    return [(lo, min(tile, n - lo)) for lo in range(0, n, tile)]


def tile_of(i, base=0, tile=256):
    return pl.ds(pl.multiple_of(base + i * tile, LANES), tile)


def front_kernel(tok, gains, wqkv, cos2, sin2, wgu, wo, wd, table,
                 x_mid, mine, wgu_all, wd_x, wd_y, gain_rows,
                 packed, tok_all, tok_col, tbl, hot, part, recv_buf, h_all, wq_out, wq, x_parts, proj,
                 ctx_x, ctx_y, wo_x, wo_y, sum_x, sum_y, got_x, got_y, sems, l_sem):
    f32, bf16 = jnp.float32, jnp.bfloat16
    pos = Place(4)
    m, local = Msgs(sems), Local(l_sem)
    line_x, line_y = Line(pos, m, 'x'), Line(pos, m, 'y')
    offs = offsets()
    here = pos.chip(0, 0)
    rows = wq_out.shape[1]
    seq, width = packed.shape[1], h_all.shape[1]
    n_slots = len(SLOTS)
    half, colb = seq // 2, width // 4
    ffb = wgu_all.shape[-1] // 2
    head_dim = packed.shape[2] // 4
    table_rows = table.shape[0]
    my_head = pl.ds(pl.multiple_of(pos.c * LANES, LANES), rows)
    my_rows = pl.ds(pl.multiple_of(pos.me * rows, CHUNK), rows)
    lines = ((line_x, ctx_x, wo_x, sum_x, line_y, got_x), (line_y, ctx_y, wo_y, sum_y, line_x, got_y))
    downs = ((line_x, wd_x), (line_y, wd_y))

    def cols_of(w, line, t):
        return w.at[:, line.lanes(t, colb)]

    def gate_up_block(j, chip):
        return wgu.at[:, pl.ds(pl.multiple_of((j * n_slots + chip) * ffb, LANES), ffb)]

    def gate_up_place(j):
        return wgu_all.at[here, pos.c, :, pl.ds(j * ffb, ffb)]

    local.start('table', table, tbl.at[pos.c])
    local.start('tok', tok, tok_all.at[0])
    for k, (line, ctx, w, *_) in enumerate(lines):
        local.start(('wo', k), cols_of(wo, line, 0), w.at[0, my_head])
    for k, (line, w) in enumerate(downs):
        local.start(('wd', k), cols_of(wd, line, 0), w.at[0, pos.c])
    for j in HALVES:
        local.start(('wgu', j), gate_up_block(j, here), gate_up_place(j))
    barrier([pos.dev(*o) for o in offs] + [pos.partner])

    for o in offs:
        m.start(('tok', o), tok, tok_all.at[slot_of(-o[0], -o[1])], pos.dev(*o))
    m.start('table', table, tbl.at[pos.c], pos.partner)
    to_send = list(offs)

    def send_gate_up(n):
        for _ in range(min(n, len(to_send))):
            o = to_send.pop(0)
            for j in HALVES:
                m.start(('wgu', j, o), gate_up_block(j, pos.chip(*o)), gate_up_place(j), pos.dev(*o))

    send_gate_up(3)
    blank = jnp.zeros((len(STEPS), LANES - rows, colb), bf16)
    for w in (wo_x, wo_y):
        for hd in HALVES:
            w[:, hd * LANES + rows:(hd + 1) * LANES, :] = blank
    block = 2 * head_dim
    for p in range(n_slots):
        pieces = [wqkv[:, (j * n_slots + p) * block:(j * n_slots + p + 1) * block] for j in range(3)]
        wq_out[p] = jnp.concatenate(pieces + [gains[...]], axis=1)
    for o in offs:
        m.start(('wq', o), wq_out.at[pos.chip(*o)], wq.at[my_rows], pos.dev(*o))
    for k, (line, ctx, w, *_) in enumerate(lines):
        for t in AWAY:
            m.start(('wo', k, t), cols_of(wo, line, t), w.at[slot_back(t), my_head], line.dev(t))
    wq[my_rows, :] = wq_out[here]

    local.wait('tok')
    for o in offs:
        m.recv(('tok', o))
    for s in range(n_slots):
        column = jnp.transpose(tok_all[s].astype(f32))
        tok_col[pl.ds(s * seq, seq), :] = column[:seq, 0:1]
    local.wait('table')
    m.recv('table')
    group = hot.shape[1]
    for g in range(n_slots * seq // group):
        mine_rows = pl.ds(g * group, group)
        for cc in HALVES:
            ids = lax.broadcasted_iota(jnp.int32, (group, table_rows), 1) + (here * 2 + cc) * table_rows
            hot[cc] = jnp.where(tok_col[mine_rows, :] == ids.astype(f32), 1.0, 0.0).astype(bf16)

        @pl.loop(0, len(tiles(width)))
        def _(i):
            cols = tile_of(i)
            part[mine_rows, cols] = sum(jnp.dot(hot[cc], tbl[cc, :, cols], preferred_element_type=f32)
                                        for cc in HALVES).astype(bf16)

    scatter = Scatter(pos, m, part, recv_buf, seq, width)
    scatter.begin()

    def forward(name, ref):
        m.start(('to partner', name), ref, ref, pos.partner)

    forward(('wq', 0), wq.at[my_rows])
    for o in offs:
        m.recv(('wq', o))
        forward(('wq', o), wq.at[pl.ds(pl.multiple_of(pos.dev(-o[0], -o[1]) * rows, CHUNK), rows)])
    for o in [0] + offs:
        m.recv(('to partner', ('wq', o)))
    qkv_width = 3 * block
    for lo, n in tiles(width, LANES):
        square = jnp.transpose(wq[pl.ds(lo, n), qkv_width // LANES * LANES:].astype(f32))
        gain_rows[:, lo:lo + n] = square[qkv_width % LANES:qkv_width % LANES + gain_rows.shape[0], :]

    scatter.finish(lambda i: send_gate_up(1 if 5 < i < 14 else 0))

    @pl.loop(0, seq // CHUNK)
    def _(i):
        h_all[chunk(i), :] = norm_rows(part[chunk(i), :].astype(f32), gain_rows[0:1, :])

    def attend(first, n):
        for lo, size in tiles(proj.shape[1]):
            proj[pl.ds(0, n * seq), lo:lo + size] = jnp.dot(
                h_all[pl.ds(first * seq, n * seq), :], wq[:, lo:lo + size], preferred_element_type=f32)
        lane = lax.broadcasted_iota(jnp.int32, (seq, LANES), 1)
        causal = lax.broadcasted_iota(jnp.int32, (seq, seq), 0) >= lax.broadcasted_iota(jnp.int32, (seq, seq), 1)
        turn = head_dim // 2

        def wide(u):
            return jnp.concatenate([u, jnp.zeros((seq, LANES - head_dim), u.dtype)], axis=1)

        def rope(u):
            u = wide(u)
            other = jnp.where(lane < turn, pltpu.roll(u, LANES - turn, 1), pltpu.roll(u, turn, 1))
            return (u * cos2[...] + other * sin2[...]).astype(bf16)

        for lo, size in tiles(n, 2):
            heads = [(s, hd) for s in range(lo, lo + size) for hd in HALVES]

            def cut(s, j, hd):
                at = (2 * j + hd) * head_dim
                return proj[pl.ds(s * seq, seq), at:at + head_dim]

            q, k = ([rope(cut(s, j, hd)) for s, hd in heads] for j in HALVES)
            v = [cut(s, 2, hd).astype(bf16) for s, hd in heads]
            scores = [lax.dot_general(a, b, (((1,), (1,)), ((), ())), preferred_element_type=f32) for a, b in zip(q, k)]
            scores = [jnp.where(causal, u * (head_dim ** -0.5), -jnp.inf) for u in scores]
            e = [jnp.exp(u - jnp.max(u, axis=-1, keepdims=True)) for u in scores]
            probs = [(u / jnp.sum(u, axis=-1, keepdims=True)).astype(bf16) for u in e]
            context = [wide(jnp.dot(p, u, preferred_element_type=f32).astype(bf16)) for p, u in zip(probs, v)]
            for i, (s, hd) in enumerate(heads):
                a, b = SLOTS[first + s]
                yq, xq = line_y.index(a), line_x.index(b)
                at = slice(hd * LANES, (hd + 1) * LANES)
                ctx_x[0, pl.ds(pl.multiple_of((yq * pos.side + xq) * half, half), half), at] = context[i][:half]
                ctx_y[0, pl.ds(pl.multiple_of((xq * pos.side + yq) * half, half), half), at] = context[i][half:]
                if hd == 1:
                    pair = [u[:, :head_dim] for u in k[i - 1:i + 1] + v[i - 1:i + 1]]
                    packed[first + s] = jnp.concatenate(pair, axis=1)

    gather = Gather(pos, m, lambda s, lo, n: h_all.at[pl.ds(s * seq, seq), pl.ds(lo, n)], width)
    local.wait(*[(name, k) for name in ('wo', 'wd', 'wgu') for k in HALVES])
    forward('wgu', wgu_all.at[here, pos.c])
    for k, (line, ctx, w, *_) in enumerate(lines):
        forward(('wo', k, 0), w.at[0, my_head])
        forward(('wd', k, 0), downs[k][1].at[0, pos.c])
        for t in AWAY:
            m.recv(('wo', k, t))
            forward(('wo', k, t), w.at[slot_back(t), my_head])

    arrived = list(offs)

    def forward_gate_up(n):
        for _ in range(min(n, len(arrived))):
            o = arrived.pop(0)
            for j in HALVES:
                m.recv(('wgu', j, o))
            forward(('wgu', o), wgu_all.at[pos.chip(-o[0], -o[1]), pos.c])

    gather.begin()
    attend(0, 5)
    for a in (-1, 1):
        gather.second_forward(a)
    attend(5, 4)
    forward_gate_up(n_slots - 1 - len(to_send))
    gather.second_forward(2)
    for k, line in enumerate((line_x, line_y)):
        for t in AWAY:
            m.start(('x', k, t), part.at[pl.ds(k * half, half), line.lanes(t, colb)], x_parts.at[k, slot_back(t)], line.dev(t))
        x_parts[k, 0] = part[pl.ds(k * half, half), line.lanes(0, colb)]
    send_gate_up(n_slots)
    gather.last(0)
    attend(9, 2)
    for a in (-1, 1):
        gather.last(a)
    attend(11, 4)
    gather.last(2)
    attend(15, 1)

    every = pl.ds(*whole(ctx_x.shape[1]))
    for line, ctx, *_ in lines:
        line.share(ctx, 'ctx', every)
    for line, ctx, *_ in lines:
        line.share_on(ctx, 'ctx', lambda cut: pl.ds(*cut(ctx_x.shape[1])))

    def send_kv():
        local.start('kv', packed.at[0], mine.at[here])
        for s, o in enumerate(SLOTS[1:]):
            m.start(('kv', o), packed.at[s + 1], mine.at[here], pos.dev(*o))

    def send_down(k):
        line, w = downs[k]
        for t in AWAY:
            m.start(('wd', k, t), cols_of(wd, line, t), w.at[slot_back(t), pos.c], line.dev(t))

    def forward_down(k):
        line, w = downs[k]
        for t in AWAY:
            m.recv(('wd', k, t))
            forward(('wd', k, t), w.at[slot_back(t), pos.c])

    send_down(0)
    send_kv()
    for k in HALVES:
        for t in STEPS:
            m.recv(('to partner', ('wo', k, t)))

    def project(ctx, w, total, first, last):
        @pl.loop(0, len(tiles(colb)))
        def _(i):
            cols = tile_of(i)
            acc = sum(jnp.dot(ctx[j], w[j, :, cols], preferred_element_type=f32) for j in range(first, last))
            total[:, cols] = total[:, cols] + acc if first else acc

    n_rows = sum_x.shape[0] // 4
    for line, ctx, w, total, *_ in lines:
        project(ctx, w, total, 0, 3)
    for line, ctx, w, total, other, got in lines:
        line.share_last('ctx')
        project(ctx, w, total, 3, 4)
        other.scatter_begin(total, got, n_rows)
    send_down(1)
    for line, ctx, w, total, other, got in lines:
        other.scatter_middle(total, got, n_rows)
    forward_gate_up(n_slots)
    forward_down(0)
    for k, (line, ctx, w, total, other, got) in enumerate(lines):
        other.scatter_last(total, got, n_rows)
        for t in AWAY:
            m.recv(('x', k, t))
        for i, t in enumerate(STEPS):
            lo = pl.multiple_of(line.index(t) * half, half)
            x_mid[k, pl.ds(lo, half), :] = (x_parts[k, i].astype(f32) + total[other.block(0, n_rows, lo, half), :]).astype(bf16)
    forward_down(1)
    local.wait('kv')

    m.finish()


def mlp_kernel(piece, gain_rows, wgu_hbm, wdx_hbm, wdy_hbm, out,
               mid_x, mid_y, normed, wgu, wd_x, wd_y, act_x, act_y, sum_x, sum_y, got_x, got_y, fin, sems, l_sem):
    pos = Place(4)
    f32, bf16 = jnp.float32, jnp.bfloat16
    width = out.shape[1]
    n_rows, colb = piece.shape[1:]
    half_rows = n_rows // 4
    ffb = act_x.shape[2]
    m, local = Msgs(sems), Local(l_sem)
    line_x, line_y = Line(pos, m, 'x'), Line(pos, m, 'y')
    sets = ((mid_x, line_y, line_x, act_x, wd_x, sum_x, got_x), (mid_y, line_x, line_y, act_y, wd_y, sum_y, got_y))

    def blk(p, lo, n):
        y, x = lax.div(p, pos.side), lax.rem(p, pos.side)
        r, c, ref, lo = (y, x, mid_x, lo) if lo < colb else (x, y, mid_y, lo - colb)
        return ref.at[pl.ds(pl.multiple_of(r * n_rows, n_rows), n_rows), pl.ds(pl.multiple_of(c * colb + lo, LANES), n)]

    here = pos.chip(0, 0)
    for k in HALVES:
        local.start(('piece', k), piece.at[k], blk(here, k * colb, colb))
    local.start('wgu', wgu_hbm, wgu)
    local.start(('wd', 0), wdx_hbm, wd_x)
    local.start(('wd', 1), wdy_hbm, wd_y)
    barrier([line.dev(t) for line in (line_x, line_y) for t in AWAY])
    local.wait(('piece', 0), ('piece', 1))
    gather = Gather(pos, m, blk, 2 * colb, by_chip=True)

    def gate_up(v, some=HALVES):
        for k in some:
            mid, sline, *_ = sets[k]

            @pl.loop(0, n_rows // CHUNK, unroll=2)
            def _(j):
                x = mid[sline.block(v, n_rows, j * CHUNK, CHUNK), :].astype(f32)
                normed[chunk(j, k * n_rows), :] = norm_rows(x, gain_rows[1:2, :])

        @pl.loop(0, len(tiles(ffb)))
        def _(i):
            mine = pl.ds(some[0] * n_rows, len(some) * n_rows)
            g, u = (jnp.dot(normed[mine, :], wgu[:, :, :, tile_of(i, base)].reshape(width, -1), preferred_element_type=f32)
                    for base in (0, ffb))
            a = (jax.nn.silu(g) * u).astype(bf16)
            for i_k, k in enumerate(some):
                mid, sline, gline, act, *_ = sets[k]
                act[0, sline.block(v, n_rows), tile_of(i)] = a[i_k * n_rows:(i_k + 1) * n_rows]

    def share(v, some=HALVES):
        for mid, sline, gline, act, *_ in (sets[k] for k in some):
            rows = sline.block(v, n_rows)
            gline.share(act, v, rows)
            if v == 2:
                gline.start(('direct', v), act.at[0, rows], act.at[slot_back(2), rows], 2)

    def share_on(v):
        for mid, sline, gline, act, *_ in sets:
            gline.share_on(act, v, lambda cut: sline.block(v, n_rows, *cut(n_rows)))

    def down(v):
        at = STEPS.index(v)
        for mid, sline, gline, act, w, total, got in sets:
            if v == 2:
                for sign in SIGNS:
                    gline.recv('share', sign, v)
                gline.recv('direct', v)
            else:
                gline.share_last(v)

            @pl.loop(0, len(tiles(colb)))
            def _(i):
                total[at, :, tile_of(i)] = sum(
                    jnp.dot(act[t, sline.block(v, n_rows), :], w[t, :, :, tile_of(i)].reshape(ffb, -1), preferred_element_type=f32)
                    for t in range(len(STEPS)))

            if v != 0:
                sline.start(('sum', v), total.at[at], got.at[slot_back(v) - 1], v)

    gather.begin()
    local.wait('wgu')
    gate_up(0)
    share(0)
    gather.forward()
    gate_up(1)
    share(1)
    share_on(0)
    gate_up(-1)
    share(-1)
    share_on(1)
    for a in STEPS:
        gather.last(a)
    share_on(-1)
    for k in HALVES:
        gate_up(2, (k,))
        share(2, (k,))
    local.wait(('wd', 0), ('wd', 1))
    for v in (1, -1, 2, 0):
        down(v)
    for k, (mid, sline, gline, act, w, total, got) in enumerate(sets):
        for v in AWAY:
            sline.recv('sum', v)
        cols = gline.lanes(0, colb)

        @pl.loop(0, n_rows // CHUNK)
        def _(j):
            rows = chunk(j)
            x = mid[sline.block(0, n_rows, j * CHUNK, CHUNK), cols].astype(f32)
            fin[k, rows, :] = (x + (total[0, rows, :] + sum(got[i, rows, :] for i in range(len(AWAY))))).astype(bf16)

        mine_rows = pl.ds(k * half_rows, half_rows)
        for t in AWAY:
            gline.start(('out', t), fin.at[k, gline.block(t, half_rows)], out.at[mine_rows, cols], t)
        out[mine_rows, cols] = fin[k, gline.block(0, half_rows), :]
    m.finish()


def dma(n):
    return pltpu.SemaphoreType.DMA((n,))


def dma2(n):
    return pltpu.SemaphoreType.DMA((2, n))


def params(cid):
    return pltpu.CompilerParams(collective_id=cid, has_side_effects=True, vmem_limit_bytes=VMEM_LIMIT)


def rope_tables(rope_scale, seq_len, lanes):
    half_dim = rope_scale.shape[0]
    freq_expo = jnp.arange(half_dim, dtype=jnp.float32) * (2.0 / (2 * half_dim))
    inv_freq = 1.0 / (rope_scale * jnp.power(ROPE_THETA, freq_expo))
    angles = jnp.arange(seq_len, dtype=jnp.float32)[:, None] * inv_freq[None, :]
    cos, sin = jnp.cos(angles), jnp.sin(angles)
    rest = jnp.zeros((seq_len, lanes - 2 * half_dim), jnp.float32)
    return jnp.concatenate([cos, cos, rest], axis=1), jnp.concatenate([-sin, sin, rest], axis=1)


def solution(mesh):
    batch_axes = ('dp', AXIS)
    row_spec = P(AXIS, None)
    n_dev = mesh.shape[AXIS]
    chips = n_dev // 2
    n_off = chips - 1

    def device_step(tokens, embed_table, norm_attn, w_qkv, w_out, norm_mlp, w_gate_up, w_down, rope_scale):
        f32, bf16 = jnp.float32, jnp.bfloat16
        seq = tokens.shape[1]
        rows, d_model = w_out.shape
        head_dim = 2 * rope_scale.shape[0]
        ffb = w_gate_up.shape[1] // (2 * chips)
        qkv_width = w_qkv.shape[1] // chips
        wide = pl.cdiv(qkv_width + 2, LANES) * LANES
        toks, half_toks, colb = chips * seq, chips * seq // 2, d_model // 4
        tok = jnp.zeros((8, LANES), jnp.int32) + jnp.pad(tokens, ((0, 0), (0, LANES - seq)))
        column = lax.broadcasted_iota(jnp.int32, (rows, wide - qkv_width), 1)
        gains = (jnp.where(column == 0, norm_attn[:, None], 0) + jnp.where(column == 1, norm_mlp[:, None], 0)).astype(bf16)
        cos2, sin2 = rope_tables(rope_scale, seq, LANES)
        vmem = pl.BlockSpec(memory_space=pltpu.VMEM)
        shape = jax.ShapeDtypeStruct

        def buf(*dims, dtype=bf16):
            return pltpu.VMEM(dims, dtype)

        wgu_shape = (chips, 2, rows, 2 * ffb)
        wd_shape = (4, 2, ffb // 2, colb)
        kv_shape = (chips, seq, 4 * head_dim)
        sum_blocks = half_toks // 4
        x_mid, mine, wgu_all, wd_x, wd_y, gain_rows = pl.pallas_call(
            front_kernel, name='front',
            out_shape=(shape((2, sum_blocks, colb), bf16), shape(kv_shape, bf16), shape(wgu_shape, bf16),
                       shape(wd_shape, bf16), shape(wd_shape, bf16), shape((8, d_model), f32)),
            in_specs=[ANY] + [vmem] * 4 + [ANY] * 4, out_specs=(vmem, ANY, ANY, ANY, ANY, vmem),
            scratch_shapes=[buf(*kv_shape), buf(chips, 8, LANES, dtype=jnp.int32), buf(toks, 1, dtype=f32), buf(2, *embed_table.shape),
                            buf(2, toks // 4, embed_table.shape[0]), buf(toks, d_model), buf(seq, d_model * n_off),
                            buf(toks, d_model), buf(chips, rows, wide), buf(d_model, wide), buf(2, 4, seq // 2, colb),
                            buf(5 * seq, wide, dtype=f32)]
                           + [buf(4, half_toks, 2 * LANES)] * 2 + [buf(4, 2 * LANES, colb)] * 2
                           + [buf(half_toks, colb, dtype=f32)] * 2 + [buf(3 * sum_blocks, colb, dtype=f32)] * 2
                           + [dma2(240), dma(9)],
            compiler_params=params(1),
        )(tok, gains, w_qkv, cos2, sin2, w_gate_up, w_out, w_down, embed_table)

        layer_out = pl.pallas_call(
            mlp_kernel, name='mlp',
            out_shape=shape((seq, d_model), bf16),
            in_specs=[ANY, vmem] + [ANY] * 3, out_specs=vmem,
            scratch_shapes=[buf(half_toks, d_model)] * 2 + [buf(half_toks // 2, d_model), buf(*wgu_shape)]
                           + [buf(*wd_shape)] * 2 + [buf(4, half_toks, ffb)] * 2
                           + [buf(4, sum_blocks, colb, dtype=f32)] * 2 + [buf(3, sum_blocks, colb, dtype=f32)] * 2
                           + [buf(2, sum_blocks, colb), dma2(84), dma(5)],
            compiler_params=params(2),
        )(x_mid, gain_rows, wgu_all, wd_x, wd_y)

        def by_head(lo):
            part = mine[:, :, lo:lo + 2 * head_dim].transpose(1, 0, 2)
            return part.reshape(1, seq, 2 * chips, head_dim)

        key_own, val_own = by_head(0), by_head(2 * head_dim)
        return layer_out[None], key_own, val_own

    return jax.shard_map(
        device_step,
        mesh=mesh,
        in_specs=(P(batch_axes, None), row_spec, P(AXIS), row_spec, row_spec, P(AXIS), row_spec, row_spec, P(None)),
        out_specs=(P(batch_axes, None, None), P(batch_axes, None, None, None), P(batch_axes, None, None, None)),
        check_vma=False,
    )
```

```python
import jax
import jax.numpy as jnp
from jax import lax
from jax.experimental import pallas as pl
from jax.experimental.pallas import tpu as pltpu
from jax.sharding import PartitionSpec as P

NORM_EPS = 1e-5
ROPE_THETA = 10000.0
AXIS = 'fsdp'
MESH = pl.DeviceIdType.MESH
ANY = pl.BlockSpec(memory_space=pl.ANY)
VMEM_LIMIT = 60 * 1024 * 1024


class Place:
    def __init__(self, side):
        me = lax.axis_index(AXIS)
        self.side = side
        self.c = lax.rem(me, 2)
        chip = lax.div(me, 2)
        self.y = lax.div(chip, side)
        self.x = lax.rem(chip, side)
        self.me = me
        self.partner = me + 1 - 2 * self.c

    def chip(self, dy, dx):
        s = self.side
        return lax.rem(self.y + dy + s, s) * s + lax.rem(self.x + dx + s, s)

    def dev(self, dy, dx):
        return self.chip(dy, dx) * 2 + self.c


def barrier(devices):
    sem = pltpu.get_barrier_semaphore()
    for d in devices:
        pl.semaphore_signal(sem, inc=1, device_id={AXIS: d}, device_id_type=MESH)
    pl.semaphore_wait(sem, len(devices))


def remote(src, dst, sems, i, dev):
    send, recv = (sems.at[k, i] for k in (0, 1))
    return pltpu.make_async_remote_copy(src_ref=src, dst_ref=dst, send_sem=send, recv_sem=recv,
                                        device_id={AXIS: dev}, device_id_type=MESH)


class Msgs:
    def __init__(self, sems):
        self.sems, self.copies, self.received = sems, {}, set()

    def start(self, name, src, dst, dev):
        assert name not in self.copies
        self.copies[name] = remote(src, dst, self.sems, len(self.copies), dev)
        self.copies[name].start()

    def recv(self, name):
        self.received.add(name)
        self.copies[name].wait_recv()

    def finish(self):
        for name in self.copies:
            if name not in self.received:
                self.recv(name)
            self.copies[name].wait_send()


class Local:
    def __init__(self, sems):
        self.sems, self.copies = sems, {}

    def start(self, name, src, dst):
        self.copies[name] = pltpu.make_async_copy(src, dst, self.sems.at[len(self.copies)])
        self.copies[name].start()

    def wait(self, *names):
        for name in names:
            self.copies[name].wait()


STEPS = (0, 1, -1, 2)
AWAY = STEPS[1:]
SLOTS = sorted(((a, b) for a in STEPS for b in STEPS), key=lambda o: (2 in o, abs(o[0]) + abs(o[1])))


def slot_of(a, b):
    return SLOTS.index(((a + 1) % 4 - 1, (b + 1) % 4 - 1))


def slot_back(t):
    return STEPS.index(2 if t == 2 else -t)


def swap_if(h, a, b):
    return (b, a) if h == 0 else (a, b)


HALVES = (0, 1)
SIGNS = (1, -1)
LANES = 128
CHUNK = 16


def whole(n):
    return 0, n


def part_for(sign):
    return lambda n: (0 if sign > 0 else n // 2, n // 2)


def chunk(i, base=0):
    return pl.ds(pl.multiple_of(base + i * CHUNK, CHUNK), CHUNK)


class Gather:
    def __init__(self, pos, m, blk, width, by_chip=False):
        self.pos, self.m, self.blk, self.half, self.by_chip = pos, m, blk, width // 2, by_chip

    def send(self, h, name, a, b, cut, ta, tb):
        lo, n = cut(self.half)
        lo += self.half * h
        if self.by_chip:
            src = dst = self.blk(self.pos.chip(*swap_if(h, a, b)), lo, n)
        else:
            src = self.blk(slot_of(*swap_if(h, a, b)), lo, n)
            dst = self.blk(slot_of(*swap_if(h, a - ta, b - tb)), lo, n)
        self.m.start((h,) + name, src, dst, self.pos.dev(*swap_if(h, ta, tb)))

    def second(self, h, a):
        for sign in SIGNS:
            self.send(h, ('second', sign, a), a, 0, whole, 0, sign)

    def second_forward(self, a):
        for h in HALVES:
            for sign in SIGNS:
                self.m.recv((h, 'second', sign, a))
                self.send(h, ('second on', sign, a), a, -sign, part_for(sign), 0, sign)

    def last(self, a):
        for h in HALVES:
            for sign in SIGNS:
                self.m.recv((h, 'second on', sign, a))

    def begin(self):
        for h in HALVES:
            for sign in SIGNS:
                self.send(h, ('first', sign), 0, 0, whole, sign, 0)
        for h in HALVES:
            self.second(h, 0)
        for sign in SIGNS:
            for h in HALVES:
                self.m.recv((h, 'first', sign))
                self.send(h, ('first on', sign), -sign, 0, part_for(sign), sign, 0)
                self.second(h, -sign)
        self.second_forward(0)
        for h in HALVES:
            for sign in SIGNS:
                self.m.recv((h, 'first on', sign))
            self.second(h, 2)

    def forward(self):
        for a in AWAY:
            self.second_forward(a)


class Scatter:
    def __init__(self, pos, m, part, recv_buf, rows, width):
        self.pos, self.m, self.part, self.recv_buf = pos, m, part, recv_buf
        self.rows, self.half, self.used, self.places = rows, width // 2, 0, {}

    def send(self, h, name, a, b, cut, ta, tb):
        lo, n = cut(self.half)
        key = (h,) + name
        there = self.places[key] = pl.ds(self.used, n)
        self.used += n
        src = self.part.at[pl.ds(slot_of(*swap_if(1 - h, a, b)) * self.rows, self.rows), pl.ds(self.half * h + lo, n)]
        self.m.start(key, src, self.recv_buf.at[:, there], self.pos.dev(*swap_if(1 - h, ta, tb)))

    def recv_add(self, h, name, a, b, cut):
        lo, n = cut(self.half)
        key = (h,) + name
        self.m.recv(key)
        there, here = self.places[key], pl.ds(self.half * h + lo, n)
        base = slot_of(*swap_if(1 - h, a, b)) * self.rows

        @pl.loop(0, self.rows // CHUNK)
        def _(i):
            mine, theirs = chunk(i, base), chunk(i)
            self.part[mine, here] = self.part[mine, here] + self.recv_buf[theirs, there]

    def begin(self):
        for b in AWAY[::-1] + (0,):
            for h in HALVES:
                for sign in SIGNS:
                    self.send(h, ('first on', sign, b), 2, b, part_for(sign), sign, 0)

    def finish(self, hook):
        calls = iter(range(len(SLOTS)))
        order = AWAY[::-1] + (0,)
        for b in order:
            for h in HALVES:
                for sign in SIGNS:
                    self.recv_add(h, ('first on', sign, b), sign, b, part_for(sign))
                    self.send(h, ('first', sign, b), sign, b, whole, sign, 0)
                hook(next(calls))
        for b in order:
            for h in HALVES:
                for sign in SIGNS:
                    self.recv_add(h, ('first', sign, b), 0, b, whole)
                if b == 2:
                    for sign in SIGNS:
                        self.send(h, ('second on', sign), 0, b, part_for(sign), 0, sign)
                elif b == 0:
                    for sign in SIGNS:
                        self.recv_add(h, ('second', sign), 0, b, whole)
                else:
                    self.recv_add(h, ('second on', b), 0, b, part_for(b))
                    self.send(h, ('second', b), 0, b, whole, 0, b)
                hook(next(calls))


class Line:
    def __init__(self, pos, m, axis):
        self.pos, self.m, self.axis = pos, m, axis

    def dev(self, t):
        return self.pos.dev(0, t) if self.axis == 'x' else self.pos.dev(t, 0)

    def index(self, t):
        side = self.pos.side
        return lax.rem((self.pos.x if self.axis == 'x' else self.pos.y) + t + side, side)

    def block(self, t, n, lo=0, size=None):
        return pl.ds(pl.multiple_of(self.index(t) * n + lo, CHUNK), n if size is None else size)

    def lanes(self, t, n):
        return pl.ds(pl.multiple_of(self.index(t) * n, LANES), n)

    def start(self, key, src, dst, t):
        self.m.start((self.axis,) + key, src, dst, self.dev(t))

    def recv(self, *key):
        self.m.recv((self.axis,) + key)

    def share(self, buf, v, rows):
        for sign in SIGNS:
            self.start(('share', sign, v), buf.at[0, rows], buf.at[slot_back(sign), rows], sign)

    def share_on(self, buf, v, rows_of):
        for sign in SIGNS:
            self.recv('share', sign, v)
            rows = rows_of(part_for(sign))
            self.start(('share on', sign, v), buf.at[slot_back(sign), rows], buf.at[slot_back(2), rows], sign)

    def share_last(self, v):
        for sign in SIGNS:
            self.recv('share on', sign, v)

    def scatter_begin(self, part, recv_buf, rows):
        for sign in SIGNS:
            cols = pl.ds(*part_for(sign)(part.shape[1]))
            self.start(('sum on', sign), part.at[self.block(2, rows), cols], recv_buf.at[pl.ds(0, rows), cols], sign)

    def add(self, part, recv_buf, t, rows, first, cols):
        @pl.loop(0, rows // CHUNK)
        def _(i):
            mine = self.block(t, rows, i * CHUNK, CHUNK)
            part[mine, cols] = part[mine, cols] + recv_buf[chunk(i, first * rows), cols]

    def scatter_middle(self, part, recv_buf, rows):
        for sign in SIGNS:
            self.recv('sum on', sign)
            self.add(part, recv_buf, sign, rows, 0, pl.ds(*part_for(sign)(part.shape[1])))
            to = recv_buf.at[pl.ds(slot_back(sign) * rows, rows)]
            self.start(('sum', sign), part.at[self.block(sign, rows)], to, sign)

    def scatter_last(self, part, recv_buf, rows):
        for sign in SIGNS:
            self.recv('sum', sign)
            self.add(part, recv_buf, 0, rows, slot_back(sign), pl.ds(*whole(part.shape[1])))


def offsets():
    return SLOTS[5:9] + SLOTS[1:5] + SLOTS[15:] + SLOTS[9:15]


def norm_rows(x, gain):
    inv = lax.rsqrt(jnp.mean(x * x, axis=-1, keepdims=True) + NORM_EPS)
    return (x * inv * gain).astype(jnp.bfloat16)


def tiles(n, tile=256):
    return [(lo, min(tile, n - lo)) for lo in range(0, n, tile)]


def tile_of(i, base=0, tile=256):
    return pl.ds(pl.multiple_of(base + i * tile, LANES), tile)


def front_kernel(tok, gain_attn, gain_mlp, wqkv, cos2, sin2, wgu, wo, wd, table,
                 x_mid, mine, wgu_all, wd_x, wd_y, gain_rows,
                 packed, tok_own, gain_own, tok_all, tok_col, tbl, hot, part, recv_buf, h_all, wq_out, wq, x_parts, proj,
                 ctx_x, ctx_y, wo_x, wo_y, sum_x, sum_y, got_x, got_y, sems, l_sem):
    f32, bf16 = jnp.float32, jnp.bfloat16
    pos = Place(4)
    m, local = Msgs(sems), Local(l_sem)
    line_x, line_y = Line(pos, m, 'x'), Line(pos, m, 'y')
    offs = offsets()
    here = pos.chip(0, 0)
    rows = wq_out.shape[1]
    seq, width = packed.shape[1], h_all.shape[1]
    n_slots = len(SLOTS)
    half, colb = seq // 2, width // 4
    ffb = wgu_all.shape[-1] // 2
    head_dim = packed.shape[2] // 4
    table_rows = table.shape[0]
    my_head = pl.ds(pl.multiple_of(pos.c * LANES, LANES), rows)
    my_rows = pl.ds(pl.multiple_of(pos.me * rows, CHUNK), rows)
    lines = ((line_x, ctx_x, wo_x, sum_x, line_y, got_x), (line_y, ctx_y, wo_y, sum_y, line_x, got_y))
    downs = ((line_x, wd_x), (line_y, wd_y))

    def cols_of(w, line, t):
        return w.at[:, line.lanes(t, colb)]

    def gate_up_block(j, chip):
        return wgu.at[:, pl.ds(pl.multiple_of((j * n_slots + chip) * ffb, LANES), ffb)]

    def gate_up_place(j):
        return wgu_all.at[here, pos.c, :, pl.ds(j * ffb, ffb)]

    local.start('table', table, tbl.at[pos.c])
    for k, (line, ctx, w, *_) in enumerate(lines):
        local.start(('wo', k), cols_of(wo, line, 0), w.at[0, my_head])
    for k, (line, w) in enumerate(downs):
        local.start(('wd', k), cols_of(wd, line, 0), w.at[0, pos.c])
    for j in HALVES:
        local.start(('wgu', j), gate_up_block(j, here), gate_up_place(j))
    tok_own[...] = jnp.zeros_like(tok_own)
    tok_own[0:1, 0:seq] = tok[...]
    tok_all[0] = tok_own[...]
    barrier([pos.dev(*o) for o in offs] + [pos.partner])

    for o in offs:
        m.start(('tok', o), tok_own, tok_all.at[slot_of(-o[0], -o[1])], pos.dev(*o))
    m.start('table', table, tbl.at[pos.c], pos.partner)
    to_send = list(offs)

    def send_gate_up(n):
        for _ in range(min(n, len(to_send))):
            o = to_send.pop(0)
            for j in HALVES:
                m.start(('wgu', j, o), gate_up_block(j, pos.chip(*o)), gate_up_place(j), pos.dev(*o))

    send_gate_up(6)
    blank = jnp.zeros((len(STEPS), LANES - rows, colb), bf16)
    for w in (wo_x, wo_y):
        for hd in HALVES:
            w[:, hd * LANES + rows:(hd + 1) * LANES, :] = blank
    block = 2 * head_dim
    gain_own[...] = jnp.zeros_like(gain_own)
    for i, gain in enumerate((gain_attn, gain_mlp)):
        gain_own[i:i + 1, 0:rows] = gain[...].astype(f32)
    gains = jnp.transpose(gain_own[...])[:rows].astype(bf16)
    gains = jnp.concatenate([gains, jnp.zeros((rows, wq.shape[1] - 3 * block - gains.shape[1]), bf16)], axis=1)
    for p in range(n_slots):
        pieces = [wqkv[:, (j * n_slots + p) * block:(j * n_slots + p + 1) * block] for j in range(3)]
        wq_out[p] = jnp.concatenate(pieces + [gains], axis=1)
    for o in offs:
        m.start(('wq', o), wq_out.at[pos.chip(*o)], wq.at[my_rows], pos.dev(*o))
    for k, (line, ctx, w, *_) in enumerate(lines):
        for t in AWAY:
            m.start(('wo', k, t), cols_of(wo, line, t), w.at[slot_back(t), my_head], line.dev(t))
    wq[my_rows, :] = wq_out[here]

    for o in offs:
        m.recv(('tok', o))
    for s in range(n_slots):
        column = jnp.transpose(tok_all[s].astype(f32))
        tok_col[pl.ds(s * seq, seq), :] = column[:seq, 0:1]
    local.wait('table')
    m.recv('table')
    group = hot.shape[1]
    for g in range(n_slots * seq // group):
        mine_rows = pl.ds(g * group, group)
        for cc in HALVES:
            ids = lax.broadcasted_iota(jnp.int32, (group, table_rows), 1) + (here * 2 + cc) * table_rows
            hot[cc] = jnp.where(tok_col[mine_rows, :] == ids.astype(f32), 1.0, 0.0).astype(bf16)

        @pl.loop(0, len(tiles(width)))
        def _(i):
            cols = tile_of(i)
            part[mine_rows, cols] = sum(jnp.dot(hot[cc], tbl[cc, :, cols], preferred_element_type=f32)
                                        for cc in HALVES).astype(bf16)

    scatter = Scatter(pos, m, part, recv_buf, seq, width)
    scatter.begin()

    def forward(name, ref):
        m.start(('to partner', name), ref, ref, pos.partner)

    forward(('wq', 0), wq.at[my_rows])
    for o in offs:
        m.recv(('wq', o))
        forward(('wq', o), wq.at[pl.ds(pl.multiple_of(pos.dev(-o[0], -o[1]) * rows, CHUNK), rows)])
    for o in [0] + offs:
        m.recv(('to partner', ('wq', o)))
    qkv_width = 3 * block
    for lo, n in tiles(width, LANES):
        square = jnp.transpose(wq[pl.ds(lo, n), qkv_width // LANES * LANES:].astype(f32))
        gain_rows[:, lo:lo + n] = square[qkv_width % LANES:qkv_width % LANES + gain_rows.shape[0], :]

    scatter.finish(lambda i: send_gate_up(1 if 5 < i < 14 else 0))

    @pl.loop(0, seq // CHUNK)
    def _(i):
        h_all[chunk(i), :] = norm_rows(part[chunk(i), :].astype(f32), gain_rows[0:1, :])

    def attend(first, n):
        for lo, size in tiles(proj.shape[1]):
            proj[pl.ds(0, n * seq), lo:lo + size] = jnp.dot(
                h_all[pl.ds(first * seq, n * seq), :], wq[:, lo:lo + size], preferred_element_type=f32)
        lane = lax.broadcasted_iota(jnp.int32, (seq, LANES), 1)
        causal = lax.broadcasted_iota(jnp.int32, (seq, seq), 0) >= lax.broadcasted_iota(jnp.int32, (seq, seq), 1)
        turn = head_dim // 2

        def wide(u):
            return jnp.concatenate([u, jnp.zeros((seq, LANES - head_dim), u.dtype)], axis=1)

        def rope(u):
            u = wide(u)
            other = jnp.where(lane < turn, pltpu.roll(u, LANES - turn, 1), pltpu.roll(u, turn, 1))
            return (u * cos2[...] + other * sin2[...]).astype(bf16)

        for lo, size in tiles(n, 2):
            heads = [(s, hd) for s in range(lo, lo + size) for hd in HALVES]

            def cut(s, j, hd):
                at = (2 * j + hd) * head_dim
                return proj[pl.ds(s * seq, seq), at:at + head_dim]

            q, k = ([rope(cut(s, j, hd)) for s, hd in heads] for j in HALVES)
            v = [cut(s, 2, hd).astype(bf16) for s, hd in heads]
            scores = [lax.dot_general(a, b, (((1,), (1,)), ((), ())), preferred_element_type=f32) for a, b in zip(q, k)]
            scores = [jnp.where(causal, u * (head_dim ** -0.5), -jnp.inf) for u in scores]
            e = [jnp.exp(u - jnp.max(u, axis=-1, keepdims=True)) for u in scores]
            probs = [(u / jnp.sum(u, axis=-1, keepdims=True)).astype(bf16) for u in e]
            context = [wide(jnp.dot(p, u, preferred_element_type=f32).astype(bf16)) for p, u in zip(probs, v)]
            for i, (s, hd) in enumerate(heads):
                a, b = SLOTS[first + s]
                yq, xq = line_y.index(a), line_x.index(b)
                at = slice(hd * LANES, (hd + 1) * LANES)
                ctx_x[0, pl.ds(pl.multiple_of((yq * pos.side + xq) * half, half), half), at] = context[i][:half]
                ctx_y[0, pl.ds(pl.multiple_of((xq * pos.side + yq) * half, half), half), at] = context[i][half:]
                if hd == 1:
                    pair = [u[:, :head_dim] for u in k[i - 1:i + 1] + v[i - 1:i + 1]]
                    packed[first + s] = jnp.concatenate(pair, axis=1)

    gather = Gather(pos, m, lambda s, lo, n: h_all.at[pl.ds(s * seq, seq), pl.ds(lo, n)], width)
    local.wait(*[(name, k) for name in ('wo', 'wd', 'wgu') for k in HALVES])
    forward('wgu', wgu_all.at[here, pos.c])
    for k, (line, ctx, w, *_) in enumerate(lines):
        forward(('wo', k, 0), w.at[0, my_head])
        forward(('wd', k, 0), downs[k][1].at[0, pos.c])
        for t in AWAY:
            m.recv(('wo', k, t))
            forward(('wo', k, t), w.at[slot_back(t), my_head])

    arrived = list(offs)

    def forward_gate_up(n):
        for _ in range(min(n, len(arrived))):
            o = arrived.pop(0)
            for j in HALVES:
                m.recv(('wgu', j, o))
            forward(('wgu', o), wgu_all.at[pos.chip(-o[0], -o[1]), pos.c])

    gather.begin()
    attend(0, 5)
    for a in (-1, 1):
        gather.second_forward(a)
    attend(5, 4)
    forward_gate_up(n_slots - 1 - len(to_send))
    gather.second_forward(2)
    for k, line in enumerate((line_x, line_y)):
        for t in AWAY:
            m.start(('x', k, t), part.at[pl.ds(k * half, half), line.lanes(t, colb)], x_parts.at[k, slot_back(t)], line.dev(t))
        x_parts[k, 0] = part[pl.ds(k * half, half), line.lanes(0, colb)]
    send_gate_up(n_slots)
    gather.last(0)
    attend(9, 2)
    for a in (-1, 1):
        gather.last(a)
    attend(11, 4)
    gather.last(2)
    attend(15, 1)

    every = pl.ds(*whole(ctx_x.shape[1]))
    for line, ctx, *_ in lines:
        line.share(ctx, 'ctx', every)
    for line, ctx, *_ in lines:
        line.share_on(ctx, 'ctx', lambda cut: pl.ds(*cut(ctx_x.shape[1])))

    def send_kv():
        local.start('kv', packed.at[0], mine.at[here])
        for s, o in enumerate(SLOTS[1:]):
            m.start(('kv', o), packed.at[s + 1], mine.at[here], pos.dev(*o))

    def send_down(k):
        line, w = downs[k]
        for t in AWAY:
            m.start(('wd', k, t), cols_of(wd, line, t), w.at[slot_back(t), pos.c], line.dev(t))

    def forward_down(k):
        line, w = downs[k]
        for t in AWAY:
            m.recv(('wd', k, t))
            forward(('wd', k, t), w.at[slot_back(t), pos.c])

    send_down(0)
    send_kv()
    for k in HALVES:
        for t in STEPS:
            m.recv(('to partner', ('wo', k, t)))

    def project(ctx, w, total, first, last):
        @pl.loop(0, len(tiles(colb)))
        def _(i):
            cols = tile_of(i)
            acc = sum(jnp.dot(ctx[j], w[j, :, cols], preferred_element_type=f32) for j in range(first, last))
            total[:, cols] = total[:, cols] + acc if first else acc

    n_rows = sum_x.shape[0] // 4
    for line, ctx, w, total, *_ in lines:
        project(ctx, w, total, 0, 3)
    for line, ctx, w, total, other, got in lines:
        line.share_last('ctx')
        project(ctx, w, total, 3, 4)
        other.scatter_begin(total, got, n_rows)
    send_down(1)
    for line, ctx, w, total, other, got in lines:
        other.scatter_middle(total, got, n_rows)
    forward_gate_up(n_slots)
    forward_down(0)
    for k, (line, ctx, w, total, other, got) in enumerate(lines):
        other.scatter_last(total, got, n_rows)
        for t in AWAY:
            m.recv(('x', k, t))
        for i, t in enumerate(STEPS):
            lo = pl.multiple_of(line.index(t) * half, half)
            x_mid[k, pl.ds(lo, half), :] = (x_parts[k, i].astype(f32) + total[other.block(0, n_rows, lo, half), :]).astype(bf16)
    forward_down(1)
    local.wait('kv')

    m.finish()


def mlp_kernel(piece, gain_rows, wgu_hbm, wdx_hbm, wdy_hbm, out,
               mid_x, mid_y, normed, wgu, wd_x, wd_y, act_x, act_y, sum_x, sum_y, got_x, got_y, fin, sems, l_sem):
    pos = Place(4)
    f32, bf16 = jnp.float32, jnp.bfloat16
    width = out.shape[1]
    n_rows, colb = piece.shape[1:]
    half_rows = n_rows // 4
    ffb = act_x.shape[2]
    m, local = Msgs(sems), Local(l_sem)
    line_x, line_y = Line(pos, m, 'x'), Line(pos, m, 'y')
    sets = ((mid_x, line_y, line_x, act_x, wd_x, sum_x, got_x), (mid_y, line_x, line_y, act_y, wd_y, sum_y, got_y))

    def blk(p, lo, n):
        y, x = lax.div(p, pos.side), lax.rem(p, pos.side)
        r, c, ref, lo = (y, x, mid_x, lo) if lo < colb else (x, y, mid_y, lo - colb)
        return ref.at[pl.ds(pl.multiple_of(r * n_rows, n_rows), n_rows), pl.ds(pl.multiple_of(c * colb + lo, LANES), n)]

    here = pos.chip(0, 0)
    for k in HALVES:
        local.start(('piece', k), piece.at[k], blk(here, k * colb, colb))
    local.start('wgu', wgu_hbm, wgu)
    local.start(('wd', 0), wdx_hbm, wd_x)
    local.start(('wd', 1), wdy_hbm, wd_y)
    barrier([line.dev(t) for line in (line_x, line_y) for t in AWAY])
    local.wait(('piece', 0), ('piece', 1))
    gather = Gather(pos, m, blk, 2 * colb, by_chip=True)

    def gate_up(v, some=HALVES):
        for k in some:
            mid, sline, *_ = sets[k]

            @pl.loop(0, n_rows // CHUNK, unroll=2)
            def _(j):
                x = mid[sline.block(v, n_rows, j * CHUNK, CHUNK), :].astype(f32)
                normed[chunk(j, k * n_rows), :] = norm_rows(x, gain_rows[1:2, :])

        @pl.loop(0, len(tiles(ffb)))
        def _(i):
            mine = pl.ds(some[0] * n_rows, len(some) * n_rows)
            g, u = (jnp.dot(normed[mine, :], wgu[:, :, :, tile_of(i, base)].reshape(width, -1), preferred_element_type=f32)
                    for base in (0, ffb))
            a = (jax.nn.silu(g) * u).astype(bf16)
            for i_k, k in enumerate(some):
                mid, sline, gline, act, *_ = sets[k]
                act[0, sline.block(v, n_rows), tile_of(i)] = a[i_k * n_rows:(i_k + 1) * n_rows]

    def share(v, some=HALVES):
        for mid, sline, gline, act, *_ in (sets[k] for k in some):
            rows = sline.block(v, n_rows)
            gline.share(act, v, rows)
            if v == 2:
                gline.start(('direct', v), act.at[0, rows], act.at[slot_back(2), rows], 2)

    def share_on(v):
        for mid, sline, gline, act, *_ in sets:
            gline.share_on(act, v, lambda cut: sline.block(v, n_rows, *cut(n_rows)))

    def down(v):
        at = STEPS.index(v)
        for mid, sline, gline, act, w, total, got in sets:
            if v == 2:
                for sign in SIGNS:
                    gline.recv('share', sign, v)
                gline.recv('direct', v)
            else:
                gline.share_last(v)

            @pl.loop(0, len(tiles(colb)))
            def _(i):
                total[at, :, tile_of(i)] = sum(
                    jnp.dot(act[t, sline.block(v, n_rows), :], w[t, :, :, tile_of(i)].reshape(ffb, -1), preferred_element_type=f32)
                    for t in range(len(STEPS)))

            if v != 0:
                sline.start(('sum', v), total.at[at], got.at[slot_back(v) - 1], v)

    gather.begin()
    local.wait('wgu')
    gate_up(0)
    share(0)
    gather.forward()
    gate_up(1)
    share(1)
    share_on(0)
    gate_up(-1)
    share(-1)
    share_on(1)
    for a in STEPS:
        gather.last(a)
    share_on(-1)
    for k in HALVES:
        gate_up(2, (k,))
        share(2, (k,))
    local.wait(('wd', 0), ('wd', 1))
    for v in (1, -1, 2, 0):
        down(v)
    for k, (mid, sline, gline, act, w, total, got) in enumerate(sets):
        for v in AWAY:
            sline.recv('sum', v)
        cols = gline.lanes(0, colb)

        @pl.loop(0, n_rows // CHUNK)
        def _(j):
            rows = chunk(j)
            x = mid[sline.block(0, n_rows, j * CHUNK, CHUNK), cols].astype(f32)
            fin[k, rows, :] = (x + (total[0, rows, :] + sum(got[i, rows, :] for i in range(len(AWAY))))).astype(bf16)

        mine_rows = pl.ds(k * half_rows, half_rows)
        for t in AWAY:
            gline.start(('out', t), fin.at[k, gline.block(t, half_rows)], out.at[mine_rows, cols], t)
        out[mine_rows, cols] = fin[k, gline.block(0, half_rows), :]
    m.finish()


def dma(n):
    return pltpu.SemaphoreType.DMA((n,))


def dma2(n):
    return pltpu.SemaphoreType.DMA((2, n))


def params(cid):
    return pltpu.CompilerParams(collective_id=cid, has_side_effects=True, vmem_limit_bytes=VMEM_LIMIT)


def rope_tables(rope_scale, seq_len, lanes):
    half_dim = rope_scale.shape[0]
    freq_expo = jnp.arange(half_dim, dtype=jnp.float32) * (2.0 / (2 * half_dim))
    inv_freq = 1.0 / (rope_scale * jnp.power(ROPE_THETA, freq_expo))
    angles = jnp.arange(seq_len, dtype=jnp.float32)[:, None] * inv_freq[None, :]
    cos, sin = jnp.cos(angles), jnp.sin(angles)
    rest = jnp.zeros((seq_len, lanes - 2 * half_dim), jnp.float32)
    return jnp.concatenate([cos, cos, rest], axis=1), jnp.concatenate([-sin, sin, rest], axis=1)


def solution(mesh):
    batch_axes = ('dp', AXIS)
    row_spec = P(AXIS, None)
    n_dev = mesh.shape[AXIS]
    chips = n_dev // 2
    n_off = chips - 1

    def device_step(tokens, embed_table, norm_attn, w_qkv, w_out, norm_mlp, w_gate_up, w_down, rope_scale):
        f32, bf16 = jnp.float32, jnp.bfloat16
        seq = tokens.shape[1]
        rows, d_model = w_out.shape
        head_dim = 2 * rope_scale.shape[0]
        ffb = w_gate_up.shape[1] // (2 * chips)
        qkv_width = w_qkv.shape[1] // chips
        wide = pl.cdiv(qkv_width + 2, LANES) * LANES
        toks, half_toks, colb = chips * seq, chips * seq // 2, d_model // 4
        cos2, sin2 = rope_tables(rope_scale, seq, LANES)
        vmem = pl.BlockSpec(memory_space=pltpu.VMEM)
        shape = jax.ShapeDtypeStruct

        def buf(*dims, dtype=bf16):
            return pltpu.VMEM(dims, dtype)

        wgu_shape = (chips, 2, rows, 2 * ffb)
        wd_shape = (4, 2, ffb // 2, colb)
        kv_shape = (chips, seq, 4 * head_dim)
        sum_blocks = half_toks // 4
        x_mid, mine, wgu_all, wd_x, wd_y, gain_rows = pl.pallas_call(
            front_kernel, name='front',
            out_shape=(shape((2, sum_blocks, colb), bf16), shape(kv_shape, bf16), shape(wgu_shape, bf16),
                       shape(wd_shape, bf16), shape(wd_shape, bf16), shape((8, d_model), f32)),
            in_specs=[vmem] * 6 + [ANY] * 4, out_specs=(vmem, ANY, ANY, ANY, ANY, vmem),
            scratch_shapes=[buf(*kv_shape), buf(8, LANES, dtype=jnp.int32), buf(8, LANES, dtype=f32), buf(chips, 8, LANES, dtype=jnp.int32), buf(toks, 1, dtype=f32), buf(2, *embed_table.shape),
                            buf(2, toks // 4, embed_table.shape[0]), buf(toks, d_model), buf(seq, d_model * n_off),
                            buf(toks, d_model), buf(chips, rows, wide), buf(d_model, wide), buf(2, 4, seq // 2, colb),
                            buf(5 * seq, wide, dtype=f32)]
                           + [buf(4, half_toks, 2 * LANES)] * 2 + [buf(4, 2 * LANES, colb)] * 2
                           + [buf(half_toks, colb, dtype=f32)] * 2 + [buf(3 * sum_blocks, colb, dtype=f32)] * 2
                           + [dma2(240), dma(8)],
            compiler_params=params(1),
        )(tokens, norm_attn[None], norm_mlp[None], w_qkv, cos2, sin2, w_gate_up, w_out, w_down, embed_table)

        layer_out = pl.pallas_call(
            mlp_kernel, name='mlp',
            out_shape=shape((seq, d_model), bf16),
            in_specs=[ANY, vmem] + [ANY] * 3, out_specs=vmem,
            scratch_shapes=[buf(half_toks, d_model)] * 2 + [buf(half_toks // 2, d_model), buf(*wgu_shape)]
                           + [buf(*wd_shape)] * 2 + [buf(4, half_toks, ffb)] * 2
                           + [buf(4, sum_blocks, colb, dtype=f32)] * 2 + [buf(3, sum_blocks, colb, dtype=f32)] * 2
                           + [buf(2, sum_blocks, colb), dma2(84), dma(5)],
            compiler_params=params(2),
        )(x_mid, gain_rows, wgu_all, wd_x, wd_y)

        def by_head(lo):
            part = mine[:, :, lo:lo + 2 * head_dim].transpose(1, 0, 2)
            return part.reshape(1, seq, 2 * chips, head_dim)

        key_own, val_own = by_head(0), by_head(2 * head_dim)
        return layer_out[None], key_own, val_own

    return jax.shard_map(
        device_step,
        mesh=mesh,
        in_specs=(P(batch_axes, None), row_spec, P(AXIS), row_spec, row_spec, P(AXIS), row_spec, row_spec, P(None)),
        out_specs=(P(batch_axes, None, None), P(batch_axes, None, None, None), P(batch_axes, None, None, None)),
        check_vma=False,
    )
```

```python
import jax
import jax.numpy as jnp
from jax import lax
from jax.experimental import pallas as pl
from jax.experimental.pallas import tpu as pltpu
from jax.sharding import PartitionSpec as P

NORM_EPS = 1e-5
ROPE_THETA = 10000.0
AXIS = 'fsdp'
MESH = pl.DeviceIdType.MESH
ANY = pl.BlockSpec(memory_space=pl.ANY)
VMEM_LIMIT = 60 * 1024 * 1024


class Place:
    def __init__(self, side):
        me = lax.axis_index(AXIS)
        self.side = side
        self.c = lax.rem(me, 2)
        chip = lax.div(me, 2)
        self.y = lax.div(chip, side)
        self.x = lax.rem(chip, side)
        self.me = me
        self.partner = me + 1 - 2 * self.c

    def chip(self, dy, dx):
        s = self.side
        return lax.rem(self.y + dy + s, s) * s + lax.rem(self.x + dx + s, s)

    def dev(self, dy, dx):
        return self.chip(dy, dx) * 2 + self.c


def barrier(devices):
    sem = pltpu.get_barrier_semaphore()
    for d in devices:
        pl.semaphore_signal(sem, inc=1, device_id={AXIS: d}, device_id_type=MESH)
    pl.semaphore_wait(sem, len(devices))


def remote(src, dst, sems, i, dev):
    send, recv = (sems.at[k, i] for k in (0, 1))
    return pltpu.make_async_remote_copy(src_ref=src, dst_ref=dst, send_sem=send, recv_sem=recv,
                                        device_id={AXIS: dev}, device_id_type=MESH)


class Msgs:
    def __init__(self, sems):
        self.sems, self.copies, self.received = sems, {}, set()

    def start(self, name, src, dst, dev):
        assert name not in self.copies
        self.copies[name] = remote(src, dst, self.sems, len(self.copies), dev)
        self.copies[name].start()

    def recv(self, name):
        self.received.add(name)
        self.copies[name].wait_recv()

    def finish(self):
        for name in self.copies:
            if name not in self.received:
                self.recv(name)
            self.copies[name].wait_send()


class Local:
    def __init__(self, sems):
        self.sems, self.copies = sems, {}

    def start(self, name, src, dst):
        self.copies[name] = pltpu.make_async_copy(src, dst, self.sems.at[len(self.copies)])
        self.copies[name].start()

    def wait(self, *names):
        for name in names:
            self.copies[name].wait()


STEPS = (0, 1, -1, 2)
AWAY = STEPS[1:]
SLOTS = sorted(((a, b) for a in STEPS for b in STEPS), key=lambda o: (2 in o, abs(o[0]) + abs(o[1])))


def slot_of(a, b):
    return SLOTS.index(((a + 1) % 4 - 1, (b + 1) % 4 - 1))


def slot_back(t):
    return STEPS.index(2 if t == 2 else -t)


def swap_if(h, a, b):
    return (b, a) if h == 0 else (a, b)


HALVES = (0, 1)
SIGNS = (1, -1)
LANES = 128
CHUNK = 16


def whole(n):
    return 0, n


def part_for(sign):
    return lambda n: (0 if sign > 0 else n // 2, n // 2)


def chunk(i, base=0):
    return pl.ds(pl.multiple_of(base + i * CHUNK, CHUNK), CHUNK)


class Gather:
    def __init__(self, pos, m, blk, width, by_chip=False):
        self.pos, self.m, self.blk, self.half, self.by_chip = pos, m, blk, width // 2, by_chip

    def send(self, h, name, a, b, cut, ta, tb):
        lo, n = cut(self.half)
        lo += self.half * h
        if self.by_chip:
            src = dst = self.blk(self.pos.chip(*swap_if(h, a, b)), lo, n)
        else:
            src = self.blk(slot_of(*swap_if(h, a, b)), lo, n)
            dst = self.blk(slot_of(*swap_if(h, a - ta, b - tb)), lo, n)
        self.m.start((h,) + name, src, dst, self.pos.dev(*swap_if(h, ta, tb)))

    def second(self, h, a):
        for sign in SIGNS:
            self.send(h, ('second', sign, a), a, 0, whole, 0, sign)

    def second_forward(self, a):
        for h in HALVES:
            for sign in SIGNS:
                self.m.recv((h, 'second', sign, a))
                self.send(h, ('second on', sign, a), a, -sign, part_for(sign), 0, sign)

    def last(self, a):
        for h in HALVES:
            for sign in SIGNS:
                self.m.recv((h, 'second on', sign, a))

    def begin(self):
        for h in HALVES:
            for sign in SIGNS:
                self.send(h, ('first', sign), 0, 0, whole, sign, 0)
        for h in HALVES:
            self.second(h, 0)
        for sign in SIGNS:
            for h in HALVES:
                self.m.recv((h, 'first', sign))
                self.send(h, ('first on', sign), -sign, 0, part_for(sign), sign, 0)
                self.second(h, -sign)
        self.second_forward(0)
        for h in HALVES:
            for sign in SIGNS:
                self.m.recv((h, 'first on', sign))
            self.second(h, 2)

    def forward(self):
        for a in AWAY:
            self.second_forward(a)


class Scatter:
    def __init__(self, pos, m, part, recv_buf, rows, width):
        self.pos, self.m, self.part, self.recv_buf = pos, m, part, recv_buf
        self.rows, self.half, self.used, self.places = rows, width // 2, 0, {}

    def send(self, h, name, a, b, cut, ta, tb):
        lo, n = cut(self.half)
        key = (h,) + name
        there = self.places[key] = pl.ds(self.used, n)
        self.used += n
        src = self.part.at[pl.ds(slot_of(*swap_if(1 - h, a, b)) * self.rows, self.rows), pl.ds(self.half * h + lo, n)]
        self.m.start(key, src, self.recv_buf.at[:, there], self.pos.dev(*swap_if(1 - h, ta, tb)))

    def recv_add(self, h, name, a, b, cut):
        lo, n = cut(self.half)
        key = (h,) + name
        self.m.recv(key)
        there, here = self.places[key], pl.ds(self.half * h + lo, n)
        base = slot_of(*swap_if(1 - h, a, b)) * self.rows

        @pl.loop(0, self.rows // CHUNK)
        def _(i):
            mine, theirs = chunk(i, base), chunk(i)
            self.part[mine, here] = self.part[mine, here] + self.recv_buf[theirs, there]

    def begin(self):
        for b in AWAY[::-1] + (0,):
            for h in HALVES:
                for sign in SIGNS:
                    self.send(h, ('first on', sign, b), 2, b, part_for(sign), sign, 0)

    def finish(self, hook):
        calls = iter(range(len(SLOTS)))
        order = AWAY[::-1] + (0,)
        for b in order:
            for h in HALVES:
                for sign in SIGNS:
                    self.recv_add(h, ('first on', sign, b), sign, b, part_for(sign))
                    self.send(h, ('first', sign, b), sign, b, whole, sign, 0)
                hook(next(calls))
        for b in order:
            for h in HALVES:
                for sign in SIGNS:
                    self.recv_add(h, ('first', sign, b), 0, b, whole)
                if b == 2:
                    for sign in SIGNS:
                        self.send(h, ('second on', sign), 0, b, part_for(sign), 0, sign)
                elif b == 0:
                    for sign in SIGNS:
                        self.recv_add(h, ('second', sign), 0, b, whole)
                else:
                    self.recv_add(h, ('second on', b), 0, b, part_for(b))
                    self.send(h, ('second', b), 0, b, whole, 0, b)
                hook(next(calls))


class Line:
    def __init__(self, pos, m, axis):
        self.pos, self.m, self.axis = pos, m, axis

    def dev(self, t):
        return self.pos.dev(0, t) if self.axis == 'x' else self.pos.dev(t, 0)

    def index(self, t):
        side = self.pos.side
        return lax.rem((self.pos.x if self.axis == 'x' else self.pos.y) + t + side, side)

    def block(self, t, n, lo=0, size=None):
        return pl.ds(pl.multiple_of(self.index(t) * n + lo, CHUNK), n if size is None else size)

    def lanes(self, t, n):
        return pl.ds(pl.multiple_of(self.index(t) * n, LANES), n)

    def start(self, key, src, dst, t):
        self.m.start((self.axis,) + key, src, dst, self.dev(t))

    def recv(self, *key):
        self.m.recv((self.axis,) + key)

    def share(self, buf, v, rows):
        for sign in SIGNS:
            self.start(('share', sign, v), buf.at[0, rows], buf.at[slot_back(sign), rows], sign)

    def share_on(self, buf, v, rows_of):
        for sign in SIGNS:
            self.recv('share', sign, v)
            rows = rows_of(part_for(sign))
            self.start(('share on', sign, v), buf.at[slot_back(sign), rows], buf.at[slot_back(2), rows], sign)

    def share_last(self, v):
        for sign in SIGNS:
            self.recv('share on', sign, v)

    def scatter_begin(self, part, recv_buf, rows):
        for sign in SIGNS:
            cols = pl.ds(*part_for(sign)(part.shape[1]))
            self.start(('sum on', sign), part.at[self.block(2, rows), cols], recv_buf.at[pl.ds(0, rows), cols], sign)

    def add(self, part, recv_buf, t, rows, first, cols):
        @pl.loop(0, rows // CHUNK)
        def _(i):
            mine = self.block(t, rows, i * CHUNK, CHUNK)
            part[mine, cols] = part[mine, cols] + recv_buf[chunk(i, first * rows), cols]

    def scatter_middle(self, part, recv_buf, rows):
        for sign in SIGNS:
            self.recv('sum on', sign)
            self.add(part, recv_buf, sign, rows, 0, pl.ds(*part_for(sign)(part.shape[1])))
            to = recv_buf.at[pl.ds(slot_back(sign) * rows, rows)]
            self.start(('sum', sign), part.at[self.block(sign, rows)], to, sign)

    def scatter_last(self, part, recv_buf, rows):
        for sign in SIGNS:
            self.recv('sum', sign)
            self.add(part, recv_buf, 0, rows, slot_back(sign), pl.ds(*whole(part.shape[1])))


def offsets():
    return SLOTS[5:9] + SLOTS[1:5] + SLOTS[15:] + SLOTS[9:15]


def norm_rows(x, gain):
    inv = lax.rsqrt(jnp.mean(x * x, axis=-1, keepdims=True) + NORM_EPS)
    return (x * inv * gain).astype(jnp.bfloat16)


def tiles(n, tile=256):
    return [(lo, min(tile, n - lo)) for lo in range(0, n, tile)]


def tile_of(i, base=0, tile=256):
    return pl.ds(pl.multiple_of(base + i * tile, LANES), tile)


def front_kernel(tok, gain_attn, gain_mlp, wqkv, cos2, sin2, wgu, wo, wd, table,
                 x_mid, mine, wgu_all, wd_x, wd_y, gain_rows,
                 packed, tok_own, gain_own, tok_all, tok_col, tbl, hot, part, recv_buf, h_all, wq_out, wq, x_parts, proj,
                 ctx_x, ctx_y, wo_x, wo_y, sum_x, sum_y, got_x, got_y, sems, l_sem):
    f32, bf16 = jnp.float32, jnp.bfloat16
    pos = Place(4)
    m, local = Msgs(sems), Local(l_sem)
    line_x, line_y = Line(pos, m, 'x'), Line(pos, m, 'y')
    offs = offsets()
    here = pos.chip(0, 0)
    rows = wq_out.shape[1]
    seq, width = packed.shape[1], h_all.shape[1]
    n_slots = len(SLOTS)
    half, colb = seq // 2, width // 4
    ffb = wgu_all.shape[-1] // 2
    head_dim = packed.shape[2] // 4
    table_rows = table.shape[0]
    my_head = pl.ds(pl.multiple_of(pos.c * LANES, LANES), rows)
    my_rows = pl.ds(pl.multiple_of(pos.me * rows, CHUNK), rows)
    lines = ((line_x, ctx_x, wo_x, sum_x, line_y, got_x), (line_y, ctx_y, wo_y, sum_y, line_x, got_y))
    downs = ((line_x, wd_x), (line_y, wd_y))

    def cols_of(w, line, t):
        return w.at[:, line.lanes(t, colb)]

    def gate_up_block(j, chip):
        return wgu.at[:, pl.ds(pl.multiple_of((j * n_slots + chip) * ffb, LANES), ffb)]

    def gate_up_place(j):
        return wgu_all.at[here, pos.c, :, pl.ds(j * ffb, ffb)]

    local.start('table', table, tbl.at[pos.c])
    for k, (line, ctx, w, *_) in enumerate(lines):
        local.start(('wo', k), cols_of(wo, line, 0), w.at[0, my_head])
    for k, (line, w) in enumerate(downs):
        local.start(('wd', k), cols_of(wd, line, 0), w.at[0, pos.c])
    for j in HALVES:
        local.start(('wgu', j), gate_up_block(j, here), gate_up_place(j))
    tok_own[...] = jnp.zeros_like(tok_own)
    tok_own[0:1, 0:seq] = tok[...]
    tok_all[0] = tok_own[...]
    barrier([pos.dev(*o) for o in offs] + [pos.partner])

    for o in offs:
        m.start(('tok', o), tok_own, tok_all.at[slot_of(-o[0], -o[1])], pos.dev(*o))
    m.start('table', table, tbl.at[pos.c], pos.partner)
    to_send = list(offs)

    def send_gate_up(n):
        for _ in range(min(n, len(to_send))):
            o = to_send.pop(0)
            for j in HALVES:
                m.start(('wgu', j, o), gate_up_block(j, pos.chip(*o)), gate_up_place(j), pos.dev(*o))

    send_gate_up(6)
    blank = jnp.zeros((len(STEPS), LANES - rows, colb), bf16)
    for w in (wo_x, wo_y):
        for hd in HALVES:
            w[:, hd * LANES + rows:(hd + 1) * LANES, :] = blank
    block = 2 * head_dim
    gain_own[...] = jnp.zeros_like(gain_own)
    for i, gain in enumerate((gain_attn, gain_mlp)):
        gain_own[i:i + 1, 0:rows] = gain[...].astype(f32)
    gains = jnp.transpose(gain_own[...])[:rows].astype(bf16)
    gains = jnp.concatenate([gains, jnp.zeros((rows, wq.shape[1] - 3 * block - gains.shape[1]), bf16)], axis=1)
    for p in range(n_slots):
        pieces = [wqkv[:, (j * n_slots + p) * block:(j * n_slots + p + 1) * block] for j in range(3)]
        wq_out[p] = jnp.concatenate(pieces + [gains], axis=1)
    for o in offs:
        m.start(('wq', o), wq_out.at[pos.chip(*o)], wq.at[my_rows], pos.dev(*o))
    for k, (line, ctx, w, *_) in enumerate(lines):
        for t in AWAY:
            m.start(('wo', k, t), cols_of(wo, line, t), w.at[slot_back(t), my_head], line.dev(t))
    wq[my_rows, :] = wq_out[here]

    for o in offs:
        m.recv(('tok', o))
    for s in range(n_slots):
        column = jnp.transpose(tok_all[s].astype(f32))
        tok_col[pl.ds(s * seq, seq), :] = column[:seq, 0:1]
    local.wait('table')
    m.recv('table')
    group = hot.shape[1]
    for g in range(n_slots * seq // group):
        mine_rows = pl.ds(g * group, group)
        for cc in HALVES:
            ids = lax.broadcasted_iota(jnp.int32, (group, table_rows), 1) + (here * 2 + cc) * table_rows
            hot[cc] = jnp.where(tok_col[mine_rows, :] == ids.astype(f32), 1.0, 0.0).astype(bf16)

        @pl.loop(0, len(tiles(width)))
        def _(i):
            cols = tile_of(i)
            part[mine_rows, cols] = sum(jnp.dot(hot[cc], tbl[cc, :, cols], preferred_element_type=f32)
                                        for cc in HALVES).astype(bf16)

    scatter = Scatter(pos, m, part, recv_buf, seq, width)
    scatter.begin()

    def forward(name, ref):
        m.start(('to partner', name), ref, ref, pos.partner)

    forward(('wq', 0), wq.at[my_rows])
    for o in offs:
        m.recv(('wq', o))
        forward(('wq', o), wq.at[pl.ds(pl.multiple_of(pos.dev(-o[0], -o[1]) * rows, CHUNK), rows)])
    for o in [0] + offs:
        m.recv(('to partner', ('wq', o)))
    qkv_width = 3 * block
    for lo, n in tiles(width, LANES):
        square = jnp.transpose(wq[pl.ds(lo, n), qkv_width // LANES * LANES:].astype(f32))
        gain_rows[:, lo:lo + n] = square[qkv_width % LANES:qkv_width % LANES + gain_rows.shape[0], :]

    scatter.finish(lambda i: send_gate_up(1 if 6 < i else 0))

    @pl.loop(0, seq // CHUNK)
    def _(i):
        h_all[chunk(i), :] = norm_rows(part[chunk(i), :].astype(f32), gain_rows[0:1, :])

    def attend(first, n):
        for lo, size in tiles(proj.shape[1]):
            proj[pl.ds(0, n * seq), lo:lo + size] = jnp.dot(
                h_all[pl.ds(first * seq, n * seq), :], wq[:, lo:lo + size], preferred_element_type=f32)
        lane = lax.broadcasted_iota(jnp.int32, (seq, LANES), 1)
        causal = lax.broadcasted_iota(jnp.int32, (seq, seq), 0) >= lax.broadcasted_iota(jnp.int32, (seq, seq), 1)
        turn = head_dim // 2

        def wide(u):
            return jnp.concatenate([u, jnp.zeros((seq, LANES - head_dim), u.dtype)], axis=1)

        def rope(u):
            u = wide(u)
            other = jnp.where(lane < turn, pltpu.roll(u, LANES - turn, 1), pltpu.roll(u, turn, 1))
            return (u * cos2[...] + other * sin2[...]).astype(bf16)

        for lo, size in tiles(n, 2):
            heads = [(s, hd) for s in range(lo, lo + size) for hd in HALVES]

            def cut(s, j, hd):
                at = (2 * j + hd) * head_dim
                return proj[pl.ds(s * seq, seq), at:at + head_dim]

            q, k = ([rope(cut(s, j, hd)) for s, hd in heads] for j in HALVES)
            v = [cut(s, 2, hd).astype(bf16) for s, hd in heads]
            scores = [lax.dot_general(a, b, (((1,), (1,)), ((), ())), preferred_element_type=f32) for a, b in zip(q, k)]
            scores = [jnp.where(causal, u * (head_dim ** -0.5), -jnp.inf) for u in scores]
            e = [jnp.exp(u - jnp.max(u, axis=-1, keepdims=True)) for u in scores]
            probs = [(u / jnp.sum(u, axis=-1, keepdims=True)).astype(bf16) for u in e]
            context = [wide(jnp.dot(p, u, preferred_element_type=f32).astype(bf16)) for p, u in zip(probs, v)]
            for i, (s, hd) in enumerate(heads):
                a, b = SLOTS[first + s]
                yq, xq = line_y.index(a), line_x.index(b)
                at = slice(hd * LANES, (hd + 1) * LANES)
                ctx_x[0, pl.ds(pl.multiple_of((yq * pos.side + xq) * half, half), half), at] = context[i][:half]
                ctx_y[0, pl.ds(pl.multiple_of((xq * pos.side + yq) * half, half), half), at] = context[i][half:]
                if hd == 1:
                    pair = [u[:, :head_dim] for u in k[i - 1:i + 1] + v[i - 1:i + 1]]
                    packed[first + s] = jnp.concatenate(pair, axis=1)

    gather = Gather(pos, m, lambda s, lo, n: h_all.at[pl.ds(s * seq, seq), pl.ds(lo, n)], width)
    local.wait(*[(name, k) for name in ('wo', 'wd', 'wgu') for k in HALVES])
    forward('wgu', wgu_all.at[here, pos.c])
    for k, (line, ctx, w, *_) in enumerate(lines):
        forward(('wo', k, 0), w.at[0, my_head])
        forward(('wd', k, 0), downs[k][1].at[0, pos.c])
        for t in AWAY:
            m.recv(('wo', k, t))
            forward(('wo', k, t), w.at[slot_back(t), my_head])

    arrived = list(offs)

    def forward_gate_up(n):
        for _ in range(min(n, len(arrived))):
            o = arrived.pop(0)
            for j in HALVES:
                m.recv(('wgu', j, o))
            forward(('wgu', o), wgu_all.at[pos.chip(-o[0], -o[1]), pos.c])

    def send_kv():
        local.start('kv', packed.at[0], mine.at[here])
        for s, o in enumerate(SLOTS[1:]):
            m.start(('kv', o), packed.at[s + 1], mine.at[here], pos.dev(*o))

    def send_down(*offsets_sent):
        for t in offsets_sent:
            for k, (line, w) in enumerate(downs):
                m.start(('wd', k, t), cols_of(wd, line, t), w.at[slot_back(t), pos.c], line.dev(t))

    def forward_down(k):
        line, w = downs[k]
        for t in AWAY:
            m.recv(('wd', k, t))
            forward(('wd', k, t), w.at[slot_back(t), pos.c])

    gather.begin()
    attend(0, 5)
    for a in (-1, 1):
        gather.second_forward(a)
    attend(5, 4)
    forward_gate_up(n_slots - 1 - len(to_send))
    gather.second_forward(2)
    for k, line in enumerate((line_x, line_y)):
        for t in AWAY:
            m.start(('x', k, t), part.at[pl.ds(k * half, half), line.lanes(t, colb)], x_parts.at[k, slot_back(t)], line.dev(t))
        x_parts[k, 0] = part[pl.ds(k * half, half), line.lanes(0, colb)]
    send_gate_up(n_slots)
    gather.last(0)
    attend(9, 2)
    for a in AWAY:
        gather.last(a)
    attend(11, 5)

    every = pl.ds(*whole(ctx_x.shape[1]))
    for line, ctx, *_ in lines:
        line.share(ctx, 'ctx', every)
    for line, ctx, *_ in lines:
        line.share_on(ctx, 'ctx', lambda cut: pl.ds(*cut(ctx_x.shape[1])))

    send_down(1, -1)
    for k in HALVES:
        for t in STEPS:
            m.recv(('to partner', ('wo', k, t)))

    def project(ctx, w, total, first, last):
        @pl.loop(0, len(tiles(colb)))
        def _(i):
            cols = tile_of(i)
            acc = sum(jnp.dot(ctx[j], w[j, :, cols], preferred_element_type=f32) for j in range(first, last))
            total[:, cols] = total[:, cols] + acc if first else acc

    n_rows = sum_x.shape[0] // 4
    for line, ctx, w, total, *_ in lines:
        project(ctx, w, total, 0, 3)
    for line, ctx, w, total, other, got in lines:
        line.share_last('ctx')
        project(ctx, w, total, 3, 4)
        other.scatter_begin(total, got, n_rows)
    send_down(2)
    send_kv()
    for line, ctx, w, total, other, got in lines:
        other.scatter_middle(total, got, n_rows)
    forward_gate_up(n_slots)
    forward_down(0)
    for k, (line, ctx, w, total, other, got) in enumerate(lines):
        other.scatter_last(total, got, n_rows)
        for t in AWAY:
            m.recv(('x', k, t))
        for i, t in enumerate(STEPS):
            lo = pl.multiple_of(line.index(t) * half, half)
            x_mid[k, pl.ds(lo, half), :] = (x_parts[k, i].astype(f32) + total[other.block(0, n_rows, lo, half), :]).astype(bf16)
    forward_down(1)
    local.wait('kv')

    m.finish()


def mlp_kernel(piece, gain_rows, wgu_hbm, wdx_hbm, wdy_hbm, out,
               mid_x, mid_y, normed, wgu, wd_x, wd_y, act_x, act_y, sum_x, sum_y, got_x, got_y, fin, sems, l_sem):
    pos = Place(4)
    f32, bf16 = jnp.float32, jnp.bfloat16
    width = out.shape[1]
    n_rows, colb = piece.shape[1:]
    half_rows = n_rows // 4
    ffb = act_x.shape[2]
    m, local = Msgs(sems), Local(l_sem)
    line_x, line_y = Line(pos, m, 'x'), Line(pos, m, 'y')
    sets = ((mid_x, line_y, line_x, act_x, wd_x, sum_x, got_x), (mid_y, line_x, line_y, act_y, wd_y, sum_y, got_y))

    def blk(p, lo, n):
        y, x = lax.div(p, pos.side), lax.rem(p, pos.side)
        r, c, ref, lo = (y, x, mid_x, lo) if lo < colb else (x, y, mid_y, lo - colb)
        return ref.at[pl.ds(pl.multiple_of(r * n_rows, n_rows), n_rows), pl.ds(pl.multiple_of(c * colb + lo, LANES), n)]

    here = pos.chip(0, 0)
    for k in HALVES:
        local.start(('piece', k), piece.at[k], blk(here, k * colb, colb))
    local.start('wgu', wgu_hbm, wgu)
    local.start(('wd', 0), wdx_hbm, wd_x)
    local.start(('wd', 1), wdy_hbm, wd_y)
    barrier([line.dev(t) for line in (line_x, line_y) for t in AWAY])
    local.wait(('piece', 0), ('piece', 1))
    gather = Gather(pos, m, blk, 2 * colb, by_chip=True)

    def gate_up(v, some=HALVES):
        for k in some:
            mid, sline, *_ = sets[k]

            @pl.loop(0, n_rows // CHUNK, unroll=2)
            def _(j):
                x = mid[sline.block(v, n_rows, j * CHUNK, CHUNK), :].astype(f32)
                normed[chunk(j, k * n_rows), :] = norm_rows(x, gain_rows[1:2, :])

        @pl.loop(0, len(tiles(ffb)))
        def _(i):
            mine = pl.ds(some[0] * n_rows, len(some) * n_rows)
            g, u = (jnp.dot(normed[mine, :], wgu[:, :, :, tile_of(i, base)].reshape(width, -1), preferred_element_type=f32)
                    for base in (0, ffb))
            a = (jax.nn.silu(g) * u).astype(bf16)
            for i_k, k in enumerate(some):
                mid, sline, gline, act, *_ = sets[k]
                act[0, sline.block(v, n_rows), tile_of(i)] = a[i_k * n_rows:(i_k + 1) * n_rows]

    def share(v, some=HALVES):
        for mid, sline, gline, act, *_ in (sets[k] for k in some):
            rows = sline.block(v, n_rows)
            gline.share(act, v, rows)
            if v == 2:
                gline.start(('direct', v), act.at[0, rows], act.at[slot_back(2), rows], 2)

    def share_on(v):
        for mid, sline, gline, act, *_ in sets:
            gline.share_on(act, v, lambda cut: sline.block(v, n_rows, *cut(n_rows)))

    def down(v):
        at = STEPS.index(v)
        for mid, sline, gline, act, w, total, got in sets:
            if v == 2:
                for sign in SIGNS:
                    gline.recv('share', sign, v)
                gline.recv('direct', v)
            else:
                gline.share_last(v)

            @pl.loop(0, len(tiles(colb)))
            def _(i):
                total[at, :, tile_of(i)] = sum(
                    jnp.dot(act[t, sline.block(v, n_rows), :], w[t, :, :, tile_of(i)].reshape(ffb, -1), preferred_element_type=f32)
                    for t in range(len(STEPS)))

            if v != 0:
                sline.start(('sum', v), total.at[at], got.at[slot_back(v) - 1], v)

    gather.begin()
    local.wait('wgu')
    gate_up(0)
    share(0)
    gather.forward()
    gate_up(1)
    share(1)
    share_on(0)
    gate_up(-1)
    share(-1)
    share_on(1)
    for a in STEPS:
        gather.last(a)
    share_on(-1)
    for k in HALVES:
        gate_up(2, (k,))
        share(2, (k,))
    local.wait(('wd', 0), ('wd', 1))
    for v in (1, -1, 2, 0):
        down(v)
    for k, (mid, sline, gline, act, w, total, got) in enumerate(sets):
        for v in AWAY:
            sline.recv('sum', v)
        cols = gline.lanes(0, colb)

        @pl.loop(0, n_rows // CHUNK)
        def _(j):
            rows = chunk(j)
            x = mid[sline.block(0, n_rows, j * CHUNK, CHUNK), cols].astype(f32)
            fin[k, rows, :] = (x + (total[0, rows, :] + sum(got[i, rows, :] for i in range(len(AWAY))))).astype(bf16)

        mine_rows = pl.ds(k * half_rows, half_rows)
        for t in AWAY:
            gline.start(('out', t), fin.at[k, gline.block(t, half_rows)], out.at[mine_rows, cols], t)
        out[mine_rows, cols] = fin[k, gline.block(0, half_rows), :]
    m.finish()


def dma(n):
    return pltpu.SemaphoreType.DMA((n,))


def dma2(n):
    return pltpu.SemaphoreType.DMA((2, n))


def params(cid):
    return pltpu.CompilerParams(collective_id=cid, has_side_effects=True, vmem_limit_bytes=VMEM_LIMIT)


def rope_tables(rope_scale, seq_len, lanes):
    half_dim = rope_scale.shape[0]
    freq_expo = jnp.arange(half_dim, dtype=jnp.float32) * (2.0 / (2 * half_dim))
    inv_freq = 1.0 / (rope_scale * jnp.power(ROPE_THETA, freq_expo))
    angles = jnp.arange(seq_len, dtype=jnp.float32)[:, None] * inv_freq[None, :]
    cos, sin = jnp.cos(angles), jnp.sin(angles)
    rest = jnp.zeros((seq_len, lanes - 2 * half_dim), jnp.float32)
    return jnp.concatenate([cos, cos, rest], axis=1), jnp.concatenate([-sin, sin, rest], axis=1)


def solution(mesh):
    batch_axes = ('dp', AXIS)
    row_spec = P(AXIS, None)
    n_dev = mesh.shape[AXIS]
    chips = n_dev // 2
    n_off = chips - 1

    def device_step(tokens, embed_table, norm_attn, w_qkv, w_out, norm_mlp, w_gate_up, w_down, rope_scale):
        f32, bf16 = jnp.float32, jnp.bfloat16
        seq = tokens.shape[1]
        rows, d_model = w_out.shape
        head_dim = 2 * rope_scale.shape[0]
        ffb = w_gate_up.shape[1] // (2 * chips)
        qkv_width = w_qkv.shape[1] // chips
        wide = pl.cdiv(qkv_width + 2, LANES) * LANES
        toks, half_toks, colb = chips * seq, chips * seq // 2, d_model // 4
        cos2, sin2 = rope_tables(rope_scale, seq, LANES)
        vmem = pl.BlockSpec(memory_space=pltpu.VMEM)
        shape = jax.ShapeDtypeStruct

        def buf(*dims, dtype=bf16):
            return pltpu.VMEM(dims, dtype)

        wgu_shape = (chips, 2, rows, 2 * ffb)
        wd_shape = (4, 2, ffb // 2, colb)
        kv_shape = (chips, seq, 4 * head_dim)
        sum_blocks = half_toks // 4
        x_mid, mine, wgu_all, wd_x, wd_y, gain_rows = pl.pallas_call(
            front_kernel, name='front',
            out_shape=(shape((2, sum_blocks, colb), bf16), shape(kv_shape, bf16), shape(wgu_shape, bf16),
                       shape(wd_shape, bf16), shape(wd_shape, bf16), shape((8, d_model), f32)),
            in_specs=[vmem] * 6 + [ANY] * 4, out_specs=(vmem, ANY, ANY, ANY, ANY, vmem),
            scratch_shapes=[buf(*kv_shape), buf(8, LANES, dtype=jnp.int32), buf(8, LANES, dtype=f32), buf(chips, 8, LANES, dtype=jnp.int32), buf(toks, 1, dtype=f32), buf(2, *embed_table.shape),
                            buf(2, toks // 4, embed_table.shape[0]), buf(toks, d_model), buf(seq, d_model * n_off),
                            buf(toks, d_model), buf(chips, rows, wide), buf(d_model, wide), buf(2, 4, seq // 2, colb),
                            buf(5 * seq, wide, dtype=f32)]
                           + [buf(4, half_toks, 2 * LANES)] * 2 + [buf(4, 2 * LANES, colb)] * 2
                           + [buf(half_toks, colb, dtype=f32)] * 2 + [buf(3 * sum_blocks, colb, dtype=f32)] * 2
                           + [dma2(240), dma(8)],
            compiler_params=params(1),
        )(tokens, norm_attn[None], norm_mlp[None], w_qkv, cos2, sin2, w_gate_up, w_out, w_down, embed_table)

        layer_out = pl.pallas_call(
            mlp_kernel, name='mlp',
            out_shape=shape((seq, d_model), bf16),
            in_specs=[ANY, vmem] + [ANY] * 3, out_specs=vmem,
            scratch_shapes=[buf(half_toks, d_model)] * 2 + [buf(half_toks // 2, d_model), buf(*wgu_shape)]
                           + [buf(*wd_shape)] * 2 + [buf(4, half_toks, ffb)] * 2
                           + [buf(4, sum_blocks, colb, dtype=f32)] * 2 + [buf(3, sum_blocks, colb, dtype=f32)] * 2
                           + [buf(2, sum_blocks, colb), dma2(84), dma(5)],
            compiler_params=params(2),
        )(x_mid, gain_rows, wgu_all, wd_x, wd_y)

        def by_head(lo):
            part = mine[:, :, lo:lo + 2 * head_dim].transpose(1, 0, 2)
            return part.reshape(1, seq, 2 * chips, head_dim)

        key_own, val_own = by_head(0), by_head(2 * head_dim)
        return layer_out[None], key_own, val_own

    return jax.shard_map(
        device_step,
        mesh=mesh,
        in_specs=(P(batch_axes, None), row_spec, P(AXIS), row_spec, row_spec, P(AXIS), row_spec, row_spec, P(None)),
        out_specs=(P(batch_axes, None, None), P(batch_axes, None, None, None), P(batch_axes, None, None, None)),
        check_vma=False,
    )
```
